32 devices in a mesh: grp: 2 (over core), tok: 16 (over z, y, x).
Axes of the slice: x: 2, y: 2, z: 4, core: 2. Of those that a mesh axis runs over, the one named last changes fastest.
Arguments:
- tokens: bfloat16 [2, 8192, 768], P('grp', 'tok'), may hold values from -6 to 6
- branch_points: int32 [2, 16], P('grp', 'tok'), may hold values from 512 to 4096, as said below
- qkv_weight: bfloat16 [768, 896], P(('grp', 'tok')), may hold values from -0.21875 to 0.21875
- out_weight: bfloat16 [768, 768], P(('grp', 'tok')), may hold values from -3 to 3
- up_weight: bfloat16 [768, 3072], P(('grp', 'tok')), may hold values from -0.21875 to 0.21875
- down_weight: bfloat16 [3072, 768], P(('grp', 'tok')), may hold values from -0.109375 to 0.109375
- query_bias: bfloat16 [768], P(('grp', 'tok')), may hold values from -1.796875 to 1.796875
- out_bias: bfloat16 [768], P(('grp', 'tok')), may hold values from -1.796875 to 1.796875
- up_bias: bfloat16 [3072], P(('grp', 'tok')), may hold values from -3 to 3
- down_bias: bfloat16 [768], P(('grp', 'tok')), may hold values from -1.796875 to 1.796875
- first_gain: bfloat16 [768], P(('grp', 'tok')), may hold values from 0.25 to 1.75
- first_shift: bfloat16 [768], P(('grp', 'tok')), may hold values from -1.796875 to 1.796875
- second_gain: bfloat16 [768], P(('grp', 'tok')), may hold values from 0.25 to 1.75
- second_shift: bfloat16 [768], P(('grp', 'tok')), may hold values from -1.796875 to 1.796875
- cotangent: bfloat16 [2, 8192, 768], P('grp', 'tok'), may hold values from -6 to 6
Outputs:
- layer_out: bfloat16 [2, 8192, 768], P('grp', 'tok')
- kv_cache: bfloat16 [2, 8192, 128], P('grp', 'tok')
- input_grad: float32 [2, 8192, 768], P('grp', 'tok')
- qkv_weight_grad: float32 [768, 896], P(('grp', 'tok'))
- out_weight_grad: float32 [768, 768], P(('grp', 'tok'))
- up_weight_grad: float32 [768, 3072], P(('grp', 'tok'))
- down_weight_grad: float32 [3072, 768], P(('grp', 'tok'))
- query_bias_grad: float32 [768], P(('grp', 'tok'))
- out_bias_grad: float32 [768], P(('grp', 'tok'))
- up_bias_grad: float32 [3072], P(('grp', 'tok'))
- down_bias_grad: float32 [768], P(('grp', 'tok'))
- first_gain_grad: float32 [768], P(('grp', 'tok'))
- first_shift_grad: float32 [768], P(('grp', 'tok'))
- second_gain_grad: float32 [768], P(('grp', 'tok'))
- second_shift_grad: float32 [768], P(('grp', 'tok'))
The draws below stay inside these ranges and needn't reach their ends.
Inputs may be any that keep to these rules, and one draw needn't show every extreme that they name: `branch_points`: entries of prompt blocks (b < 8) and of block 8, the first continuation, are 4096; the others lie in 512 to 4096.
All inputs are finite; a program needn't handle non-finite values.
Results may differ from the reference program's by a relative error of at most 0.01.
Values may be sent and summed in bfloat16 or wider, within the bound.
A program may use at most 192 MiB of HBM per device.

```python
import jax
import jax.numpy as jnp
from jax import lax

D = 768
HEADS = 12
HDIM = 64
ROT = 16
FF = 3072
TOK_DEV = 512
PDEV = 8
GROUPS = 2
BLOCKS = 16
GTOK = 8192
PROMPT = 4096
QKV = 896


def draw_branch_points(key, part):
    drawn = jax.random.randint(key, (GROUPS, BLOCKS), PROMPT // 8, PROMPT + 1)
    column = jnp.arange(BLOCKS)[None, :]
    return jnp.where(column <= PDEV, PROMPT, drawn).astype(jnp.int32)


def shard_levels(stream_key, shape, split, smallest, largest):
    factor_of = 1.0
    for position, shards_of in split:
        steps = jax.random.uniform(jax.random.fold_in(jax.random.fold_in(stream_key, 6), position), (shards_of,), jnp.float32, smallest / len(split), largest / len(split))
        factor_of = factor_of * jnp.repeat(jnp.exp(steps), shape[position] // shards_of).reshape((-1,) + (1,) * (len(shape) - 1 - position))
    return factor_of


def bell_draw(key, extent, width, bound, shards=(), kind=jnp.bfloat16):
    values = jax.random.normal(key, extent, jnp.float32) * width
    if len(shards) > 0:
        values = shard_levels(key, extent, shards, -0.22, 0.18) * values
    return jnp.clip(values, min=-bound, max=bound).astype(kind)


def setup_inputs(seed: int = 0) -> dict:
    keys = jax.random.split(jax.random.key(seed), 16)
    tokens = bell_draw(keys[0], (GROUPS, GTOK, D), 1.0, 6.0, ((0, 2), (1, 16)))
    branch_points = draw_branch_points(jax.random.fold_in(keys[15], 71), 0)
    qkv_weight = bell_draw(keys[2], (D, QKV), D ** -0.5, 0.21875, ((0, 32),))
    out_weight = bell_draw(keys[3], (D, D), 4 ** -0.5, 3.0, ((0, 32),))
    up_weight = bell_draw(keys[4], (D, FF), D ** -0.5, 0.21875, ((0, 32),))
    down_weight = bell_draw(keys[5], (FF, D), FF ** -0.5, 0.109375, ((0, 32),))
    query_bias = bell_draw(keys[6], (D,), 0.3, 1.796875, ((0, 32),))
    out_bias = bell_draw(keys[7], (D,), 0.3, 1.796875, ((0, 32),))
    up_bias = bell_draw(keys[8], (FF,), 0.5, 3.0, ((0, 32),))
    down_bias = bell_draw(keys[9], (D,), 0.3, 1.796875, ((0, 32),))
    first_gain = jnp.clip(1.0 + 0.15 * jax.random.normal(keys[10], (D,), jnp.float32), 0.25, 1.75).astype(jnp.bfloat16)
    first_shift = bell_draw(keys[11], (D,), 0.3, 1.796875, ((0, 32),))
    second_gain = jnp.clip(1.0 + 0.15 * jax.random.normal(keys[12], (D,), jnp.float32), 0.25, 1.75).astype(jnp.bfloat16)
    second_shift = bell_draw(keys[13], (D,), 0.3, 1.796875, ((0, 32),))
    cotangent = bell_draw(keys[14], (GROUPS, GTOK, D), 1.0, 6.0, ((0, 2), (1, 16)))
    return dict(tokens=tokens, branch_points=branch_points, qkv_weight=qkv_weight, out_weight=out_weight, up_weight=up_weight, down_weight=down_weight, query_bias=query_bias, out_bias=out_bias, up_bias=up_bias, down_bias=down_bias, first_gain=first_gain, first_shift=first_shift, second_gain=second_gain, second_shift=second_shift, cotangent=cotangent)


SCORE_SCALE = 0.125
NEGATIVE = -1e+30

@jax.custom_vjp
def low(v):
    return lax.optimization_barrier(v.astype(jnp.bfloat16)).astype(jnp.float32)

@jax.custom_vjp
def low_back(v):
    return v

def low_keep(v):
    return (low(v), None)

def low_pass(kept, grad):
    return (grad,)

def back_keep(v):
    return (v, None)

def back_low(kept, grad):
    return (low(grad),)
low.defvjp(low_keep, low_pass)
low_back.defvjp(back_keep, back_low)

def matmul_high(left, right):
    return jnp.dot(left, right, preferred_element_type=jnp.float32, precision=lax.Precision.HIGHEST)

def layer_norm(values, gain, shift):
    centered = values - lax.optimization_barrier(jnp.mean(values, axis=-1, keepdims=True))
    variance = lax.optimization_barrier(jnp.mean(centered * centered, axis=-1, keepdims=True))
    return centered * lax.rsqrt(variance + 1e-05) * gain + shift

def rotate(values, positions, turn_sign):
    half_dims = ROT // 2
    frequency = 10000.0 ** (-(jnp.arange(half_dims, dtype=jnp.float32) * 2.0) / ROT)
    angles = positions[:, None] * frequency[None, :]
    new_shape = (values.shape[0],) + (1,) * (values.ndim - 2) + (half_dims,)
    cosine = jnp.cos(angles).reshape(new_shape)
    sine_part = (turn_sign * jnp.sin(angles)).reshape(new_shape)
    lower_part = values[..., :half_dims]
    upper_part = values[..., half_dims:ROT]
    return jnp.concatenate([lower_part * cosine - upper_part * sine_part, upper_part * cosine + lower_part * sine_part, values[..., ROT:]], axis=-1)

def softmax_rows(scores):
    shifted = scores - lax.optimization_barrier(jnp.max(scores, axis=-1, keepdims=True))
    weights = jnp.exp(shifted)
    return weights / lax.optimization_barrier(jnp.sum(weights, axis=-1, keepdims=True))

def group_layer(group_x, group_branch, weights):
    qkv_w, out_w, up_w, down_w, query_b, out_b, up_b, down_b, gain_one, shift_one, gain_two, shift_two = weights
    total_rows = group_x.shape[0]
    first_norm = low(layer_norm(group_x, gain_one, shift_one))
    second_norm = low(layer_norm(group_x, gain_two, shift_two))
    block_ids = jnp.arange(BLOCKS, dtype=jnp.int32)
    block_starts = jnp.where(block_ids >= PDEV, group_branch, block_ids * TOK_DEV)
    positions = (block_starts[:, None] + jnp.arange(TOK_DEV, dtype=jnp.int32)[None, :]).reshape(total_rows).astype(jnp.float32)
    qkv_bias = jnp.concatenate([query_b, jnp.zeros((2 * HDIM,), jnp.float32)])
    projected = low_back(matmul_high(first_norm, qkv_w) + qkv_bias)
    queries = low(rotate(projected[:, :D].reshape(total_rows, HEADS, HDIM), positions, 1.0))
    key_rows = low(rotate(projected[:, D:D + HDIM], positions, 1.0))
    value_rows = low(projected[:, D + HDIM:])
    prompt_keys = key_rows[:PROMPT]
    prompt_values = value_rows[:PROMPT]

    def attend(block_item):
        block_q, block_k, block_v, block_branch, block_id = block_item
        is_cont = block_id >= PDEV
        columns = jnp.arange(PROMPT, dtype=jnp.int32)
        row_ids = jnp.arange(TOK_DEV, dtype=jnp.int32)
        query_pos = block_id * TOK_DEV + row_ids
        prompt_visible = jnp.where(is_cont, columns[None, :] < block_branch, columns[None, :] <= query_pos[:, None])
        own_visible = jnp.logical_and(is_cont, row_ids[None, :] <= row_ids[:, None])
        visible = jnp.concatenate([prompt_visible, own_visible], axis=1)
        all_keys = jnp.concatenate([prompt_keys, block_k], axis=0)
        all_values = jnp.concatenate([prompt_values, block_v], axis=0)
        raw = jnp.einsum('thd,jd->thj', block_q, all_keys, precision=lax.Precision.HIGHEST, preferred_element_type=jnp.float32)
        scores = low_back(raw * SCORE_SCALE)
        scores = jnp.where(visible[:, None, :], scores, NEGATIVE)
        key_probs = low(softmax_rows(scores))
        mixed = jnp.einsum('thj,jd->thd', key_probs, all_values, precision=lax.Precision.HIGHEST, preferred_element_type=jnp.float32)
        return mixed.reshape(TOK_DEV, D)
    block_items = (queries.reshape(BLOCKS, TOK_DEV, HEADS, HDIM), key_rows.reshape(BLOCKS, TOK_DEV, HDIM), value_rows.reshape(BLOCKS, TOK_DEV, HDIM), group_branch, block_ids)
    context = lax.map(jax.checkpoint(attend), block_items).reshape(total_rows, D)
    context = low(low_back(context))
    hidden = low(jax.nn.gelu(low_back(matmul_high(second_norm, up_w) + up_b), approximate=False))
    result = group_x + matmul_high(context, out_w) + out_b + matmul_high(hidden, down_w) + down_b
    return (result, jnp.concatenate([key_rows, value_rows], axis=1))

def reference(tokens, branch_points, qkv_weight, out_weight, up_weight, down_weight, query_bias, out_bias, up_bias, down_bias, first_gain, first_shift, second_gain, second_shift, cotangent):
    params = tuple((weight_arg.astype(jnp.float32) for weight_arg in (qkv_weight, out_weight, up_weight, down_weight, query_bias, out_bias, up_bias, down_bias, first_gain, first_shift, second_gain, second_shift)))
    inputs = tokens.astype(jnp.float32)

    def forward(inputs_f, *weights):

        def one_group(group_item):
            return group_layer(group_item[0], group_item[1], weights)
        outputs, kv_rows = lax.map(one_group, (inputs_f, branch_points))
        return (outputs, kv_rows)
    outputs, pullback, kv_rows = jax.vjp(forward, inputs, *params, has_aux=True)
    all_grads = pullback(cotangent.astype(jnp.float32))
    return (outputs.astype(jnp.bfloat16), kv_rows.astype(jnp.bfloat16), all_grads[0], all_grads[1], all_grads[2], all_grads[3], all_grads[4], all_grads[5], all_grads[6], all_grads[7], all_grads[8], all_grads[9], all_grads[10], all_grads[11], all_grads[12])
```

```python
from functools import partial

import jax
import jax.numpy as jnp
from jax import lax
from jax.experimental import pallas as pl
from jax.experimental.pallas import tpu as pltpu
from jax.sharding import PartitionSpec as P

HEADS = 12
HDIM = 64
ROT = 16
PDEV = 8
SCORE_SCALE = 0.125
NEGATIVE = -1e30
AXES = ("grp", "tok")
CHUNK = 512


def layer_norm(values, gain, shift):
    centered = values - jnp.mean(values, axis=-1, keepdims=True)
    variance = jnp.mean(centered * centered, axis=-1, keepdims=True)
    return centered * lax.rsqrt(variance + 1e-05) * gain + shift


def turn_tables(positions, width):
    half = ROT // 2
    lane = jnp.arange(width, dtype=jnp.int32) % HDIM
    frequency = 10000.0 ** (-((lane % half).astype(jnp.float32) * 2.0) / ROT)
    short = frequency[:half]
    angles = positions[:, None] * short[None, :]
    reps = width // half
    cosine = jnp.tile(jnp.cos(angles), (1, reps))
    sine = jnp.tile(jnp.sin(angles), (1, reps))
    own = jnp.where(lane < ROT, cosine, 1.0)
    from_right = jnp.where(lane < half, -sine, 0.0)
    from_left = jnp.where(jnp.logical_and(lane >= half, lane < ROT), sine, 0.0)
    return own, from_right, from_left


def turn(values, tables, sign):
    own, from_right, from_left = tables
    reps = values.shape[1] // own.shape[1]
    half = ROT // 2
    own, from_right, from_left = (jnp.tile(t, (1, reps)) for t in tables)
    return (
        values * own
        + sign * (jnp.roll(values, -half, axis=1) * from_right)
        + sign * (jnp.roll(values, half, axis=1) * from_left)
    )


def attention_kernel(
    key_count,
    q_ref,
    dc_ref,
    k2_ref,
    k2t_ref,
    v2_ref,
    v2t_ref,
    bias_ref,
    ctx_ref,
    dq_ref,
    dkt_ref,
    dvt_ref,
    s_ref,
    e_ref,
):
    rows = q_ref.shape[0]
    pair = 2 * HDIM
    prompt = key_count - rows
    unroll = 4

    @pl.when(pl.program_id(0) == 0)
    def _():
        dkt_ref[...] = jnp.zeros_like(dkt_ref)
        dvt_ref[...] = jnp.zeros_like(dvt_ref)

    first_head = lax.broadcasted_iota(jnp.int32, (rows, pair), 1) < HDIM

    def stacked(both):
        return jnp.concatenate(
            [jnp.where(first_head, both, 0.0), jnp.where(first_head, 0.0, both)], axis=0
        ).astype(jnp.bfloat16)

    def turned(both):
        flipped = both.T.astype(jnp.bfloat16)
        return jnp.concatenate([flipped[:HDIM], flipped[HDIM:]], axis=1)

    q_both = q_ref[...].astype(jnp.float32)
    q_rows = stacked(q_both)
    q_cols = turned(q_both)

    def lane_max(top, scores):
        for j in range(scores.shape[1] // pair):
            top = jnp.maximum(top, scores[:, j * pair : (j + 1) * pair])
        return top

    def score_step(c, top):
        cols = pl.ds(pl.multiple_of(c * CHUNK, CHUNK), CHUNK)
        scores = jnp.dot(q_rows, k2t_ref[:, cols], preferred_element_type=jnp.float32)
        scores = scores + bias_ref[0:1, cols]
        s_ref[:, cols] = scores
        return lane_max(top, scores)

    top = lax.fori_loop(
        0,
        prompt // CHUNK,
        score_step,
        jnp.full((2 * rows, pair), NEGATIVE, jnp.float32),
        unroll=unroll,
    )
    row_id = lax.broadcasted_iota(jnp.int32, (2 * rows, rows), 0) % rows
    col_id = lax.broadcasted_iota(jnp.int32, (2 * rows, rows), 1)
    scores = jnp.dot(q_rows, k2t_ref[:, prompt:], preferred_element_type=jnp.float32)
    scores = jnp.where(col_id <= row_id, scores, NEGATIVE)
    s_ref[:, prompt:] = scores
    top = jnp.max(lane_max(top, scores), axis=1, keepdims=True)

    def weight_step(c, carry):
        total, mixed = carry
        cols = pl.ds(pl.multiple_of(c * CHUNK, CHUNK), CHUNK)
        weights = jnp.exp(s_ref[:, cols] - top)
        for j in range(CHUNK // pair):
            total = total + weights[:, j * pair : (j + 1) * pair]
        low = weights.astype(jnp.bfloat16)
        e_ref[:, cols] = low
        mixed = mixed + jnp.dot(low, v2_ref[cols, :], preferred_element_type=jnp.float32)
        return total, mixed

    zero = jnp.zeros((2 * rows, pair), jnp.float32)
    total, mixed = lax.fori_loop(
        0, key_count // CHUNK, weight_step, (zero, zero), unroll=unroll
    )
    scale = 1.0 / jnp.sum(total, axis=1, keepdims=True)
    mixed = mixed * scale
    context = jnp.where(first_head, mixed[:rows], mixed[rows:])
    ctx_ref[...] = context.astype(ctx_ref.dtype)
    d_context = dc_ref[...]
    product = d_context * context
    delta_a = jnp.sum(jnp.where(first_head, product, 0.0), axis=1, keepdims=True)
    delta_b = jnp.sum(jnp.where(first_head, 0.0, product), axis=1, keepdims=True)
    delta = jnp.concatenate([delta_a, delta_b], axis=0) * scale
    d_both = d_context * jnp.where(first_head, scale[:rows], scale[rows:])
    d_rows = stacked(d_both)
    d_cols = turned(d_both)

    def grad_step(c, d_query):
        cols = pl.ds(pl.multiple_of(c * CHUNK, CHUNK), CHUNK)
        d_probs = jnp.dot(d_rows, v2t_ref[:, cols], preferred_element_type=jnp.float32)
        low = e_ref[:, cols]
        d_scores = (low.astype(jnp.float32) * (d_probs - delta)).astype(jnp.bfloat16)
        dvt_ref[:, cols] += jnp.dot(d_cols, low, preferred_element_type=jnp.float32)
        dkt_ref[:, cols] += jnp.dot(q_cols, d_scores, preferred_element_type=jnp.float32)
        return d_query + jnp.dot(d_scores, k2_ref[cols, :], preferred_element_type=jnp.float32)

    d_query = lax.fori_loop(0, key_count // CHUNK, grad_step, zero, unroll=unroll)
    dq_ref[...] = jnp.where(first_head, d_query[:rows], d_query[rows:]) * SCORE_SCALE


def attention(queries, d_context, keys_values, limit):
    key_count = keys_values.shape[0]
    rows, width = queries.shape
    pair = 2 * HDIM
    keys = keys_values[:, :HDIM]
    values = keys_values[:, HDIM:]
    k2 = jnp.concatenate([keys, keys], axis=1)
    v2 = jnp.concatenate([values, values], axis=1)
    column = jnp.arange(key_count, dtype=jnp.int32)
    shown = jnp.logical_or(column < limit, column >= key_count - rows)
    bias = jnp.broadcast_to(jnp.where(shown, 0.0, NEGATIVE)[None], (8, key_count))

    def whole(*shape):
        return pl.BlockSpec(shape, lambda i: (0, 0))

    block = pl.BlockSpec((rows, pair), lambda i: (0, i))
    return pl.pallas_call(
        partial(attention_kernel, key_count),
        grid=(width // pair,),
        in_specs=[
            block,
            block,
            whole(key_count, pair),
            whole(pair, key_count),
            whole(key_count, pair),
            whole(pair, key_count),
            whole(8, key_count),
        ],
        out_specs=[block, block, whole(HDIM, key_count), whole(HDIM, key_count)],
        out_shape=[
            jax.ShapeDtypeStruct((rows, width), jnp.bfloat16),
            jax.ShapeDtypeStruct((rows, width), jnp.float32),
            jax.ShapeDtypeStruct((HDIM, key_count), jnp.float32),
            jax.ShapeDtypeStruct((HDIM, key_count), jnp.float32),
        ],
        scratch_shapes=[
            pltpu.VMEM((2 * rows, key_count), jnp.float32),
            pltpu.VMEM((2 * rows, key_count), jnp.bfloat16),
        ],
        compiler_params=pltpu.CompilerParams(
            dimension_semantics=("arbitrary",), vmem_limit_bytes=58 << 20
        ),
        cost_estimate=pl.CostEstimate(
            flops=12 * rows * width * key_count,
            bytes_accessed=8 * rows * width + 16 * key_count * pair,
            transcendentals=rows * HEADS * key_count,
        ),
        name="attention",
    )(queries, d_context, k2, k2.T, v2, v2.T, bias)


def pack_small(parts, columns):
    flat = jnp.concatenate(parts)
    rows = -(-flat.shape[0] // columns)
    return jnp.pad(flat, (0, rows * columns - flat.shape[0])).reshape(rows, columns)


def unpack_small(packed, sizes):
    shards = packed.shape[0]
    flat = packed.reshape(shards, -1)
    parts = []
    start = 0
    for size in sizes:
        parts.append(flat[:, start : start + size].reshape(shards * size))
        start += size
    return parts


def per_device(
    tokens,
    branch_points,
    qkv_weight,
    out_weight,
    up_weight,
    down_weight,
    query_bias,
    out_bias,
    up_bias,
    down_bias,
    first_gain,
    first_shift,
    second_gain,
    second_shift,
    cotangent,
):
    row_count = tokens.shape[1]
    width = tokens.shape[2]
    shards = lax.axis_size("grp") * lax.axis_size("tok")
    small = [
        query_bias,
        out_bias,
        up_bias,
        down_bias,
        first_gain,
        first_shift,
        second_gain,
        second_shift,
    ]
    sizes = [s.shape[0] for s in small]
    head = jnp.concatenate([qkv_weight, pack_small(small, qkv_weight.shape[1])], axis=0)
    head_all = lax.all_gather(head, AXES, axis=0, tiled=False)
    qkv_rows = qkv_weight.shape[0]
    qkv_full = head_all[:, :qkv_rows].reshape(shards * qkv_rows, -1)
    (
        query_full,
        out_bias_full,
        up_bias_full,
        down_bias_full,
        gain_one,
        shift_one,
        gain_two,
        shift_two,
    ) = [p.astype(jnp.float32) for p in unpack_small(head_all[:, qkv_rows:], sizes)]
    out_full = lax.all_gather(out_weight, AXES, axis=0, tiled=True)
    up_full = lax.all_gather(up_weight, AXES, axis=0, tiled=True)
    down_full = lax.all_gather(down_weight, AXES, axis=0, tiled=True)

    block_index = lax.axis_index("tok")
    is_cont = block_index >= PDEV
    offsets = jnp.arange(row_count, dtype=jnp.int32)
    limit = jnp.where(is_cont, branch_points[0, 0], block_index * row_count)
    positions = (limit + offsets).astype(jnp.float32)
    tables = turn_tables(positions, 2 * HDIM)
    inputs = tokens[0].astype(jnp.float32)
    first_norm, first_back = jax.vjp(layer_norm, inputs, gain_one, shift_one)
    second_norm, second_back = jax.vjp(layer_norm, inputs, gain_two, shift_two)
    first_low = first_norm.astype(jnp.bfloat16)
    second_low = second_norm.astype(jnp.bfloat16)
    projected = jnp.dot(first_low, qkv_full, preferred_element_type=jnp.float32)
    queries = turn(projected[:, :width] + query_full, tables, 1.0).astype(jnp.bfloat16)
    queries = queries * jnp.asarray(SCORE_SCALE, jnp.bfloat16)
    key_lane = jnp.arange(2 * HDIM, dtype=jnp.int32) < HDIM
    key_tables = (
        jnp.where(key_lane, tables[0], 1.0),
        jnp.where(key_lane, tables[1], 0.0),
        jnp.where(key_lane, tables[2], 0.0),
    )
    key_value = turn(projected[:, width:], key_tables, 1.0).astype(jnp.bfloat16)
    prompt_len = PDEV * row_count
    all_kv = lax.all_gather(key_value, "tok", axis=0, tiled=True)
    keys_values = jnp.concatenate([all_kv[:prompt_len], key_value], axis=0)

    grad_rows = cotangent[0]
    grad_float = grad_rows.astype(jnp.float32)
    contract_last = (((1,), (1,)), ((), ()))
    contract_first = (((0,), (0,)), ((), ()))
    matmul = partial(lax.dot_general, preferred_element_type=jnp.float32)
    d_context = matmul(grad_rows, out_full, contract_last)
    context_low, d_query, d_keys_t, d_values_t = attention(
        queries, d_context, keys_values, limit
    )
    kv_terms = jnp.concatenate([d_keys_t, d_values_t], axis=0).T
    own_term = kv_terms[prompt_len:]
    group_rows = row_count * lax.axis_size("tok")
    sent = jnp.pad(
        kv_terms[:prompt_len].astype(jnp.bfloat16), ((0, group_rows - prompt_len), (0, 0))
    )
    kv_grad = own_term + lax.psum_scatter(
        sent, "tok", scatter_dimension=0, tiled=True
    ).astype(jnp.float32)

    pre_act = matmul(second_low, up_full, (((1,), (0,)), ((), ()))) + up_bias_full
    hidden, gelu_back = jax.vjp(partial(jax.nn.gelu, approximate=False), pre_act)
    hidden_low = hidden.astype(jnp.bfloat16)
    result = (
        inputs
        + jnp.dot(context_low, out_full, preferred_element_type=jnp.float32)
        + out_bias_full
    )
    result = (
        result
        + jnp.dot(hidden_low, down_full, preferred_element_type=jnp.float32)
        + down_bias_full
    )
    layer_out = result.astype(jnp.bfloat16)[None]
    d_hidden = matmul(grad_rows, down_full, contract_last)
    d_pre_low = gelu_back(d_hidden)[0].astype(jnp.bfloat16)
    d_query_back = turn(d_query, tables, -1.0)
    d_kv_back = turn(kv_grad, key_tables, -1.0)
    d_projected = jnp.concatenate([d_query_back, d_kv_back], axis=1).astype(jnp.bfloat16)
    grad_up_w = matmul(second_low, d_pre_low, contract_first)
    grad_down_w = matmul(hidden_low, grad_rows, contract_first)
    grad_out_w = matmul(context_low, grad_rows, contract_first)
    grad_qkv_w = matmul(first_low, d_projected, contract_first)
    grad_query_b = jnp.sum(d_projected[:, :width].astype(jnp.float32), axis=0)
    grad_out_b = jnp.sum(grad_float, axis=0)
    grad_up_b = jnp.sum(d_pre_low.astype(jnp.float32), axis=0)
    d_first = matmul(d_projected, qkv_full, contract_last)
    d_second = matmul(d_pre_low, up_full, contract_last)
    input_one, grad_gain_one, grad_shift_one = first_back(d_first)
    input_two, grad_gain_two, grad_shift_two = second_back(d_second)
    input_grad = (grad_float + input_one + input_two)[None]

    small_grads = [
        grad_query_b,
        grad_out_b,
        grad_up_b,
        grad_gain_one,
        grad_shift_one,
        grad_gain_two,
        grad_shift_two,
    ]
    grad_sizes = [g.shape[0] // shards for g in small_grads]
    small_flat = jnp.concatenate(
        [g.reshape(shards, -1) for g in small_grads], axis=1
    )
    columns = qkv_weight.shape[1]
    small_rows = -(-small_flat.shape[1] // columns)
    small_flat = jnp.pad(
        small_flat, ((0, 0), (0, small_rows * columns - small_flat.shape[1]))
    ).reshape(shards, small_rows, columns)
    tail = jnp.concatenate(
        [grad_qkv_w.reshape(shards, qkv_rows, columns), small_flat], axis=1
    )

    def scattered(term):
        return lax.psum_scatter(
            term.astype(jnp.bfloat16), AXES, scatter_dimension=0, tiled=True
        ).astype(jnp.float32)

    sum_up_w = scattered(grad_up_w)
    sum_down_w = scattered(grad_down_w)
    sum_out_w = scattered(grad_out_w)
    sum_tail = scattered(tail)[0]
    sum_qkv_w = sum_tail[:qkv_rows]
    (
        sum_query_b,
        sum_out_b,
        sum_up_b,
        sum_gain_one,
        sum_shift_one,
        sum_gain_two,
        sum_shift_two,
    ) = unpack_small(sum_tail[None, qkv_rows:], grad_sizes)
    return (
        layer_out,
        key_value[None],
        input_grad,
        sum_qkv_w,
        sum_out_w,
        sum_up_w,
        sum_down_w,
        sum_query_b,
        sum_out_b,
        sum_up_b,
        sum_out_b,
        sum_gain_one,
        sum_shift_one,
        sum_gain_two,
        sum_shift_two,
    )


def solution(mesh):
    placed = (
        P("grp", "tok", None),
        P("grp", "tok"),
        P(("grp", "tok"), None),
        P(("grp", "tok"), None),
        P(("grp", "tok"), None),
        P(("grp", "tok"), None),
        P(("grp", "tok")),
        P(("grp", "tok")),
        P(("grp", "tok")),
        P(("grp", "tok")),
        P(("grp", "tok")),
        P(("grp", "tok")),
        P(("grp", "tok")),
        P(("grp", "tok")),
        P("grp", "tok", None),
    )
    return jax.shard_map(
        per_device,
        mesh=mesh,
        in_specs=placed,
        out_specs=(
            P("grp", "tok", None),
            P("grp", "tok", None),
            P("grp", "tok", None),
            P(("grp", "tok"), None),
            P(("grp", "tok"), None),
            P(("grp", "tok"), None),
            P(("grp", "tok"), None),
            P(("grp", "tok")),
            P(("grp", "tok")),
            P(("grp", "tok")),
            P(("grp", "tok")),
            P(("grp", "tok")),
            P(("grp", "tok")),
            P(("grp", "tok")),
            P(("grp", "tok")),
        ),
        check_vma=False,
    )
```

```python
from functools import partial

import jax
import jax.numpy as jnp
from jax import lax
from jax.experimental import pallas as pl
from jax.experimental.pallas import tpu as pltpu
from jax.sharding import PartitionSpec as P

HEADS = 12
HDIM = 64
ROT = 16
PDEV = 8
SCORE_SCALE = 0.125
NEGATIVE = -1e30
AXES = ("grp", "tok")
CHUNK = 512


def layer_norm(values, gain, shift):
    centered = values - jnp.mean(values, axis=-1, keepdims=True)
    variance = jnp.mean(centered * centered, axis=-1, keepdims=True)
    return centered * lax.rsqrt(variance + 1e-05) * gain + shift


def turn_tables(positions, width):
    half = ROT // 2
    lane = jnp.arange(width, dtype=jnp.int32) % HDIM
    frequency = 10000.0 ** (-((lane % half).astype(jnp.float32) * 2.0) / ROT)
    short = frequency[:half]
    angles = positions[:, None] * short[None, :]
    reps = width // half
    cosine = jnp.tile(jnp.cos(angles), (1, reps))
    sine = jnp.tile(jnp.sin(angles), (1, reps))
    own = jnp.where(lane < ROT, cosine, 1.0)
    from_right = jnp.where(lane < half, -sine, 0.0)
    from_left = jnp.where(jnp.logical_and(lane >= half, lane < ROT), sine, 0.0)
    return own, from_right, from_left


def turn(values, tables, sign):
    own, from_right, from_left = tables
    reps = values.shape[1] // own.shape[1]
    half = ROT // 2
    own, from_right, from_left = (jnp.tile(t, (1, reps)) for t in tables)
    return (
        values * own
        + sign * (jnp.roll(values, -half, axis=1) * from_right)
        + sign * (jnp.roll(values, half, axis=1) * from_left)
    )


def attention_kernel(
    key_count,
    q_ref,
    dc_ref,
    k2_ref,
    k2t_ref,
    v2_ref,
    v2t_ref,
    bias_ref,
    ctx_ref,
    dq_ref,
    dkt_ref,
    dvt_ref,
    s_ref,
    e_ref,
):
    rows = q_ref.shape[0]
    pair = 2 * HDIM
    prompt = key_count - rows
    unroll = 4

    @pl.when(pl.program_id(0) == 0)
    def _():
        dkt_ref[...] = jnp.zeros_like(dkt_ref)
        dvt_ref[...] = jnp.zeros_like(dvt_ref)

    first_head = lax.broadcasted_iota(jnp.int32, (rows, pair), 1) < HDIM

    def stacked(both):
        return jnp.concatenate(
            [jnp.where(first_head, both, 0.0), jnp.where(first_head, 0.0, both)], axis=0
        ).astype(jnp.bfloat16)

    def turned(both):
        flipped = both.T.astype(jnp.bfloat16)
        return jnp.concatenate([flipped[:HDIM], flipped[HDIM:]], axis=1)

    q_both = q_ref[...].astype(jnp.float32)
    q_rows = stacked(q_both)
    q_cols = turned(q_both)

    def lane_max(top, scores):
        for j in range(scores.shape[1] // pair):
            top = jnp.maximum(top, scores[:, j * pair : (j + 1) * pair])
        return top

    def score_step(c, top):
        cols = pl.ds(pl.multiple_of(c * CHUNK, CHUNK), CHUNK)
        scores = jnp.dot(q_rows, k2t_ref[:, cols], preferred_element_type=jnp.float32)
        scores = scores + bias_ref[0:1, cols]
        s_ref[:, cols] = scores
        return lane_max(top, scores)

    top = lax.fori_loop(
        0,
        prompt // CHUNK,
        score_step,
        jnp.full((2 * rows, pair), NEGATIVE, jnp.float32),
        unroll=unroll,
    )
    row_id = lax.broadcasted_iota(jnp.int32, (2 * rows, rows), 0) % rows
    col_id = lax.broadcasted_iota(jnp.int32, (2 * rows, rows), 1)
    scores = jnp.dot(q_rows, k2t_ref[:, prompt:], preferred_element_type=jnp.float32)
    scores = jnp.where(col_id <= row_id, scores, NEGATIVE)
    s_ref[:, prompt:] = scores
    top = jnp.max(lane_max(top, scores), axis=1, keepdims=True)

    def weight_step(c, carry):
        total, mixed = carry
        cols = pl.ds(pl.multiple_of(c * CHUNK, CHUNK), CHUNK)
        weights = jnp.exp(s_ref[:, cols] - top)
        for j in range(CHUNK // pair):
            total = total + weights[:, j * pair : (j + 1) * pair]
        low = weights.astype(jnp.bfloat16)
        e_ref[:, cols] = low
        mixed = mixed + jnp.dot(low, v2_ref[cols, :], preferred_element_type=jnp.float32)
        return total, mixed

    zero = jnp.zeros((2 * rows, pair), jnp.float32)
    total, mixed = lax.fori_loop(
        0, key_count // CHUNK, weight_step, (zero, zero), unroll=unroll
    )
    scale = 1.0 / jnp.sum(total, axis=1, keepdims=True)
    mixed = mixed * scale
    context = jnp.where(first_head, mixed[:rows], mixed[rows:])
    ctx_ref[...] = context.astype(ctx_ref.dtype)
    d_context = dc_ref[...]
    product = d_context * context
    delta_a = jnp.sum(jnp.where(first_head, product, 0.0), axis=1, keepdims=True)
    delta_b = jnp.sum(jnp.where(first_head, 0.0, product), axis=1, keepdims=True)
    delta = jnp.concatenate([delta_a, delta_b], axis=0) * scale
    d_both = d_context * jnp.where(first_head, scale[:rows], scale[rows:])
    d_rows = stacked(d_both)
    d_cols = turned(d_both)

    def grad_step(c, d_query):
        cols = pl.ds(pl.multiple_of(c * CHUNK, CHUNK), CHUNK)
        d_probs = jnp.dot(d_rows, v2t_ref[:, cols], preferred_element_type=jnp.float32)
        low = e_ref[:, cols]
        d_scores = (low.astype(jnp.float32) * (d_probs - delta)).astype(jnp.bfloat16)
        dvt_ref[:, cols] += jnp.dot(d_cols, low, preferred_element_type=jnp.float32)
        dkt_ref[:, cols] += jnp.dot(q_cols, d_scores, preferred_element_type=jnp.float32)
        return d_query + jnp.dot(d_scores, k2_ref[cols, :], preferred_element_type=jnp.float32)

    d_query = lax.fori_loop(0, key_count // CHUNK, grad_step, zero, unroll=unroll)
    dq_ref[...] = jnp.where(first_head, d_query[:rows], d_query[rows:]) * SCORE_SCALE


def attention(queries, d_context, keys_values, limit):
    key_count = keys_values.shape[0]
    rows, width = queries.shape
    pair = 2 * HDIM
    keys = keys_values[:, :HDIM]
    values = keys_values[:, HDIM:]
    k2 = jnp.concatenate([keys, keys], axis=1)
    v2 = jnp.concatenate([values, values], axis=1)
    column = jnp.arange(key_count, dtype=jnp.int32)
    shown = jnp.logical_or(column < limit, column >= key_count - rows)
    bias = jnp.broadcast_to(jnp.where(shown, 0.0, NEGATIVE)[None], (8, key_count))

    def whole(*shape):
        return pl.BlockSpec(shape, lambda i: (0, 0))

    block = pl.BlockSpec((rows, pair), lambda i: (0, i))
    return pl.pallas_call(
        partial(attention_kernel, key_count),
        grid=(width // pair,),
        in_specs=[
            block,
            block,
            whole(key_count, pair),
            whole(pair, key_count),
            whole(key_count, pair),
            whole(pair, key_count),
            whole(8, key_count),
        ],
        out_specs=[block, block, whole(HDIM, key_count), whole(HDIM, key_count)],
        out_shape=[
            jax.ShapeDtypeStruct((rows, width), jnp.bfloat16),
            jax.ShapeDtypeStruct((rows, width), jnp.float32),
            jax.ShapeDtypeStruct((HDIM, key_count), jnp.float32),
            jax.ShapeDtypeStruct((HDIM, key_count), jnp.float32),
        ],
        scratch_shapes=[
            pltpu.VMEM((2 * rows, key_count), jnp.float32),
            pltpu.VMEM((2 * rows, key_count), jnp.bfloat16),
        ],
        compiler_params=pltpu.CompilerParams(
            dimension_semantics=("arbitrary",), vmem_limit_bytes=58 << 20
        ),
        cost_estimate=pl.CostEstimate(
            flops=12 * rows * width * key_count,
            bytes_accessed=8 * rows * width + 16 * key_count * pair,
            transcendentals=rows * HEADS * key_count,
        ),
        name="attention",
    )(queries, d_context, k2, k2.T, v2, v2.T, bias)


MESH = pl.DeviceIdType.MESH
Z_CHIPS = 4
ROUTES = ("yx", "xy", "yx", "xy")
SLABS = 32


def chip_place():
    tok = lax.axis_index("tok")
    return tok // 4, (tok // 2) % 2, tok % 2, lax.axis_index("grp")


def near(place, k=0, fy=0, fx=0, fg=0):
    z, y, x, g = place
    zz = (z, z + 1 - 2 * (z % 2), (z + 2) % Z_CHIPS, Z_CHIPS - 1 - z)[k]
    return zz, (1 - y if fy else y), (1 - x if fx else x), (1 - g if fg else g)


def device_at(coords):
    z, y, x, g = coords
    return {"tok": z * 4 + y * 2 + x, "grp": g}


def slot_at(coords):
    z, y, x, g = coords
    return g * 16 + z * 4 + y * 2 + x


def near_pq(place, order, k=0, fp=0, fq=0, fg=0):
    if order == "yx":
        return near(place, k, fp, fq, fg)
    return near(place, k, fq, fp, fg)


def greet(place):
    barrier = pltpu.get_barrier_semaphore()
    peers = [near(place, k=1), near(place, k=2), near(place, k=3)]
    peers += [near(place, fy=1), near(place, fx=1), near(place, fg=1)]
    for peer in peers:
        pl.semaphore_signal(barrier, inc=1, device_id=device_at(peer), device_id_type=MESH)
    pl.semaphore_wait(barrier, len(peers))


def remote(src, dst, send_sem, recv_sem, coords):
    return pltpu.make_async_remote_copy(
        src_ref=src,
        dst_ref=dst,
        send_sem=send_sem,
        recv_sem=recv_sem,
        device_id=device_at(coords),
        device_id_type=MESH,
    )


class Gather:
    def __init__(self, place, orders, ins, outs, send, recv, local):
        self.place, self.orders, self.ins, self.outs = place, orders, ins, outs
        self.send, self.recv, self.local = send, recv, local
        self.started = []

    def push(self, a, src, slot, index, coords):
        copy = remote(
            src, self.outs[a].at[slot], self.send.at[a, index], self.recv.at[a, index], coords
        )
        copy.start()
        self.started.append(copy)

    def spread(self, a, k, fp, fq):
        place, order = self.place, self.orders[a]
        slot = slot_at(near_pq(place, order, k, fp, fq))
        own = k == 0 and fp == 0 and fq == 0
        src = self.ins[a] if own else self.outs[a].at[slot]
        if own:
            for j in (1, 2, 3):
                self.push(a, src, slot, j * 4, near(place, k=j))
        if fp == 0 and fq == 0:
            self.push(a, src, slot, k * 4 + 2, near_pq(place, order, fp=1))
        if fq == 0:
            self.push(a, src, slot, k * 4 + fp * 2 + 1, near_pq(place, order, fq=1))
        self.push(a, src, slot, 16 + k * 4 + fp * 2 + fq, near(place, fg=1))

    def arrived(self, a, k, fp, fq, fg=0):
        slot = slot_at(near_pq(self.place, self.orders[a], k, fp, fq, fg))
        index = 16 * fg + k * 4 + fp * 2 + fq
        block = self.outs[a].at[slot]
        remote(
            block, block, self.send.at[a, index], self.recv.at[a, index], near(self.place, fg=1)
        ).wait_recv()

    def own_copy(self, a):
        slot = slot_at(self.place)
        return pltpu.make_async_copy(self.ins[a], self.outs[a].at[slot], self.local.at[a])

    def begin(self, arrays):
        for a in arrays:
            self.spread(a, 0, 0, 0)
            self.own_copy(a).start()

    def pass_on(self, arrays, slabs):
        for slab in slabs:
            for a in arrays:
                self.arrived(a, *slab)
                self.spread(a, *slab)

    def finish(self, arrays):
        for a in arrays:
            self.own_copy(a).wait()
            for k in range(4):
                for fp in range(2):
                    for fq in range(2):
                        self.arrived(a, k, fp, fq, 1)
        for copy in self.started:
            copy.wait_send()


Z_SLABS = [(1, 0, 0), (2, 0, 0), (3, 0, 0)]
P_SLABS = [(k, 1, 0) for k in range(4)]
Q_SLABS = [(k, fp, 1) for fp in range(2) for k in range(4)]


def gather_kernel(orders, *refs):
    n = len(orders)
    ins, outs = refs[:n], refs[n : 2 * n]
    send, recv, local = refs[2 * n :]
    place = chip_place()
    greet(place)
    gather = Gather(place, orders, ins, outs, send, recv, local)
    arrays = range(n)
    gather.begin(arrays)
    gather.pass_on(arrays, Z_SLABS + P_SLABS + Q_SLABS)
    gather.finish(arrays)


def gather_shards(shards, orders, collective_id, name):
    n = len(shards)
    return pl.pallas_call(
        partial(gather_kernel, orders),
        in_specs=[pl.BlockSpec(memory_space=pl.ANY)] * n,
        out_specs=[pl.BlockSpec(memory_space=pl.ANY)] * n,
        out_shape=[jax.ShapeDtypeStruct((SLABS,) + s.shape, s.dtype) for s in shards],
        scratch_shapes=[
            pltpu.SemaphoreType.DMA((n, 32)),
            pltpu.SemaphoreType.DMA((n, 32)),
            pltpu.SemaphoreType.DMA((n,)),
        ],
        compiler_params=pltpu.CompilerParams(collective_id=collective_id, has_side_effects=True),
        name=name,
    )(*shards)


class Reduce:
    def __init__(self, place, orders, ins, outs, accs, boxes, send, recv, local):
        self.place, self.orders, self.ins, self.outs = place, orders, ins, outs
        self.accs, self.boxes = accs, boxes
        self.send, self.recv, self.local = send, recv, local
        self.started = []

    def mail(self, a, src, index, coords):
        copy = remote(
            src, self.boxes[a].at[index], self.send.at[a, index], self.recv.at[a, index], coords
        )
        copy.start()
        self.started.append(copy)

    def load(self, a, k, fp, fq):
        slot = slot_at(near_pq(self.place, self.orders[a], k, fp, fq))
        sid = k * 4 + fp * 2 + fq
        return pltpu.make_async_copy(
            self.ins[a].at[slot], self.accs[a].at[sid], self.local.at[a, sid]
        )

    def begin(self, arrays, slabs):
        for k, fp, fq in slabs:
            for a in arrays:
                slot = slot_at(near_pq(self.place, self.orders[a], k, fp, fq, 1))
                sid = k * 4 + fp * 2 + fq
                self.mail(a, self.ins[a].at[slot], sid, near(self.place, fg=1))
                self.load(a, k, fp, fq).start()

    def arrived(self, a, index):
        box = self.boxes[a].at[index]
        remote(
            box, box, self.send.at[a, index], self.recv.at[a, index], near(self.place, fg=1)
        ).wait_recv()
        return box[...].astype(jnp.float32)

    def step(self, a, k, fp, fq):
        sid = k * 4 + fp * 2 + fq
        self.load(a, k, fp, fq).wait()
        total = self.accs[a][sid].astype(jnp.float32) + self.arrived(a, sid)
        place, order = self.place, self.orders[a]
        if fq == 0:
            total = total + self.arrived(a, 16 + k * 2 + fp)
        if fq == 0 and fp == 0:
            total = total + self.arrived(a, 24 + k)
        if (k, fp, fq) == (0, 0, 0):
            for j in (1, 2, 3):
                total = total + self.arrived(a, 27 + j)
            self.outs[a][...] = total
            return
        self.accs[a][sid] = total.astype(jnp.bfloat16)
        src = self.accs[a].at[sid]
        if fq == 1:
            self.mail(a, src, 16 + k * 2 + fp, near_pq(place, order, fq=1))
        elif fp == 1:
            self.mail(a, src, 24 + k, near_pq(place, order, fp=1))
        else:
            self.mail(a, src, 27 + k, near(place, k=k))

    def finish(self):
        for copy in self.started:
            copy.wait_send()


SUM_SLABS = (
    [(k, 1, 1) for k in (3, 2, 1, 0)]
    + [(k, 0, 1) for k in (3, 2, 1, 0)]
    + [(k, 1, 0) for k in (3, 2, 1, 0)]
    + [(k, 0, 0) for k in (3, 2, 1, 0)]
)


def reduce_kernel(orders, *refs):
    n = len(orders)
    ins, outs, accs, boxes = (refs[i * n : (i + 1) * n] for i in range(4))
    send, recv, local = refs[4 * n :]
    place = chip_place()
    greet(place)
    reduce = Reduce(place, orders, ins, outs, accs, boxes, send, recv, local)
    arrays = range(n)
    reduce.begin(arrays, SUM_SLABS)
    for slab in SUM_SLABS:
        for a in arrays:
            reduce.step(a, *slab)
    reduce.finish()


def reduce_shards(terms, orders, collective_id, name):
    n = len(terms)
    return pl.pallas_call(
        partial(reduce_kernel, orders),
        in_specs=[pl.BlockSpec(memory_space=pl.ANY)] * n,
        out_specs=[pl.BlockSpec(memory_space=pltpu.VMEM)] * n,
        out_shape=[jax.ShapeDtypeStruct(t.shape[1:], jnp.float32) for t in terms],
        scratch_shapes=[pltpu.VMEM((16,) + t.shape[1:], t.dtype) for t in terms]
        + [pltpu.VMEM((31,) + t.shape[1:], t.dtype) for t in terms]
        + [
            pltpu.SemaphoreType.DMA((n, 31)),
            pltpu.SemaphoreType.DMA((n, 31)),
            pltpu.SemaphoreType.DMA((n, 16)),
        ],
        compiler_params=pltpu.CompilerParams(
            collective_id=collective_id, has_side_effects=True, vmem_limit_bytes=58 << 20
        ),
        name=name,
    )(*terms)


def kv_route(place, half, fp=0, fq=0):
    if half == 0:
        return near(place, fy=fp, fx=fq)
    return near(place, fy=fq, fx=fp)


def kv_slot(coords, plane):
    return plane * 4 + coords[1] * 2 + coords[2]


def kv_gather_kernel(kv_ref, all_ref, send, recv, local):
    place = chip_place()
    z, y, x, g = place
    rows = kv_ref.shape[0] // 2
    greet(place)

    def at_z(zz):
        return (zz, y, x, g)

    def block(slot, half=None):
        if half is None:
            return all_ref.at[slot]
        return all_ref.at[slot, pl.ds(half * rows, rows)]

    def waiter(ref, index):
        remote(ref, ref, send.at[index], recv.at[index], near(place, fg=1)).wait_recv()

    own = pltpu.make_async_copy(kv_ref, block(kv_slot(place, z % 2)), local.at[0])

    def own_push(index, zz):
        return remote(
            kv_ref, block(kv_slot(place, z % 2)), send.at[index], recv.at[z % 2], at_z(zz)
        )

    def relay(plane):
        ref = block(kv_slot(place, plane))
        return remote(ref, ref, send.at[plane], recv.at[plane], at_z(3))

    @pl.when(z < 2)
    def _():
        own_push(0, 1 - z % 2).start()
        own_push(1, 2).start()
        own.start()

    started = []

    def push(ref, index, coords):
        copy = remote(ref, ref, send.at[index], recv.at[index], coords)
        copy.start()
        started.append(copy)

    @pl.when(z < 2)
    def _():
        own.wait()

    def here(plane):
        @pl.when(z != plane)
        def _():
            waiter(block(kv_slot(place, plane)), plane)

        @pl.when(z == 2)
        def _():
            relay(plane).start()

    for plane in (1, 0):
        here(plane)
        for half in range(2):
            ref = block(kv_slot(place, plane), half)
            push(ref, 2 + plane * 2 + half, kv_route(place, half, fp=1))
            push(ref, 6 + plane * 4 + half, kv_route(place, half, fq=1))
    for plane in (1, 0):
        for half in range(2):
            ref = block(kv_slot(kv_route(place, half, fp=1), plane), half)
            waiter(ref, 2 + plane * 2 + half)
            push(ref, 6 + plane * 4 + 2 + half, kv_route(place, half, fq=1))
    for plane in (1, 0):
        for fp in range(2):
            for half in range(2):
                ref = block(kv_slot(kv_route(place, half, fp, 1), plane), half)
                waiter(ref, 6 + plane * 4 + fp * 2 + half)
    for copy in started:
        copy.wait_send()

    @pl.when(z < 2)
    def _():
        own_push(0, 1 - z % 2).wait_send()
        own_push(1, 2).wait_send()

    @pl.when(z == 2)
    def _():
        relay(0).wait_send()
        relay(1).wait_send()


def gather_kv(key_value, collective_id):
    return pl.pallas_call(
        kv_gather_kernel,
        in_specs=[pl.BlockSpec(memory_space=pl.ANY)],
        out_specs=pl.BlockSpec(memory_space=pl.ANY),
        out_shape=jax.ShapeDtypeStruct((PDEV,) + key_value.shape, key_value.dtype),
        scratch_shapes=[
            pltpu.SemaphoreType.DMA((14,)),
            pltpu.SemaphoreType.DMA((14,)),
            pltpu.SemaphoreType.DMA((1,)),
        ],
        compiler_params=pltpu.CompilerParams(collective_id=collective_id, has_side_effects=True),
        name="gather_kv",
    )(key_value)


def kv_reduce_kernel(in_ref, out_ref, acc, q_box, p_box, z_box, send, recv):
    place = chip_place()
    z, y, x, g = place
    greet(place)
    started = []

    def at_z(zz):
        return (zz, y, x, g)

    def mail(src, dst, index, coords):
        copy = remote(src, dst, send.at[index], recv.at[index], coords)
        copy.start()
        started.append(copy)

    def arrived(box, index):
        remote(box, box, send.at[index], recv.at[index], near(place, fg=1)).wait_recv()
        return box[...].astype(jnp.float32)

    def slot(plane, half, fp=0, fq=0):
        return kv_slot(kv_route(place, half, fp, fq), plane)

    order = [(plane, half) for plane in (0, 1) for half in (0, 1)]
    for fp in (1, 0):
        for plane, half in order:
            index = plane * 4 + fp * 2 + half
            mail(
                in_ref.at[slot(plane, half, fp, 1), half],
                q_box.at[index],
                index,
                kv_route(place, half, fq=1),
            )
    for plane, half in order:
        index = plane * 2 + half
        box = q_box.at[plane * 4 + 2 + half]
        total = in_ref[slot(plane, half, 1, 0), half].astype(jnp.float32) + arrived(
            box, plane * 4 + 2 + half
        )
        acc[4 + index] = total.astype(acc.dtype)
        mail(acc.at[4 + index], p_box.at[index], 8 + index, kv_route(place, half, fp=1))

    def to_z(index, box, zz):
        return remote(acc.at[index], z_box.at[box], send.at[12 + index], recv.at[12 + box], at_z(zz))

    for plane, half in order:
        index = plane * 2 + half
        total = in_ref[slot(plane, half), half].astype(jnp.float32)
        total = total + arrived(q_box.at[plane * 4 + half], plane * 4 + half)
        total = total + arrived(p_box.at[index], 8 + index)

        @pl.when(z == 2)
        def _():
            acc[index] = (total + arrived(z_box.at[index], 12 + index)).astype(acc.dtype)
            to_z(index, half, plane).start()

        @pl.when(z == 3)
        def _():
            acc[index] = total.astype(acc.dtype)
            to_z(index, index, 2).start()

        @pl.when(z == 1 - plane)
        def _():
            acc[index] = total.astype(acc.dtype)
            to_z(index, 2 + half, plane).start()

        @pl.when(z == plane)
        def _():
            out_ref[half] = total

    @pl.when(z < 2)
    def _():
        for half in range(2):
            first = arrived(z_box.at[2 + half], 14 + half)
            second = arrived(z_box.at[half], 12 + half)
            out_ref[half] = out_ref[half] + first + second

    @pl.when(z >= 2)
    def _():
        out_ref[...] = jnp.zeros_like(out_ref)

    for copy in started:
        copy.wait_send()
    for plane, half in order:
        index = plane * 2 + half

        @pl.when(z == 2)
        def _():
            to_z(index, half, plane).wait_send()

        @pl.when(z == 3)
        def _():
            to_z(index, index, 2).wait_send()

        @pl.when(z == 1 - plane)
        def _():
            to_z(index, 2 + half, plane).wait_send()


def reduce_kv(terms, collective_id):
    slab = terms.shape[2:]
    return pl.pallas_call(
        kv_reduce_kernel,
        in_specs=[pl.BlockSpec(memory_space=pltpu.VMEM)],
        out_specs=pl.BlockSpec(memory_space=pltpu.VMEM),
        out_shape=jax.ShapeDtypeStruct(terms.shape[1:], jnp.float32),
        scratch_shapes=[
            pltpu.VMEM((8,) + slab, terms.dtype),
            pltpu.VMEM((8,) + slab, terms.dtype),
            pltpu.VMEM((4,) + slab, terms.dtype),
            pltpu.VMEM((4,) + slab, terms.dtype),
            pltpu.SemaphoreType.DMA((16,)),
            pltpu.SemaphoreType.DMA((16,)),
        ],
        compiler_params=pltpu.CompilerParams(collective_id=collective_id, has_side_effects=True),
        name="reduce_kv",
    )(terms)


def pack_small(flat, rows_above, columns):
    shards, count = flat.shape
    rows = -(-count // columns)
    rows += -(rows_above + rows) % 8
    flat = jnp.pad(flat, ((0, 0), (0, rows * columns - count)))
    return flat.reshape(shards, rows, columns)


def unpack_small(packed, sizes):
    shards = packed.shape[0]
    flat = packed.reshape(shards, -1)
    parts = []
    start = 0
    for size in sizes:
        parts.append(flat[:, start : start + size].reshape(shards * size))
        start += size
    return parts


def per_device(
    direct,
    tokens,
    branch_points,
    qkv_weight,
    out_weight,
    up_weight,
    down_weight,
    query_bias,
    out_bias,
    up_bias,
    down_bias,
    first_gain,
    first_shift,
    second_gain,
    second_shift,
    cotangent,
):
    row_count = tokens.shape[1]
    width = tokens.shape[2]
    shards = lax.axis_size("grp") * lax.axis_size("tok")
    small = [
        query_bias,
        out_bias,
        up_bias,
        down_bias,
        first_gain,
        first_shift,
        second_gain,
        second_shift,
    ]
    sizes = [s.shape[0] for s in small]
    qkv_rows, columns = qkv_weight.shape
    packed = pack_small(jnp.concatenate(small)[None], qkv_rows, columns)[0]
    head = jnp.concatenate([qkv_weight, packed], axis=0)
    weights = (head, out_weight, up_weight, down_weight)
    if direct:
        gathered = gather_shards(weights, ROUTES, 0, "gather")
    else:
        gathered = [lax.all_gather(w, AXES, axis=0, tiled=False) for w in weights]
    head_all, out_full, up_full, down_full = gathered
    out_full = out_full.reshape(-1, out_full.shape[2])
    up_full = up_full.reshape(-1, up_full.shape[2])
    down_full = down_full.reshape(-1, down_full.shape[2])
    qkv_full = head_all[:, :qkv_rows].reshape(shards * qkv_rows, -1)
    (
        query_full,
        out_bias_full,
        up_bias_full,
        down_bias_full,
        gain_one,
        shift_one,
        gain_two,
        shift_two,
    ) = [p.astype(jnp.float32) for p in unpack_small(head_all[:, qkv_rows:], sizes)]
    block_index = lax.axis_index("tok")
    is_cont = block_index >= PDEV
    offsets = jnp.arange(row_count, dtype=jnp.int32)
    limit = jnp.where(is_cont, branch_points[0, 0], block_index * row_count)
    positions = (limit + offsets).astype(jnp.float32)
    tables = turn_tables(positions, 2 * HDIM)
    inputs = tokens[0].astype(jnp.float32)
    first_norm, first_back = jax.vjp(layer_norm, inputs, gain_one, shift_one)
    second_norm, second_back = jax.vjp(layer_norm, inputs, gain_two, shift_two)
    first_low = first_norm.astype(jnp.bfloat16)
    second_low = second_norm.astype(jnp.bfloat16)
    projected = jnp.dot(first_low, qkv_full, preferred_element_type=jnp.float32)
    queries = turn(projected[:, :width] + query_full, tables, 1.0).astype(jnp.bfloat16)
    queries = queries * jnp.asarray(SCORE_SCALE, jnp.bfloat16)
    key_lane = jnp.arange(2 * HDIM, dtype=jnp.int32) < HDIM
    key_tables = (
        jnp.where(key_lane, tables[0], 1.0),
        jnp.where(key_lane, tables[1], 0.0),
        jnp.where(key_lane, tables[2], 0.0),
    )
    key_value = turn(projected[:, width:], key_tables, 1.0).astype(jnp.bfloat16)
    prompt_len = PDEV * row_count
    if direct:
        prompt_kv = gather_kv(key_value, 1).reshape(prompt_len, 2 * HDIM)
    else:
        prompt_kv = lax.all_gather(key_value, "tok", axis=0, tiled=True)[:prompt_len]
    keys_values = jnp.concatenate([prompt_kv, key_value], axis=0)

    grad_rows = cotangent[0]
    grad_float = grad_rows.astype(jnp.float32)
    contract_last = (((1,), (1,)), ((), ()))
    contract_first = (((0,), (0,)), ((), ()))
    matmul = partial(lax.dot_general, preferred_element_type=jnp.float32)
    d_context = matmul(grad_rows, out_full, contract_last)
    context_low, d_query, d_keys_t, d_values_t = attention(
        queries, d_context, keys_values, limit
    )
    kv_terms = jnp.stack([d_keys_t, d_values_t])
    own_term = kv_terms[:, :, prompt_len:]
    sent = kv_terms[:, :, :prompt_len].astype(jnp.bfloat16)
    sent = sent.reshape(2, HDIM, PDEV, row_count).transpose(2, 0, 1, 3)
    if direct:
        summed = reduce_kv(sent, 2)
    else:
        idle = lax.axis_size("tok") - PDEV
        sent = jnp.pad(sent, ((0, idle), (0, 0), (0, 0), (0, 0)))
        summed = lax.psum_scatter(sent, "tok", scatter_dimension=0, tiled=False)
        summed = summed.astype(jnp.float32)
    kv_grad = (own_term + summed).reshape(2 * HDIM, row_count).T

    pre_act = matmul(second_low, up_full, (((1,), (0,)), ((), ()))) + up_bias_full
    hidden, gelu_back = jax.vjp(partial(jax.nn.gelu, approximate=False), pre_act)
    hidden_low = hidden.astype(jnp.bfloat16)
    result = (
        inputs
        + jnp.dot(context_low, out_full, preferred_element_type=jnp.float32)
        + out_bias_full
    )
    result = (
        result
        + jnp.dot(hidden_low, down_full, preferred_element_type=jnp.float32)
        + down_bias_full
    )
    layer_out = result.astype(jnp.bfloat16)[None]
    d_hidden = matmul(grad_rows, down_full, contract_last)
    d_pre_low = gelu_back(d_hidden)[0].astype(jnp.bfloat16)
    d_query_back = turn(d_query, tables, -1.0)
    d_kv_back = turn(kv_grad, key_tables, -1.0)
    d_projected = jnp.concatenate([d_query_back, d_kv_back], axis=1).astype(jnp.bfloat16)
    grad_up_w = matmul(second_low, d_pre_low, contract_first)
    grad_down_w = matmul(hidden_low, grad_rows, contract_first)
    grad_out_w = matmul(context_low, grad_rows, contract_first)
    grad_qkv_w = matmul(first_low, d_projected, contract_first)
    grad_query_b = jnp.sum(d_projected[:, :width].astype(jnp.float32), axis=0)
    grad_out_b = jnp.sum(grad_float, axis=0)
    grad_up_b = jnp.sum(d_pre_low.astype(jnp.float32), axis=0)
    d_first = matmul(d_projected, qkv_full, contract_last)
    d_second = matmul(d_pre_low, up_full, contract_last)
    input_one, grad_gain_one, grad_shift_one = first_back(d_first)
    input_two, grad_gain_two, grad_shift_two = second_back(d_second)
    input_grad = (grad_float + input_one + input_two)[None]

    small_grads = [
        grad_query_b,
        grad_out_b,
        grad_up_b,
        grad_gain_one,
        grad_shift_one,
        grad_gain_two,
        grad_shift_two,
    ]
    grad_sizes = [g.shape[0] // shards for g in small_grads]
    small_flat = jnp.concatenate([g.reshape(shards, -1) for g in small_grads], axis=1)
    small_flat = pack_small(small_flat, qkv_rows, columns)

    def by_shard(term):
        return term.astype(jnp.bfloat16).reshape(shards, -1, term.shape[1])

    tail = jnp.concatenate([by_shard(grad_qkv_w), small_flat.astype(jnp.bfloat16)], axis=1)
    terms = (tail, by_shard(grad_out_w), by_shard(grad_up_w), by_shard(grad_down_w))
    if direct:
        sums = reduce_shards(terms, ROUTES, 3, "reduce")
    else:
        sums = [
            lax.psum_scatter(t, AXES, scatter_dimension=0, tiled=False).astype(jnp.float32)
            for t in terms
        ]
    sum_tail, sum_out_w, sum_up_w, sum_down_w = sums
    sum_qkv_w = sum_tail[:qkv_rows]
    (
        sum_query_b,
        sum_out_b,
        sum_up_b,
        sum_gain_one,
        sum_shift_one,
        sum_gain_two,
        sum_shift_two,
    ) = unpack_small(sum_tail[None, qkv_rows:], grad_sizes)
    return (
        layer_out,
        key_value[None],
        input_grad,
        sum_qkv_w,
        sum_out_w,
        sum_up_w,
        sum_down_w,
        sum_query_b,
        sum_out_b,
        sum_up_b,
        sum_out_b,
        sum_gain_one,
        sum_shift_one,
        sum_gain_two,
        sum_shift_two,
    )


def solution(mesh):
    direct = dict(mesh.shape) == {"grp": 2, "tok": 4 * Z_CHIPS}
    placed = (
        P("grp", "tok", None),
        P("grp", "tok"),
        P(("grp", "tok"), None),
        P(("grp", "tok"), None),
        P(("grp", "tok"), None),
        P(("grp", "tok"), None),
        P(("grp", "tok")),
        P(("grp", "tok")),
        P(("grp", "tok")),
        P(("grp", "tok")),
        P(("grp", "tok")),
        P(("grp", "tok")),
        P(("grp", "tok")),
        P(("grp", "tok")),
        P("grp", "tok", None),
    )
    return jax.shard_map(
        partial(per_device, direct),
        mesh=mesh,
        in_specs=placed,
        out_specs=(
            P("grp", "tok", None),
            P("grp", "tok", None),
            P("grp", "tok", None),
            P(("grp", "tok"), None),
            P(("grp", "tok"), None),
            P(("grp", "tok"), None),
            P(("grp", "tok"), None),
            P(("grp", "tok")),
            P(("grp", "tok")),
            P(("grp", "tok")),
            P(("grp", "tok")),
            P(("grp", "tok")),
            P(("grp", "tok")),
            P(("grp", "tok")),
            P(("grp", "tok")),
        ),
        check_vma=False,
    )
```

```python
from functools import partial

import jax
import jax.numpy as jnp
from jax import lax
from jax.experimental import pallas as pl
from jax.experimental.pallas import tpu as pltpu
from jax.sharding import PartitionSpec as P

HEADS = 12
HDIM = 64
ROT = 16
PDEV = 8
SCORE_SCALE = 0.125
NEGATIVE = -1e30
AXES = ("grp", "tok")
CHUNK = 512


def layer_norm(values, gain, shift):
    centered = values - jnp.mean(values, axis=-1, keepdims=True)
    variance = jnp.mean(centered * centered, axis=-1, keepdims=True)
    return centered * lax.rsqrt(variance + 1e-05) * gain + shift


def turn_tables(positions, width):
    half = ROT // 2
    lane = jnp.arange(width, dtype=jnp.int32) % HDIM
    frequency = 10000.0 ** (-((lane % half).astype(jnp.float32) * 2.0) / ROT)
    short = frequency[:half]
    angles = positions[:, None] * short[None, :]
    reps = width // half
    cosine = jnp.tile(jnp.cos(angles), (1, reps))
    sine = jnp.tile(jnp.sin(angles), (1, reps))
    own = jnp.where(lane < ROT, cosine, 1.0)
    from_right = jnp.where(lane < half, -sine, 0.0)
    from_left = jnp.where(jnp.logical_and(lane >= half, lane < ROT), sine, 0.0)
    return own, from_right, from_left


def turn(values, tables, sign):
    own, from_right, from_left = tables
    reps = values.shape[1] // own.shape[1]
    half = ROT // 2
    own, from_right, from_left = (jnp.tile(t, (1, reps)) for t in tables)
    return (
        values * own
        + sign * (jnp.roll(values, -half, axis=1) * from_right)
        + sign * (jnp.roll(values, half, axis=1) * from_left)
    )


MESH = pl.DeviceIdType.MESH
Z_CHIPS = 4
ROUTES = ("yx", "xy")
SLABS = 32


def chip_place():
    tok = lax.axis_index("tok")
    return tok // 4, (tok // 2) % 2, tok % 2, lax.axis_index("grp")


def near(place, k=0, fy=0, fx=0, fg=0):
    z, y, x, g = place
    zz = (z, z + 1 - 2 * (z % 2), (z + 2) % Z_CHIPS, Z_CHIPS - 1 - z)[k]
    return zz, (1 - y if fy else y), (1 - x if fx else x), (1 - g if fg else g)


def device_at(coords):
    z, y, x, g = coords
    return {"tok": z * 4 + y * 2 + x, "grp": g}


def slot_at(coords):
    z, y, x, g = coords
    return g * 16 + z * 4 + y * 2 + x


def near_pq(place, order, k=0, fp=0, fq=0, fg=0):
    if order == "yx":
        return near(place, k, fp, fq, fg)
    return near(place, k, fq, fp, fg)


def greet(place):
    barrier = pltpu.get_barrier_semaphore()
    peers = [near(place, k=1), near(place, k=2), near(place, k=3)]
    peers += [near(place, fy=1), near(place, fx=1), near(place, fg=1)]
    for peer in peers:
        pl.semaphore_signal(barrier, inc=1, device_id=device_at(peer), device_id_type=MESH)
    pl.semaphore_wait(barrier, len(peers))


def remote(src, dst, send_sem, recv_sem, coords):
    return pltpu.make_async_remote_copy(
        src_ref=src,
        dst_ref=dst,
        send_sem=send_sem,
        recv_sem=recv_sem,
        device_id=device_at(coords),
        device_id_type=MESH,
    )


class Gather:
    def __init__(self, place, orders, ins, outs, send, recv, local):
        self.place, self.orders, self.ins, self.outs = place, orders, ins, outs
        self.send, self.recv, self.local = send, recv, local
        self.started = []

    def push(self, a, slab, index, target):
        def build():
            place, order = self.place, self.orders[a]
            slot = slot_at(near_pq(place, order, *slab))
            dst = self.outs[a].at[slot]
            src = self.ins[a] if slab == (0, 0, 0) else dst
            return remote(src, dst, self.send.at[a, index], self.recv.at[a, index], target())

        build().start()
        self.started.append(build)

    def spread(self, a, k, fp, fq):
        place, order, slab = self.place, self.orders[a], (k, fp, fq)
        if slab == (0, 0, 0):
            for j in (1, 2, 3):
                self.push(a, slab, j * 4, partial(near, place, k=j))
        if fp == 0 and fq == 0:
            self.push(a, slab, k * 4 + 2, partial(near_pq, place, order, fp=1))
        if fq == 0:
            self.push(a, slab, k * 4 + fp * 2 + 1, partial(near_pq, place, order, fq=1))
        self.push(a, slab, 16 + k * 4 + fp * 2 + fq, partial(near, place, fg=1))

    def arrived(self, a, k, fp, fq, fg=0):
        slot = slot_at(near_pq(self.place, self.orders[a], k, fp, fq, fg))
        index = 16 * fg + k * 4 + fp * 2 + fq
        block = self.outs[a].at[slot]
        remote(
            block, block, self.send.at[a, index], self.recv.at[a, index], near(self.place, fg=1)
        ).wait_recv()

    def own_copy(self, a):
        slot = slot_at(self.place)
        return pltpu.make_async_copy(self.ins[a], self.outs[a].at[slot], self.local.at[a])

    def begin(self, arrays):
        for a in arrays:
            self.spread(a, 0, 0, 0)
            self.own_copy(a).start()

    def pass_on(self, arrays, slabs):
        for slab in slabs:
            for a in arrays:
                self.arrived(a, *slab)
                self.spread(a, *slab)

    def finish(self, arrays):
        for a in arrays:
            self.own_copy(a).wait()
            for k in range(4):
                for fp in range(2):
                    for fq in range(2):
                        self.arrived(a, k, fp, fq, 1)
        for build in self.started:
            build().wait_send()


Z_SLABS = [(1, 0, 0), (2, 0, 0), (3, 0, 0)]
P_SLABS = [(k, 1, 0) for k in range(4)]
Q_SLABS = [(k, fp, 1) for fp in range(2) for k in range(4)]


def gather_kernel(orders, *refs):
    n = len(orders)
    ins, outs = refs[:n], refs[n : 2 * n]
    send, recv, local = refs[2 * n :]
    place = chip_place()
    greet(place)
    gather = Gather(place, orders, ins, outs, send, recv, local)
    arrays = range(n)
    gather.begin(arrays)
    gather.pass_on(arrays, Z_SLABS + P_SLABS + Q_SLABS)
    gather.finish(arrays)


def gather_shards(shards, orders, collective_id, name):
    n = len(shards)
    return pl.pallas_call(
        partial(gather_kernel, orders),
        in_specs=[pl.BlockSpec(memory_space=pl.ANY)] * n,
        out_specs=[pl.BlockSpec(memory_space=pl.ANY)] * n,
        out_shape=[jax.ShapeDtypeStruct((SLABS,) + s.shape, s.dtype) for s in shards],
        scratch_shapes=[
            pltpu.SemaphoreType.DMA((n, 32)),
            pltpu.SemaphoreType.DMA((n, 32)),
            pltpu.SemaphoreType.DMA((n,)),
        ],
        compiler_params=pltpu.CompilerParams(collective_id=collective_id, has_side_effects=True),
        name=name,
    )(*shards)


class Reduce:
    def __init__(self, place, orders, ins, outs, accs, boxes, send, recv, local):
        self.place, self.orders, self.ins, self.outs = place, orders, ins, outs
        self.accs, self.boxes = accs, boxes
        self.send, self.recv, self.local = send, recv, local
        self.started = []

    def mail(self, a, src, index, target):
        def build():
            box = self.boxes[a].at[index]
            return remote(src(), box, self.send.at[a, index], self.recv.at[a, index], target())

        build().start()
        self.started.append(build)

    def far_term(self, a, slab):
        return self.ins[a].at[slot_at(near_pq(self.place, self.orders[a], *slab, 1))]

    def load(self, a, k, fp, fq):
        slot = slot_at(near_pq(self.place, self.orders[a], k, fp, fq))
        sid = k * 4 + fp * 2 + fq
        return pltpu.make_async_copy(
            self.ins[a].at[slot], self.accs[a].at[sid], self.local.at[a, sid]
        )

    def begin(self, arrays, slabs):
        for k, fp, fq in slabs:
            for a in arrays:
                sid = k * 4 + fp * 2 + fq
                src = partial(self.far_term, a, (k, fp, fq))
                self.mail(a, src, sid, partial(near, self.place, fg=1))
                self.load(a, k, fp, fq).start()

    def arrived(self, a, index):
        box = self.boxes[a].at[index]
        remote(
            box, box, self.send.at[a, index], self.recv.at[a, index], near(self.place, fg=1)
        ).wait_recv()
        return box[...].astype(jnp.float32)

    def step(self, a, k, fp, fq):
        sid = k * 4 + fp * 2 + fq
        self.load(a, k, fp, fq).wait()
        total = self.accs[a][sid].astype(jnp.float32) + self.arrived(a, sid)
        place, order = self.place, self.orders[a]
        if fq == 0:
            total = total + self.arrived(a, 16 + k * 2 + fp)
        if fq == 0 and fp == 0:
            total = total + self.arrived(a, 24 + k)
        if (k, fp, fq) == (0, 0, 0):
            for j in (1, 2, 3):
                total = total + self.arrived(a, 27 + j)
            self.outs[a][...] = total
            return
        self.accs[a][sid] = total.astype(jnp.bfloat16)

        def src():
            return self.accs[a].at[sid]

        if fq == 1:
            self.mail(a, src, 16 + k * 2 + fp, partial(near_pq, place, order, fq=1))
        elif fp == 1:
            self.mail(a, src, 24 + k, partial(near_pq, place, order, fp=1))
        else:
            self.mail(a, src, 27 + k, partial(near, place, k=k))

    def steps(self, arrays, slabs):
        for slab in slabs:
            for a in arrays:
                self.step(a, *slab)

    def finish(self):
        for build in self.started:
            build().wait_send()


SUM_SLABS = (
    [(k, 1, 1) for k in (3, 2, 1, 0)]
    + [(k, 0, 1) for k in (3, 2, 1, 0)]
    + [(k, 1, 0) for k in (3, 2, 1, 0)]
    + [(k, 0, 0) for k in (3, 2, 1, 0)]
)


def reduce_kernel(orders, *refs):
    n = len(orders)
    ins, outs, accs, boxes = (refs[i * n : (i + 1) * n] for i in range(4))
    send, recv, local = refs[4 * n :]
    place = chip_place()
    greet(place)
    reduce = Reduce(place, orders, ins, outs, accs, boxes, send, recv, local)
    arrays = range(n)
    reduce.begin(arrays, SUM_SLABS)
    reduce.steps(arrays, SUM_SLABS)
    reduce.finish()


def reduce_shards(terms, orders, collective_id, name):
    n = len(terms)
    return pl.pallas_call(
        partial(reduce_kernel, orders),
        in_specs=[pl.BlockSpec(memory_space=pl.ANY)] * n,
        out_specs=[pl.BlockSpec(memory_space=pltpu.VMEM)] * n,
        out_shape=[jax.ShapeDtypeStruct(t.shape[1:], jnp.float32) for t in terms],
        scratch_shapes=[pltpu.VMEM((16,) + t.shape[1:], t.dtype) for t in terms]
        + [pltpu.VMEM((31,) + t.shape[1:], t.dtype) for t in terms]
        + [
            pltpu.SemaphoreType.DMA((n, 31)),
            pltpu.SemaphoreType.DMA((n, 31)),
            pltpu.SemaphoreType.DMA((n, 16)),
        ],
        compiler_params=pltpu.CompilerParams(
            collective_id=collective_id, has_side_effects=True, vmem_limit_bytes=58 << 20
        ),
        name=name,
    )(*terms)


def kv_route(place, half, fp=0, fq=0):
    if half == 0:
        return near(place, fy=fp, fx=fq)
    return near(place, fy=fq, fx=fp)


def kv_slot(coords, plane):
    return plane * 4 + coords[1] * 2 + coords[2]


def kv_gather_kernel(kv_ref, all_ref, send, recv, local):
    place = chip_place()
    z, y, x, g = place
    rows = kv_ref.shape[0] // 2
    greet(place)

    def at_z(zz):
        return (zz, y, x, g)

    def block(slot, half=None):
        if half is None:
            return all_ref.at[slot]
        return all_ref.at[slot, pl.ds(half * rows, rows)]

    def waiter(ref, index):
        remote(ref, ref, send.at[index], recv.at[index], near(place, fg=1)).wait_recv()

    own = pltpu.make_async_copy(kv_ref, block(kv_slot(place, z % 2)), local.at[0])

    def own_push(index, zz):
        return remote(
            kv_ref, block(kv_slot(place, z % 2)), send.at[index], recv.at[z % 2], at_z(zz)
        )

    def relay(plane):
        ref = block(kv_slot(place, plane))
        return remote(ref, ref, send.at[plane], recv.at[plane], at_z(3))

    @pl.when(z < 2)
    def _():
        own_push(0, 1 - z % 2).start()
        own_push(1, 2).start()
        own.start()

    started = []

    def push(ref, index, coords):
        copy = remote(ref, ref, send.at[index], recv.at[index], coords)
        copy.start()
        started.append(copy)

    @pl.when(z < 2)
    def _():
        own.wait()

    def here(plane):
        @pl.when(z != plane)
        def _():
            waiter(block(kv_slot(place, plane)), plane)

        @pl.when(z == 2)
        def _():
            relay(plane).start()

    for plane in (1, 0):
        here(plane)
        for half in range(2):
            ref = block(kv_slot(place, plane), half)
            push(ref, 2 + plane * 2 + half, kv_route(place, half, fp=1))
            push(ref, 6 + plane * 4 + half, kv_route(place, half, fq=1))
    for plane in (1, 0):
        for half in range(2):
            ref = block(kv_slot(kv_route(place, half, fp=1), plane), half)
            waiter(ref, 2 + plane * 2 + half)
            push(ref, 6 + plane * 4 + 2 + half, kv_route(place, half, fq=1))
    for plane in (1, 0):
        for fp in range(2):
            for half in range(2):
                ref = block(kv_slot(kv_route(place, half, fp, 1), plane), half)
                waiter(ref, 6 + plane * 4 + fp * 2 + half)
    for copy in started:
        copy.wait_send()

    @pl.when(z < 2)
    def _():
        own_push(0, 1 - z % 2).wait_send()
        own_push(1, 2).wait_send()

    @pl.when(z == 2)
    def _():
        relay(0).wait_send()
        relay(1).wait_send()


def gather_kv(key_value, collective_id):
    return pl.pallas_call(
        kv_gather_kernel,
        in_specs=[pl.BlockSpec(memory_space=pl.ANY)],
        out_specs=pl.BlockSpec(memory_space=pl.ANY),
        out_shape=jax.ShapeDtypeStruct((PDEV,) + key_value.shape, key_value.dtype),
        scratch_shapes=[
            pltpu.SemaphoreType.DMA((14,)),
            pltpu.SemaphoreType.DMA((14,)),
            pltpu.SemaphoreType.DMA((1,)),
        ],
        compiler_params=pltpu.CompilerParams(collective_id=collective_id, has_side_effects=True),
        name="gather_kv",
    )(key_value)


def kv_reduce_kernel(in_ref, out_ref, acc, q_box, p_box, z_box, send, recv):
    place = chip_place()
    z, y, x, g = place
    greet(place)
    started = []

    def at_z(zz):
        return (zz, y, x, g)

    def mail(src, dst, index, coords):
        copy = remote(src, dst, send.at[index], recv.at[index], coords)
        copy.start()
        started.append(copy)

    def arrived(box, index):
        remote(box, box, send.at[index], recv.at[index], near(place, fg=1)).wait_recv()
        return box[...].astype(jnp.float32)

    def slot(plane, half, fp=0, fq=0):
        return kv_slot(kv_route(place, half, fp, fq), plane)

    order = [(plane, half) for plane in (0, 1) for half in (0, 1)]
    for fp in (1, 0):
        for plane, half in order:
            index = plane * 4 + fp * 2 + half
            mail(
                in_ref.at[slot(plane, half, fp, 1), half],
                q_box.at[index],
                index,
                kv_route(place, half, fq=1),
            )
    for plane, half in order:
        index = plane * 2 + half
        box = q_box.at[plane * 4 + 2 + half]
        total = in_ref[slot(plane, half, 1, 0), half].astype(jnp.float32) + arrived(
            box, plane * 4 + 2 + half
        )
        acc[4 + index] = total.astype(acc.dtype)
        mail(acc.at[4 + index], p_box.at[index], 8 + index, kv_route(place, half, fp=1))

    def to_z(index, box, zz):
        return remote(acc.at[index], z_box.at[box], send.at[12 + index], recv.at[12 + box], at_z(zz))

    for plane, half in order:
        index = plane * 2 + half
        total = in_ref[slot(plane, half), half].astype(jnp.float32)
        total = total + arrived(q_box.at[plane * 4 + half], plane * 4 + half)
        total = total + arrived(p_box.at[index], 8 + index)

        @pl.when(z == 2)
        def _():
            acc[index] = (total + arrived(z_box.at[index], 12 + index)).astype(acc.dtype)
            to_z(index, half, plane).start()

        @pl.when(z == 3)
        def _():
            acc[index] = total.astype(acc.dtype)
            to_z(index, index, 2).start()

        @pl.when(z == 1 - plane)
        def _():
            acc[index] = total.astype(acc.dtype)
            to_z(index, 2 + half, plane).start()

        @pl.when(z == plane)
        def _():
            out_ref[half] = total

    @pl.when(z < 2)
    def _():
        for half in range(2):
            first = arrived(z_box.at[2 + half], 14 + half)
            second = arrived(z_box.at[half], 12 + half)
            out_ref[half] = out_ref[half] + first + second

    @pl.when(z >= 2)
    def _():
        out_ref[...] = jnp.zeros_like(out_ref)

    for copy in started:
        copy.wait_send()
    for plane, half in order:
        index = plane * 2 + half

        @pl.when(z == 2)
        def _():
            to_z(index, half, plane).wait_send()

        @pl.when(z == 3)
        def _():
            to_z(index, index, 2).wait_send()

        @pl.when(z == 1 - plane)
        def _():
            to_z(index, 2 + half, plane).wait_send()


def reduce_kv(terms, collective_id):
    slab = terms.shape[2:]
    return pl.pallas_call(
        kv_reduce_kernel,
        in_specs=[pl.BlockSpec(memory_space=pltpu.VMEM)],
        out_specs=pl.BlockSpec(memory_space=pltpu.VMEM),
        out_shape=jax.ShapeDtypeStruct(terms.shape[1:], jnp.float32),
        scratch_shapes=[
            pltpu.VMEM((8,) + slab, terms.dtype),
            pltpu.VMEM((8,) + slab, terms.dtype),
            pltpu.VMEM((4,) + slab, terms.dtype),
            pltpu.VMEM((4,) + slab, terms.dtype),
            pltpu.SemaphoreType.DMA((16,)),
            pltpu.SemaphoreType.DMA((16,)),
        ],
        compiler_params=pltpu.CompilerParams(collective_id=collective_id, has_side_effects=True),
        name="reduce_kv",
    )(terms)


def attention_kernel(last, plan, counts, *refs):
    inputs, outputs, comm_ins, comm_outs = counts
    q_ref, dc_ref, k2_ref, k2t_ref, v2_ref, v2t_ref, bias_ref = refs[:7]
    carried = refs[7:inputs]
    cut = inputs + comm_ins
    ctx_ref, dq_ref = refs[cut : cut + 2]
    results = refs[cut + 2 : cut + outputs]
    scratch = refs[cut + outputs + comm_outs :]
    s_ref, e_ref = scratch[:2]
    if last:
        dkt_ref, dvt_ref = scratch[2:4]
        comm_scratch = scratch[4:]
    else:
        dkt_ref, dvt_ref = results
        comm_scratch = scratch[2:]
    rows = q_ref.shape[0]
    key_count = k2_ref.shape[0]
    pair = 2 * HDIM
    prompt = key_count - rows
    unroll = 4
    step = pl.program_id(0)
    events = {}
    if plan is not None:
        events = plan(refs[inputs:cut], refs[cut + outputs : cut + outputs + comm_outs], comm_scratch)

    def point(index):
        for at_step, at_point in sorted(events):
            if at_point == index:
                pl.when(step == at_step)(events[at_step, at_point])

    @pl.when(step == 0)
    def _():
        if carried:
            dkt_ref[...] = carried[0][...]
            dvt_ref[...] = carried[1][...]
        else:
            dkt_ref[...] = jnp.zeros_like(dkt_ref)
            dvt_ref[...] = jnp.zeros_like(dvt_ref)

    point(0)
    first_head = lax.broadcasted_iota(jnp.int32, (rows, pair), 1) < HDIM

    def stacked(both):
        return jnp.concatenate(
            [jnp.where(first_head, both, 0.0), jnp.where(first_head, 0.0, both)], axis=0
        ).astype(jnp.bfloat16)

    def turned(both):
        flipped = both.T.astype(jnp.bfloat16)
        return jnp.concatenate([flipped[:HDIM], flipped[HDIM:]], axis=1)

    q_both = q_ref[...].astype(jnp.float32)
    q_rows = stacked(q_both)
    q_cols = turned(q_both)

    def lane_max(top, scores):
        for j in range(scores.shape[1] // pair):
            top = jnp.maximum(top, scores[:, j * pair : (j + 1) * pair])
        return top

    def score_step(c, top):
        cols = pl.ds(pl.multiple_of(c * CHUNK, CHUNK), CHUNK)
        scores = jnp.dot(q_rows, k2t_ref[:, cols], preferred_element_type=jnp.float32)
        scores = scores + bias_ref[0:1, cols]
        s_ref[:, cols] = scores
        return lane_max(top, scores)

    top = lax.fori_loop(
        0,
        prompt // CHUNK,
        score_step,
        jnp.full((2 * rows, pair), NEGATIVE, jnp.float32),
        unroll=unroll,
    )
    row_id = lax.broadcasted_iota(jnp.int32, (2 * rows, rows), 0) % rows
    col_id = lax.broadcasted_iota(jnp.int32, (2 * rows, rows), 1)
    scores = jnp.dot(q_rows, k2t_ref[:, prompt:], preferred_element_type=jnp.float32)
    scores = jnp.where(col_id <= row_id, scores, NEGATIVE)
    s_ref[:, prompt:] = scores
    top = jnp.max(lane_max(top, scores), axis=1, keepdims=True)
    point(1)

    def weight_step(c, carry):
        total, mixed = carry
        cols = pl.ds(pl.multiple_of(c * CHUNK, CHUNK), CHUNK)
        weights = jnp.exp(s_ref[:, cols] - top)
        for j in range(CHUNK // pair):
            total = total + weights[:, j * pair : (j + 1) * pair]
        low = weights.astype(jnp.bfloat16)
        e_ref[:, cols] = low
        mixed = mixed + jnp.dot(low, v2_ref[cols, :], preferred_element_type=jnp.float32)
        return total, mixed

    zero = jnp.zeros((2 * rows, pair), jnp.float32)
    total, mixed = lax.fori_loop(
        0, key_count // CHUNK, weight_step, (zero, zero), unroll=unroll
    )
    point(2)
    scale = 1.0 / jnp.sum(total, axis=1, keepdims=True)
    mixed = mixed * scale
    context = jnp.where(first_head, mixed[:rows], mixed[rows:])
    ctx_ref[...] = context.astype(ctx_ref.dtype)
    d_context = dc_ref[...]
    product = d_context * context
    delta_a = jnp.sum(jnp.where(first_head, product, 0.0), axis=1, keepdims=True)
    delta_b = jnp.sum(jnp.where(first_head, 0.0, product), axis=1, keepdims=True)
    delta = jnp.concatenate([delta_a, delta_b], axis=0) * scale
    d_both = d_context * jnp.where(first_head, scale[:rows], scale[rows:])
    d_rows = stacked(d_both)
    d_cols = turned(d_both)

    def grad_step(c, d_query):
        cols = pl.ds(pl.multiple_of(c * CHUNK, CHUNK), CHUNK)
        d_probs = jnp.dot(d_rows, v2t_ref[:, cols], preferred_element_type=jnp.float32)
        low = e_ref[:, cols]
        d_scores = (low.astype(jnp.float32) * (d_probs - delta)).astype(jnp.bfloat16)
        dvt_ref[:, cols] += jnp.dot(d_cols, low, preferred_element_type=jnp.float32)
        dkt_ref[:, cols] += jnp.dot(q_cols, d_scores, preferred_element_type=jnp.float32)
        return d_query + jnp.dot(d_scores, k2_ref[cols, :], preferred_element_type=jnp.float32)

    d_query = lax.fori_loop(0, key_count // CHUNK, grad_step, zero, unroll=unroll)
    dq_ref[...] = jnp.where(first_head, d_query[:rows], d_query[rows:]) * SCORE_SCALE
    point(3)
    if last:

        @pl.when(step == pl.num_programs(0) - 1)
        def _():
            sent_ref, own_ref = results
            for part, total_ref in enumerate((dkt_ref, dvt_ref)):
                for block in range(prompt // rows):
                    cols = slice(block * rows, (block + 1) * rows)
                    sent_ref[block, part] = total_ref[:, cols].astype(sent_ref.dtype)
                own_ref[part] = total_ref[:, prompt:]


def attention(half, queries, d_context, tables, carried=None, comm=None, collective_id=None):
    k2, k2t, v2, v2t, bias = tables
    key_count, pair = k2.shape
    rows, width = queries.shape
    steps = width // pair // 2
    last = half == 1
    prompt_blocks = key_count // rows - 1

    def whole(*shape):
        return pl.BlockSpec(
            shape, lambda i: (0,) * len(shape), pipeline_mode=pl.Buffered(1)
        )

    def result(*shape):
        return pl.BlockSpec(shape, lambda i: (0,) * len(shape))

    block_in = pl.BlockSpec((rows, pair), lambda i: (0, i + half * steps))
    block = pl.BlockSpec((rows, pair), lambda i: (0, i))
    args = [queries, d_context, k2, k2t, v2, v2t, bias]
    in_specs = [block_in, block_in] + [whole(*a.shape) for a in args[2:]]
    out_specs = [block, block]
    out_shape = [
        jax.ShapeDtypeStruct((rows, width // 2), jnp.bfloat16),
        jax.ShapeDtypeStruct((rows, width // 2), jnp.float32),
    ]
    scratch = [
        pltpu.VMEM((2 * rows, key_count), jnp.float32),
        pltpu.VMEM((2 * rows, key_count), jnp.bfloat16),
    ]
    sums = [jax.ShapeDtypeStruct((HDIM, key_count), jnp.float32)] * 2
    if last:
        args += list(carried)
        in_specs += [whole(*a.shape) for a in carried]
        out_shape += [
            jax.ShapeDtypeStruct((prompt_blocks, 2, HDIM, rows), jnp.bfloat16),
            jax.ShapeDtypeStruct((2, HDIM, rows), jnp.float32),
        ]
        scratch += [pltpu.VMEM(s.shape, s.dtype) for s in sums]
    else:
        out_shape += sums
    out_specs += [result(*o.shape) for o in out_shape[2:]]
    inputs, outputs = len(args), len(out_shape)
    plan = None
    comm_ins, comm_outs = 0, 0
    if comm is not None:
        plan, more_args, more_out_specs, more_out_shape, more_scratch = comm
        comm_ins, comm_outs = len(more_args), len(more_out_shape)
        args += list(more_args)
        in_specs += [pl.BlockSpec(memory_space=pl.ANY)] * comm_ins
        out_specs += more_out_specs
        out_shape += more_out_shape
        scratch += more_scratch
    return pl.pallas_call(
        partial(attention_kernel, last, plan, (inputs, outputs, comm_ins, comm_outs)),
        grid=(steps,),
        in_specs=in_specs,
        out_specs=out_specs,
        out_shape=out_shape,
        scratch_shapes=scratch,
        compiler_params=pltpu.CompilerParams(
            dimension_semantics=("arbitrary",),
            vmem_limit_bytes=63 << 20,
            collective_id=collective_id,
            has_side_effects=comm is not None,
        ),
        cost_estimate=pl.CostEstimate(
            flops=6 * rows * width * key_count,
            bytes_accessed=8 * rows * width + 16 * key_count * pair,
            transcendentals=rows * HEADS * key_count // 2,
        ),
        name="attention_with_reduce" if last else "attention_with_gather",
    )(*args)


def gather_beside(shards, orders):
    n = len(shards)
    arrays = range(n)

    def plan(ins, outs, scratch):
        place = chip_place()
        gather = Gather(place, orders, ins, outs, *scratch)

        def begin():
            greet(place)
            gather.begin(arrays)

        return {
            (0, 0): begin,
            (0, 2): lambda: gather.pass_on(arrays, Z_SLABS[:1]),
            (1, 0): lambda: gather.pass_on(arrays, Z_SLABS[1:]),
            (1, 1): lambda: gather.pass_on(arrays, P_SLABS[:2]),
            (1, 2): lambda: gather.pass_on(arrays, P_SLABS[2:]),
            (2, 0): lambda: gather.pass_on(arrays, Q_SLABS[:4]),
            (2, 2): lambda: gather.pass_on(arrays, Q_SLABS[4:]),
            (2, 3): lambda: gather.finish(arrays),
        }

    out_shape = [jax.ShapeDtypeStruct((SLABS,) + s.shape, s.dtype) for s in shards]
    out_specs = [pl.BlockSpec(memory_space=pl.ANY)] * n
    scratch = [
        pltpu.SemaphoreType.DMA((n, 32)),
        pltpu.SemaphoreType.DMA((n, 32)),
        pltpu.SemaphoreType.DMA((n,)),
    ]
    return plan, shards, out_specs, out_shape, scratch


def reduce_beside(terms, orders):
    n = len(terms)
    arrays = range(n)

    def plan(ins, outs, scratch):
        place = chip_place()
        reduce = Reduce(place, orders, ins, outs, scratch[:n], scratch[n : 2 * n], *scratch[2 * n :])

        def begin():
            greet(place)
            reduce.begin(arrays, SUM_SLABS)

        def end():
            reduce.steps(arrays, SUM_SLABS[15:])
            reduce.finish()

        return {
            (0, 0): begin,
            (0, 2): lambda: reduce.steps(arrays, SUM_SLABS[:4]),
            (1, 0): lambda: reduce.steps(arrays, SUM_SLABS[4:8]),
            (1, 2): lambda: reduce.steps(arrays, SUM_SLABS[8:10]),
            (2, 0): lambda: reduce.steps(arrays, SUM_SLABS[10:12]),
            (2, 2): lambda: reduce.steps(arrays, SUM_SLABS[12:15]),
            (2, 3): end,
        }

    slabs = [t.shape[1:] for t in terms]
    out_shape = [jax.ShapeDtypeStruct(s, jnp.float32) for s in slabs]
    out_specs = [pl.BlockSpec(s, lambda i: (0, 0)) for s in slabs]
    scratch = (
        [pltpu.VMEM((16,) + s, jnp.bfloat16) for s in slabs]
        + [pltpu.VMEM((31,) + s, jnp.bfloat16) for s in slabs]
        + [
            pltpu.SemaphoreType.DMA((n, 31)),
            pltpu.SemaphoreType.DMA((n, 31)),
            pltpu.SemaphoreType.DMA((n, 16)),
        ]
    )
    return plan, terms, out_specs, out_shape, scratch


def attention_tables(keys_values, limit, rows):
    key_count = keys_values.shape[0]
    keys = keys_values[:, :HDIM]
    values = keys_values[:, HDIM:]
    k2 = jnp.concatenate([keys, keys], axis=1)
    v2 = jnp.concatenate([values, values], axis=1)
    column = jnp.arange(key_count, dtype=jnp.int32)
    shown = jnp.logical_or(column < limit, column >= key_count - rows)
    bias = jnp.broadcast_to(jnp.where(shown, 0.0, NEGATIVE)[None], (8, key_count))
    return k2, k2.T, v2, v2.T, bias


def pack_small(flat, rows_above, columns):
    shards, count = flat.shape
    rows = -(-count // columns)
    rows += -(rows_above + rows) % 8
    flat = jnp.pad(flat, ((0, 0), (0, rows * columns - count)))
    return flat.reshape(shards, rows, columns)


def unpack_small(packed, sizes):
    shards = packed.shape[0]
    flat = packed.reshape(shards, -1)
    parts = []
    start = 0
    for size in sizes:
        parts.append(flat[:, start : start + size].reshape(shards * size))
        start += size
    return parts


def per_device(
    direct,
    tokens,
    branch_points,
    qkv_weight,
    out_weight,
    up_weight,
    down_weight,
    query_bias,
    out_bias,
    up_bias,
    down_bias,
    first_gain,
    first_shift,
    second_gain,
    second_shift,
    cotangent,
):
    row_count = tokens.shape[1]
    width = tokens.shape[2]
    shards = lax.axis_size("grp") * lax.axis_size("tok")
    small = [
        query_bias,
        out_bias,
        up_bias,
        down_bias,
        first_gain,
        first_shift,
        second_gain,
        second_shift,
    ]
    sizes = [s.shape[0] for s in small]
    qkv_rows, columns = qkv_weight.shape
    packed = pack_small(jnp.concatenate(small)[None], qkv_rows, columns)[0]
    head = jnp.concatenate([qkv_weight, packed], axis=0)

    def all_of(*shards):
        return [lax.all_gather(w, AXES, axis=0, tiled=False) for w in shards]

    def joined(gathered):
        return gathered.reshape(-1, gathered.shape[2])

    if direct:
        head_all, out_full = gather_shards((head, out_weight), ROUTES, 0, "gather")
    else:
        head_all, out_full = all_of(head, out_weight)
    out_full = joined(out_full)
    qkv_full = joined(head_all[:, :qkv_rows])
    (
        query_full,
        out_bias_full,
        up_bias_full,
        down_bias_full,
        gain_one,
        shift_one,
        gain_two,
        shift_two,
    ) = [p.astype(jnp.float32) for p in unpack_small(head_all[:, qkv_rows:], sizes)]
    block_index = lax.axis_index("tok")
    is_cont = block_index >= PDEV
    offsets = jnp.arange(row_count, dtype=jnp.int32)
    limit = jnp.where(is_cont, branch_points[0, 0], block_index * row_count)
    positions = (limit + offsets).astype(jnp.float32)
    tables = turn_tables(positions, 2 * HDIM)
    inputs = tokens[0].astype(jnp.float32)
    first_norm, first_back = jax.vjp(layer_norm, inputs, gain_one, shift_one)
    second_norm, second_back = jax.vjp(layer_norm, inputs, gain_two, shift_two)
    first_low = first_norm.astype(jnp.bfloat16)
    second_low = second_norm.astype(jnp.bfloat16)
    projected = jnp.dot(first_low, qkv_full, preferred_element_type=jnp.float32)
    queries = turn(projected[:, :width] + query_full, tables, 1.0).astype(jnp.bfloat16)
    queries = queries * jnp.asarray(SCORE_SCALE, jnp.bfloat16)
    key_lane = jnp.arange(2 * HDIM, dtype=jnp.int32) < HDIM
    key_tables = (
        jnp.where(key_lane, tables[0], 1.0),
        jnp.where(key_lane, tables[1], 0.0),
        jnp.where(key_lane, tables[2], 0.0),
    )
    key_value = turn(projected[:, width:], key_tables, 1.0).astype(jnp.bfloat16)
    prompt_len = PDEV * row_count
    if direct:
        prompt_kv = gather_kv(key_value, 1).reshape(prompt_len, 2 * HDIM)
    else:
        prompt_kv = lax.all_gather(key_value, "tok", axis=0, tiled=True)[:prompt_len]
    keys_values = jnp.concatenate([prompt_kv, key_value], axis=0)

    grad_rows = cotangent[0]
    grad_float = grad_rows.astype(jnp.float32)
    contract_last = (((1,), (1,)), ((), ()))
    contract_first = (((0,), (0,)), ((), ()))
    matmul = partial(lax.dot_general, preferred_element_type=jnp.float32)
    d_context = matmul(grad_rows, out_full, contract_last)
    tables_kv = attention_tables(keys_values, limit, row_count)
    comm = gather_beside((up_weight, down_weight), ROUTES) if direct else None
    context_a, d_query_a, d_keys, d_values, *gathered = attention(
        0, queries, d_context, tables_kv, comm=comm, collective_id=2 if direct else None
    )
    up_full, down_full = map(joined, gathered if direct else all_of(up_weight, down_weight))

    pre_act = matmul(second_low, up_full, (((1,), (0,)), ((), ()))) + up_bias_full
    hidden, gelu_back = jax.vjp(partial(jax.nn.gelu, approximate=False), pre_act)
    hidden_low = hidden.astype(jnp.bfloat16)
    d_hidden = matmul(grad_rows, down_full, contract_last)
    d_pre_low = gelu_back(d_hidden)[0].astype(jnp.bfloat16)
    grad_up_w = matmul(second_low, d_pre_low, contract_first)
    grad_down_w = matmul(hidden_low, grad_rows, contract_first)

    def by_shard(term):
        return term.astype(jnp.bfloat16).reshape(shards, -1, term.shape[1])

    def sum_of(*terms):
        return [
            lax.psum_scatter(t, AXES, scatter_dimension=0, tiled=False).astype(jnp.float32)
            for t in terms
        ]

    wide_terms = (by_shard(grad_up_w), by_shard(grad_down_w))
    comm = reduce_beside(wide_terms, ROUTES) if direct else None
    context_b, d_query_b, sent, own_term, *summed = attention(
        1,
        queries,
        d_context,
        tables_kv,
        carried=(d_keys, d_values),
        comm=comm,
        collective_id=3 if direct else None,
    )
    sum_up_w, sum_down_w = summed if direct else sum_of(*wide_terms)
    context_low = jnp.concatenate([context_a, context_b], axis=1)
    d_query = jnp.concatenate([d_query_a, d_query_b], axis=1)
    if direct:
        summed = reduce_kv(sent, 4)
    else:
        idle = lax.axis_size("tok") - PDEV
        sent = jnp.pad(sent, ((0, idle), (0, 0), (0, 0), (0, 0)))
        summed = lax.psum_scatter(sent, "tok", scatter_dimension=0, tiled=False)
        summed = summed.astype(jnp.float32)
    kv_grad = (own_term + summed).reshape(2 * HDIM, row_count).T

    result = (
        inputs
        + jnp.dot(context_low, out_full, preferred_element_type=jnp.float32)
        + out_bias_full
    )
    result = (
        result
        + jnp.dot(hidden_low, down_full, preferred_element_type=jnp.float32)
        + down_bias_full
    )
    layer_out = result.astype(jnp.bfloat16)[None]
    d_query_back = turn(d_query, tables, -1.0)
    d_kv_back = turn(kv_grad, key_tables, -1.0)
    d_projected = jnp.concatenate([d_query_back, d_kv_back], axis=1).astype(jnp.bfloat16)
    grad_out_w = matmul(context_low, grad_rows, contract_first)
    grad_qkv_w = matmul(first_low, d_projected, contract_first)
    grad_query_b = jnp.sum(d_projected[:, :width].astype(jnp.float32), axis=0)
    grad_out_b = jnp.sum(grad_float, axis=0)
    grad_up_b = jnp.sum(d_pre_low.astype(jnp.float32), axis=0)
    d_first = matmul(d_projected, qkv_full, contract_last)
    d_second = matmul(d_pre_low, up_full, contract_last)
    input_one, grad_gain_one, grad_shift_one = first_back(d_first)
    input_two, grad_gain_two, grad_shift_two = second_back(d_second)
    input_grad = (grad_float + input_one + input_two)[None]

    small_grads = [
        grad_query_b,
        grad_out_b,
        grad_up_b,
        grad_gain_one,
        grad_shift_one,
        grad_gain_two,
        grad_shift_two,
    ]
    grad_sizes = [g.shape[0] // shards for g in small_grads]
    small_flat = jnp.concatenate([g.reshape(shards, -1) for g in small_grads], axis=1)
    small_flat = pack_small(small_flat, qkv_rows, columns)

    tail = jnp.concatenate([by_shard(grad_qkv_w), small_flat.astype(jnp.bfloat16)], axis=1)
    terms = (tail, by_shard(grad_out_w))
    if direct:
        sum_tail, sum_out_w = reduce_shards(terms, ROUTES, 5, "reduce")
    else:
        sum_tail, sum_out_w = sum_of(*terms)
    sum_qkv_w = sum_tail[:qkv_rows]
    (
        sum_query_b,
        sum_out_b,
        sum_up_b,
        sum_gain_one,
        sum_shift_one,
        sum_gain_two,
        sum_shift_two,
    ) = unpack_small(sum_tail[None, qkv_rows:], grad_sizes)
    return (
        layer_out,
        key_value[None],
        input_grad,
        sum_qkv_w,
        sum_out_w,
        sum_up_w,
        sum_down_w,
        sum_query_b,
        sum_out_b,
        sum_up_b,
        sum_out_b,
        sum_gain_one,
        sum_shift_one,
        sum_gain_two,
        sum_shift_two,
    )


def solution(mesh):
    direct = dict(mesh.shape) == {"grp": 2, "tok": 4 * Z_CHIPS}
    placed = (
        P("grp", "tok", None),
        P("grp", "tok"),
        P(("grp", "tok"), None),
        P(("grp", "tok"), None),
        P(("grp", "tok"), None),
        P(("grp", "tok"), None),
        P(("grp", "tok")),
        P(("grp", "tok")),
        P(("grp", "tok")),
        P(("grp", "tok")),
        P(("grp", "tok")),
        P(("grp", "tok")),
        P(("grp", "tok")),
        P(("grp", "tok")),
        P("grp", "tok", None),
    )
    return jax.shard_map(
        partial(per_device, direct),
        mesh=mesh,
        in_specs=placed,
        out_specs=(
            P("grp", "tok", None),
            P("grp", "tok", None),
            P("grp", "tok", None),
            P(("grp", "tok"), None),
            P(("grp", "tok"), None),
            P(("grp", "tok"), None),
            P(("grp", "tok"), None),
            P(("grp", "tok")),
            P(("grp", "tok")),
            P(("grp", "tok")),
            P(("grp", "tok")),
            P(("grp", "tok")),
            P(("grp", "tok")),
            P(("grp", "tok")),
            P(("grp", "tok")),
        ),
        check_vma=False,
    )
```

```python
from functools import partial

import jax
import jax.numpy as jnp
from jax import lax
from jax.experimental import pallas as pl
from jax.experimental.pallas import tpu as pltpu
from jax.sharding import PartitionSpec as P

HEADS = 12
HDIM = 64
ROT = 16
PDEV = 8
SCORE_SCALE = 0.125
NEGATIVE = -1e30
AXES = ("grp", "tok")
CHUNK = 512


def layer_norm(values, gain, shift):
    centered = values - jnp.mean(values, axis=-1, keepdims=True)
    variance = jnp.mean(centered * centered, axis=-1, keepdims=True)
    return centered * lax.rsqrt(variance + 1e-05) * gain + shift


def turn_tables(positions, width):
    half = ROT // 2
    lane = jnp.arange(width, dtype=jnp.int32) % HDIM
    frequency = 10000.0 ** (-((lane % half).astype(jnp.float32) * 2.0) / ROT)
    short = frequency[:half]
    angles = positions[:, None] * short[None, :]
    reps = width // half
    cosine = jnp.tile(jnp.cos(angles), (1, reps))
    sine = jnp.tile(jnp.sin(angles), (1, reps))
    own = jnp.where(lane < ROT, cosine, 1.0)
    from_right = jnp.where(lane < half, -sine, 0.0)
    from_left = jnp.where(jnp.logical_and(lane >= half, lane < ROT), sine, 0.0)
    return own, from_right, from_left


def lane_tables(positions, width):
    half = ROT // 2
    lane = jnp.arange(width, dtype=jnp.int32) % HDIM
    frequency = 10000.0 ** (-((lane % half).astype(jnp.float32) * 2.0) / ROT)
    angles = positions[:, None] * frequency[None, :]
    cosine, sine = jnp.cos(angles), jnp.sin(angles)
    own = jnp.where(lane < ROT, cosine, 1.0)
    from_right = jnp.where(lane < half, -sine, 0.0)
    from_left = jnp.where(jnp.logical_and(lane >= half, lane < ROT), sine, 0.0)
    return own, from_right, from_left


def turn(values, tables, sign):
    own, from_right, from_left = tables
    reps = values.shape[1] // own.shape[1]
    half = ROT // 2
    own, from_right, from_left = (jnp.tile(t, (1, reps)) for t in tables)
    return (
        values * own
        + sign * (jnp.roll(values, -half, axis=1) * from_right)
        + sign * (jnp.roll(values, half, axis=1) * from_left)
    )


MESH = pl.DeviceIdType.MESH
Z_CHIPS = 4
ROUTES = ("yx", "xy")
SLABS = 32


def chip_place():
    tok = lax.axis_index("tok")
    return tok // 4, (tok // 2) % 2, tok % 2, lax.axis_index("grp")


def near(place, k=0, fy=0, fx=0, fg=0):
    z, y, x, g = place
    zz = (z, z + 1 - 2 * (z % 2), (z + 2) % Z_CHIPS, Z_CHIPS - 1 - z)[k]
    return zz, (1 - y if fy else y), (1 - x if fx else x), (1 - g if fg else g)


def device_at(coords):
    z, y, x, g = coords
    return {"tok": z * 4 + y * 2 + x, "grp": g}


def slot_at(coords):
    z, y, x, g = coords
    return g * 16 + z * 4 + y * 2 + x


def near_pq(place, order, k=0, fp=0, fq=0, fg=0):
    if order == "yx":
        return near(place, k, fp, fq, fg)
    return near(place, k, fq, fp, fg)


def greet(place):
    barrier = pltpu.get_barrier_semaphore()
    peers = [near(place, k=1), near(place, k=2), near(place, k=3)]
    peers += [near(place, fy=1), near(place, fx=1), near(place, fg=1)]
    for peer in peers:
        pl.semaphore_signal(barrier, inc=1, device_id=device_at(peer), device_id_type=MESH)
    pl.semaphore_wait(barrier, len(peers))


def remote(src, dst, send_sem, recv_sem, coords):
    return pltpu.make_async_remote_copy(
        src_ref=src,
        dst_ref=dst,
        send_sem=send_sem,
        recv_sem=recv_sem,
        device_id=device_at(coords),
        device_id_type=MESH,
    )


class Gather:
    def __init__(self, place, orders, ins, outs, send, recv, local):
        self.place, self.orders, self.ins, self.outs = place, orders, ins, outs
        self.send, self.recv, self.local = send, recv, local
        self.started = []

    def push(self, a, slab, index, target):
        def build():
            place, order = self.place, self.orders[a]
            slot = slot_at(near_pq(place, order, *slab))
            dst = self.outs[a].at[slot]
            src = self.ins[a] if slab == (0, 0, 0) else dst
            return remote(src, dst, self.send.at[a, index], self.recv.at[a, index], target())

        build().start()
        self.started.append(build)

    def spread(self, a, k, fp, fq):
        place, order, slab = self.place, self.orders[a], (k, fp, fq)
        if slab == (0, 0, 0):
            for j in (1, 2, 3):
                self.push(a, slab, j * 4, partial(near, place, k=j))
        if fp == 0 and fq == 0:
            self.push(a, slab, k * 4 + 2, partial(near_pq, place, order, fp=1))
        if fq == 0:
            self.push(a, slab, k * 4 + fp * 2 + 1, partial(near_pq, place, order, fq=1))
        self.push(a, slab, 16 + k * 4 + fp * 2 + fq, partial(near, place, fg=1))

    def arrived(self, a, k, fp, fq, fg=0):
        slot = slot_at(near_pq(self.place, self.orders[a], k, fp, fq, fg))
        index = 16 * fg + k * 4 + fp * 2 + fq
        block = self.outs[a].at[slot]
        remote(
            block, block, self.send.at[a, index], self.recv.at[a, index], near(self.place, fg=1)
        ).wait_recv()

    def own_copy(self, a):
        slot = slot_at(self.place)
        return pltpu.make_async_copy(self.ins[a], self.outs[a].at[slot], self.local.at[a])

    def begin(self, arrays):
        for a in arrays:
            self.spread(a, 0, 0, 0)
            self.own_copy(a).start()

    def pass_on(self, arrays, slabs):
        for slab in slabs:
            for a in arrays:
                self.arrived(a, *slab)
                self.spread(a, *slab)

    def finish(self, arrays):
        for a in arrays:
            self.own_copy(a).wait()
            for k in range(4):
                for fp in range(2):
                    for fq in range(2):
                        self.arrived(a, k, fp, fq, 1)
        for build in self.started:
            build().wait_send()


Z_SLABS = [(1, 0, 0), (2, 0, 0), (3, 0, 0)]
P_SLABS = [(k, 1, 0) for k in range(4)]
Q_SLABS = [(k, fp, 1) for fp in range(2) for k in range(4)]


def gather_kernel(orders, *refs):
    n = len(orders)
    ins, outs = refs[:n], refs[n : 2 * n]
    send, recv, local = refs[2 * n :]
    place = chip_place()
    greet(place)
    gather = Gather(place, orders, ins, outs, send, recv, local)
    arrays = range(n)
    gather.begin(arrays)
    gather.pass_on(arrays, Z_SLABS + P_SLABS + Q_SLABS)
    gather.finish(arrays)


def gather_shards(shards, orders, collective_id, name):
    n = len(shards)
    return pl.pallas_call(
        partial(gather_kernel, orders),
        in_specs=[pl.BlockSpec(memory_space=pl.ANY)] * n,
        out_specs=[pl.BlockSpec(memory_space=pl.ANY)] * n,
        out_shape=[jax.ShapeDtypeStruct((SLABS,) + s.shape, s.dtype) for s in shards],
        scratch_shapes=[
            pltpu.SemaphoreType.DMA((n, 32)),
            pltpu.SemaphoreType.DMA((n, 32)),
            pltpu.SemaphoreType.DMA((n,)),
        ],
        compiler_params=pltpu.CompilerParams(collective_id=collective_id, has_side_effects=True),
        name=name,
    )(*shards)


class Reduce:
    def __init__(self, place, orders, ins, outs, accs, boxes, send, recv, local):
        self.place, self.orders, self.ins, self.outs = place, orders, ins, outs
        self.accs, self.boxes = accs, boxes
        self.send, self.recv, self.local = send, recv, local
        self.started = []

    def mail(self, a, src, index, target):
        def build():
            box = self.boxes[a].at[index]
            return remote(src(), box, self.send.at[a, index], self.recv.at[a, index], target())

        build().start()
        self.started.append(build)

    def far_term(self, a, slab):
        return self.ins[a].at[slot_at(near_pq(self.place, self.orders[a], *slab, 1))]

    def load(self, a, k, fp, fq):
        slot = slot_at(near_pq(self.place, self.orders[a], k, fp, fq))
        sid = k * 4 + fp * 2 + fq
        return pltpu.make_async_copy(
            self.ins[a].at[slot], self.accs[a].at[sid], self.local.at[a, sid]
        )

    def begin(self, arrays, slabs):
        for k, fp, fq in slabs:
            for a in arrays:
                sid = k * 4 + fp * 2 + fq
                src = partial(self.far_term, a, (k, fp, fq))
                self.mail(a, src, sid, partial(near, self.place, fg=1))
                if self.local is not None:
                    self.load(a, k, fp, fq).start()

    def arrived(self, a, index):
        box = self.boxes[a].at[index]
        remote(
            box, box, self.send.at[a, index], self.recv.at[a, index], near(self.place, fg=1)
        ).wait_recv()
        return box[...].astype(jnp.float32)

    def step(self, a, k, fp, fq):
        sid = k * 4 + fp * 2 + fq
        place, order = self.place, self.orders[a]
        if self.local is not None:
            self.load(a, k, fp, fq).wait()
            total = self.accs[a][sid].astype(jnp.float32)
        else:
            total = self.ins[a][slot_at(near_pq(place, order, k, fp, fq))].astype(jnp.float32)
        total = total + self.arrived(a, sid)
        if fq == 0:
            total = total + self.arrived(a, 16 + k * 2 + fp)
        if fq == 0 and fp == 0:
            total = total + self.arrived(a, 24 + k)
        if (k, fp, fq) == (0, 0, 0):
            for j in (1, 2, 3):
                total = total + self.arrived(a, 27 + j)
            self.outs[a][...] = total
            return
        self.accs[a][sid] = total.astype(jnp.bfloat16)

        def src():
            return self.accs[a].at[sid]

        if fq == 1:
            self.mail(a, src, 16 + k * 2 + fp, partial(near_pq, place, order, fq=1))
        elif fp == 1:
            self.mail(a, src, 24 + k, partial(near_pq, place, order, fp=1))
        else:
            self.mail(a, src, 27 + k, partial(near, place, k=k))

    def steps(self, arrays, slabs):
        for slab in slabs:
            for a in arrays:
                self.step(a, *slab)

    def finish(self):
        for build in self.started:
            build().wait_send()


SUM_SLABS = (
    [(k, 1, 1) for k in (3, 2, 1, 0)]
    + [(k, 0, 1) for k in (3, 2, 1, 0)]
    + [(k, 1, 0) for k in (3, 2, 1, 0)]
    + [(k, 0, 0) for k in (3, 2, 1, 0)]
)


def kv_route(place, half, fp=0, fq=0):
    if half == 0:
        return near(place, fy=fp, fx=fq)
    return near(place, fy=fq, fx=fp)


def kv_slot(coords, plane):
    return plane * 4 + coords[1] * 2 + coords[2]


def attention_kernel(last, plan, counts, *refs):
    inputs, outputs, comm_ins, comm_outs = counts
    q_ref, dc_ref, kv_ref, kvt_ref, bias_ref = refs[:5]
    carried = refs[5:inputs]
    cut = inputs + comm_ins
    ctx_ref, dq_ref = refs[cut : cut + 2]
    results = refs[cut + 2 : cut + outputs]
    scratch = refs[cut + outputs + comm_outs :]
    s_ref, e_ref = scratch[:2]
    if last:
        dkt_ref, dvt_ref = scratch[2:4]
        comm_scratch = scratch[4:]
    else:
        dkt_ref, dvt_ref = results
        comm_scratch = scratch[2:]
    rows = q_ref.shape[0]
    key_count = kv_ref.shape[0]
    pair = 2 * HDIM
    prompt = key_count - rows
    unroll = 4
    step = pl.program_id(0)
    events = {}
    if plan is not None:
        events = plan(refs[inputs:cut], refs[cut + outputs : cut + outputs + comm_outs], comm_scratch)

    def point(index):
        for at_step, at_point in sorted(events):
            if at_point == index:
                pl.when(step == at_step)(events[at_step, at_point])

    @pl.when(step == 0)
    def _():
        if carried:
            dkt_ref[...] = carried[0][...]
            dvt_ref[...] = carried[1][...]
        else:
            dkt_ref[...] = jnp.zeros_like(dkt_ref)
            dvt_ref[...] = jnp.zeros_like(dvt_ref)

    point(0)
    first_head = lax.broadcasted_iota(jnp.int32, (rows, pair), 1) < HDIM

    def stacked(both, on_values):
        swapped = pltpu.roll(both, HDIM, 1)
        if on_values:
            parts = [jnp.where(first_head, 0.0, swapped), jnp.where(first_head, 0.0, both)]
        else:
            parts = [jnp.where(first_head, both, 0.0), jnp.where(first_head, swapped, 0.0)]
        return jnp.concatenate(parts, axis=0).astype(jnp.bfloat16)

    def turned(both):
        flipped = both.T.astype(jnp.bfloat16)
        return jnp.concatenate([flipped[:HDIM], flipped[HDIM:]], axis=1)

    q_both = q_ref[...].astype(jnp.float32)
    q_rows = stacked(q_both, False)
    q_cols = turned(q_both)

    def lane_max(top, scores):
        for j in range(scores.shape[1] // pair):
            top = jnp.maximum(top, scores[:, j * pair : (j + 1) * pair])
        return top

    def score_step(c, top):
        cols = pl.ds(pl.multiple_of(c * CHUNK, CHUNK), CHUNK)
        scores = jnp.dot(q_rows, kvt_ref[:, cols], preferred_element_type=jnp.float32)
        scores = scores + bias_ref[0:1, cols]
        s_ref[:, cols] = scores
        return lane_max(top, scores)

    top = lax.fori_loop(
        0,
        prompt // CHUNK,
        score_step,
        jnp.full((2 * rows, pair), NEGATIVE, jnp.float32),
        unroll=unroll,
    )
    row_id = lax.broadcasted_iota(jnp.int32, (2 * rows, rows), 0) % rows
    col_id = lax.broadcasted_iota(jnp.int32, (2 * rows, rows), 1)
    scores = jnp.dot(q_rows, kvt_ref[:, prompt:], preferred_element_type=jnp.float32)
    scores = jnp.where(col_id <= row_id, scores, NEGATIVE)
    s_ref[:, prompt:] = scores
    top = jnp.max(lane_max(top, scores), axis=1, keepdims=True)
    point(1)

    def weight_step(c, carry):
        total, mixed = carry
        cols = pl.ds(pl.multiple_of(c * CHUNK, CHUNK), CHUNK)
        weights = jnp.exp(s_ref[:, cols] - top)
        for j in range(CHUNK // pair):
            total = total + weights[:, j * pair : (j + 1) * pair]
        low = weights.astype(jnp.bfloat16)
        e_ref[:, cols] = low
        mixed = mixed + jnp.dot(low, kv_ref[cols, :], preferred_element_type=jnp.float32)
        return total, mixed

    zero = jnp.zeros((2 * rows, pair), jnp.float32)
    total, mixed = lax.fori_loop(
        0, key_count // CHUNK, weight_step, (zero, zero), unroll=unroll
    )
    point(2)
    scale = 1.0 / jnp.sum(total, axis=1, keepdims=True)
    mixed = mixed * scale
    context = jnp.where(first_head, pltpu.roll(mixed[:rows], HDIM, 1), mixed[rows:])
    ctx_ref[...] = context.astype(ctx_ref.dtype)
    d_context = dc_ref[...]
    product = d_context * context
    delta_a = jnp.sum(jnp.where(first_head, product, 0.0), axis=1, keepdims=True)
    delta_b = jnp.sum(jnp.where(first_head, 0.0, product), axis=1, keepdims=True)
    delta = jnp.concatenate([delta_a, delta_b], axis=0) * scale
    d_both = d_context * jnp.where(first_head, scale[:rows], scale[rows:])
    d_rows = stacked(d_both, True)
    d_cols = turned(d_both)

    def grad_step(c, d_query):
        cols = pl.ds(pl.multiple_of(c * CHUNK, CHUNK), CHUNK)
        d_probs = jnp.dot(d_rows, kvt_ref[:, cols], preferred_element_type=jnp.float32)
        low = e_ref[:, cols]
        d_scores = (low.astype(jnp.float32) * (d_probs - delta)).astype(jnp.bfloat16)
        dvt_ref[:, cols] += jnp.dot(d_cols, low, preferred_element_type=jnp.float32)
        dkt_ref[:, cols] += jnp.dot(q_cols, d_scores, preferred_element_type=jnp.float32)
        return d_query + jnp.dot(d_scores, kv_ref[cols, :], preferred_element_type=jnp.float32)

    d_query = lax.fori_loop(0, key_count // CHUNK, grad_step, zero, unroll=unroll)
    second = pltpu.roll(d_query[rows:], HDIM, 1)
    dq_ref[...] = jnp.where(first_head, d_query[:rows], second) * SCORE_SCALE
    point(3)
    if last:

        @pl.when(step == pl.num_programs(0) - 1)
        def _():
            sent_ref, own_ref = results
            for part, total_ref in enumerate((dkt_ref, dvt_ref)):
                for block in range(prompt // rows):
                    cols = slice(block * rows, (block + 1) * rows)
                    sent_ref[block, part] = total_ref[:, cols].astype(sent_ref.dtype)
                own_ref[part] = total_ref[:, prompt:]


def attention(half, queries, d_context, tables, carried=None, comm=None, collective_id=None):
    keys_values, flipped, bias = tables
    key_count, pair = keys_values.shape
    rows, width = queries.shape
    steps = width // pair // 2
    last = half == 1
    prompt_blocks = key_count // rows - 1

    def whole(*shape):
        return pl.BlockSpec(
            shape, lambda i: (0,) * len(shape), pipeline_mode=pl.Buffered(1)
        )

    def result(*shape):
        return pl.BlockSpec(shape, lambda i: (0,) * len(shape))

    block_in = pl.BlockSpec((rows, pair), lambda i: (0, i + half * steps))
    block = pl.BlockSpec((rows, pair), lambda i: (0, i))
    args = [queries, d_context, keys_values, flipped, bias]
    in_specs = [block_in, block_in] + [whole(*a.shape) for a in args[2:]]
    out_specs = [block, block]
    out_shape = [
        jax.ShapeDtypeStruct((rows, width // 2), jnp.bfloat16),
        jax.ShapeDtypeStruct((rows, width // 2), jnp.float32),
    ]
    scratch = [
        pltpu.VMEM((2 * rows, key_count), jnp.float32),
        pltpu.VMEM((2 * rows, key_count), jnp.bfloat16),
    ]
    sums = [jax.ShapeDtypeStruct((HDIM, key_count), jnp.float32)] * 2
    if last:
        args += list(carried)
        in_specs += [whole(*a.shape) for a in carried]
        out_shape += [
            jax.ShapeDtypeStruct((prompt_blocks, 2, HDIM, rows), jnp.bfloat16),
            jax.ShapeDtypeStruct((2, HDIM, rows), jnp.float32),
        ]
        scratch += [pltpu.VMEM(s.shape, s.dtype) for s in sums]
    else:
        out_shape += sums
    out_specs += [result(*o.shape) for o in out_shape[2:]]
    inputs, outputs = len(args), len(out_shape)
    plan = None
    comm_ins, comm_outs = 0, 0
    if comm is not None:
        plan, more_args, more_out_specs, more_out_shape, more_scratch = comm
        comm_ins, comm_outs = len(more_args), len(more_out_shape)
        args += list(more_args)
        in_specs += [pl.BlockSpec(memory_space=pl.ANY)] * comm_ins
        out_specs += more_out_specs
        out_shape += more_out_shape
        scratch += more_scratch
    return pl.pallas_call(
        partial(attention_kernel, last, plan, (inputs, outputs, comm_ins, comm_outs)),
        grid=(steps,),
        in_specs=in_specs,
        out_specs=out_specs,
        out_shape=out_shape,
        scratch_shapes=scratch,
        compiler_params=pltpu.CompilerParams(
            dimension_semantics=("arbitrary",),
            vmem_limit_bytes=63 << 20,
            collective_id=collective_id,
            has_side_effects=comm is not None,
        ),
        cost_estimate=pl.CostEstimate(
            flops=6 * rows * width * key_count,
            bytes_accessed=8 * rows * width + 16 * key_count * pair,
            transcendentals=rows * HEADS * key_count // 2,
        ),
        name="attention_with_reduce" if last else "attention_with_gather",
    )(*args)


def gather_beside(shards, orders):
    n = len(shards)
    arrays = range(n)

    def plan(ins, outs, scratch):
        place = chip_place()
        gather = Gather(place, orders, ins, outs, *scratch)

        def begin():
            greet(place)
            gather.begin(arrays)

        return {
            (0, 0): begin,
            (0, 2): lambda: gather.pass_on(arrays, Z_SLABS[:1]),
            (1, 0): lambda: gather.pass_on(arrays, Z_SLABS[1:]),
            (1, 1): lambda: gather.pass_on(arrays, P_SLABS[:2]),
            (1, 2): lambda: gather.pass_on(arrays, P_SLABS[2:]),
            (2, 0): lambda: gather.pass_on(arrays, Q_SLABS[:4]),
            (2, 2): lambda: gather.pass_on(arrays, Q_SLABS[4:]),
            (2, 3): lambda: gather.finish(arrays),
        }

    out_shape = [jax.ShapeDtypeStruct((SLABS,) + s.shape, s.dtype) for s in shards]
    out_specs = [pl.BlockSpec(memory_space=pl.ANY)] * n
    scratch = [
        pltpu.SemaphoreType.DMA((n, 32)),
        pltpu.SemaphoreType.DMA((n, 32)),
        pltpu.SemaphoreType.DMA((n,)),
    ]
    return plan, shards, out_specs, out_shape, scratch


def reduce_beside(terms, orders):
    n = len(terms)
    arrays = range(n)

    def plan(ins, outs, scratch):
        place = chip_place()
        reduce = Reduce(place, orders, ins, outs, scratch[:n], scratch[n : 2 * n], *scratch[2 * n :])

        def begin():
            greet(place)
            reduce.begin(arrays, SUM_SLABS)

        def end():
            reduce.steps(arrays, SUM_SLABS[15:])
            reduce.finish()

        return {
            (0, 0): begin,
            (0, 2): lambda: reduce.steps(arrays, SUM_SLABS[:4]),
            (1, 0): lambda: reduce.steps(arrays, SUM_SLABS[4:8]),
            (1, 2): lambda: reduce.steps(arrays, SUM_SLABS[8:10]),
            (2, 0): lambda: reduce.steps(arrays, SUM_SLABS[10:12]),
            (2, 2): lambda: reduce.steps(arrays, SUM_SLABS[12:15]),
            (2, 3): end,
        }

    slabs = [t.shape[1:] for t in terms]
    out_shape = [jax.ShapeDtypeStruct(s, jnp.float32) for s in slabs]
    out_specs = [pl.BlockSpec(s, lambda i: (0, 0)) for s in slabs]
    scratch = (
        [pltpu.VMEM((16,) + s, jnp.bfloat16) for s in slabs]
        + [pltpu.VMEM((31,) + s, jnp.bfloat16) for s in slabs]
        + [
            pltpu.SemaphoreType.DMA((n, 31)),
            pltpu.SemaphoreType.DMA((n, 31)),
            pltpu.SemaphoreType.DMA((n, 16)),
        ]
    )
    return plan, terms, out_specs, out_shape, scratch


def attention_tables(keys_values, limit, rows):
    key_count = keys_values.shape[0]
    column = jnp.arange(key_count, dtype=jnp.int32)
    shown = jnp.logical_or(column < limit, column >= key_count - rows)
    bias = jnp.broadcast_to(jnp.where(shown, 0.0, NEGATIVE)[None], (8, key_count))
    return keys_values, keys_values.T, bias


def tile_turn(values, own, from_right, from_left, sign):
    half = ROT // 2
    lanes = values.shape[1]
    ahead = pltpu.roll(values, lanes - half, 1)
    behind = pltpu.roll(values, half, 1)
    return values * own + sign * (ahead * from_right + behind * from_left)


def unit_rows(values):
    centered = values - jnp.mean(values, axis=-1, keepdims=True)
    variance = jnp.mean(centered * centered, axis=-1, keepdims=True)
    scale = lax.rsqrt(variance + 1e-05)
    return centered * scale, scale


NT = (((1,), (1,)), ((), ()))
TN = (((0,), (0,)), ((), ()))
dot_of = partial(lax.dot_general, preferred_element_type=jnp.float32)


class KvGather:
    def __init__(self, place, kv_ref, all_ref, send, recv):
        self.place, self.kv_ref, self.all_ref = place, kv_ref, all_ref
        self.send, self.recv = send, recv
        self.rows = kv_ref.shape[0] // 2
        self.started = []

    def at_z(self, zz):
        return (zz,) + self.place[1:]

    def block(self, slot, half=None):
        if half is None:
            return self.all_ref.at[slot]
        return self.all_ref.at[slot, pl.ds(half * self.rows, self.rows)]

    def wait(self, ref, index):
        remote(
            ref, ref, self.send.at[index], self.recv.at[index], near(self.place, fg=1)
        ).wait_recv()

    def own_push(self, index, zz):
        plane = self.place[0] % 2
        dst = self.block(kv_slot(self.place, plane))
        return remote(
            self.kv_ref, dst, self.send.at[index], self.recv.at[plane], self.at_z(zz)
        )

    def relay(self, plane):
        ref = self.block(kv_slot(self.place, plane))
        return remote(ref, ref, self.send.at[plane], self.recv.at[plane], self.at_z(3))

    def push(self, ref, index, coords):
        copy = remote(ref, ref, self.send.at[index], self.recv.at[index], coords)
        copy.start()
        self.started.append(copy)

    def begin(self):
        @pl.when(self.place[0] < 2)
        def _():
            self.own_push(0, 1 - self.place[0] % 2).start()
            self.own_push(1, 2).start()

    def planes(self):
        z = self.place[0]
        for plane in (1, 0):

            @pl.when(z != plane)
            def _():
                self.wait(self.block(kv_slot(self.place, plane)), plane)

            @pl.when(z == 2)
            def _():
                self.relay(plane).start()

            for half in range(2):
                ref = self.block(kv_slot(self.place, plane), half)
                self.push(ref, 2 + plane * 2 + half, kv_route(self.place, half, fp=1))
                self.push(ref, 6 + plane * 4 + half, kv_route(self.place, half, fq=1))

    def middle(self):
        for plane in (1, 0):
            for half in range(2):
                ref = self.block(kv_slot(kv_route(self.place, half, fp=1), plane), half)
                self.wait(ref, 2 + plane * 2 + half)
                self.push(ref, 6 + plane * 4 + 2 + half, kv_route(self.place, half, fq=1))

    def finish(self):
        for plane in (1, 0):
            for fp in range(2):
                for half in range(2):
                    slot = kv_slot(kv_route(self.place, half, fp, 1), plane)
                    self.wait(self.block(slot, half), 6 + plane * 4 + fp * 2 + half)
        for copy in self.started:
            copy.wait_send()
        z = self.place[0]

        @pl.when(z < 2)
        def _():
            self.own_push(0, 1 - z % 2).wait_send()
            self.own_push(1, 2).wait_send()

        @pl.when(z == 2)
        def _():
            self.relay(0).wait_send()
            self.relay(1).wait_send()


def project_kernel(
    x_ref,
    cot_ref,
    qkv_ref,
    out_ref,
    par_ref,
    own_ref,
    right_ref,
    left_ref,
    q_ref,
    kv_ref,
    all_ref,
    kvt_ref,
    dc_ref,
    first_ref,
    second_ref,
    send,
    recv,
):
    place = chip_place()
    greet(place)
    rows = kv_ref.shape[0]
    pair = 2 * HDIM
    width = q_ref.shape[1]
    unit, _ = unit_rows(x_ref[0].astype(jnp.float32))
    first = (unit * par_ref[3:4] + par_ref[4:5]).astype(jnp.bfloat16)
    first_ref[...] = first
    own, right, left = own_ref[...], right_ref[...], left_ref[...]
    is_key = lax.broadcasted_iota(jnp.int32, (rows, pair), 1) < HDIM
    raw = jnp.dot(first, qkv_ref[:, width:], preferred_element_type=jnp.float32)
    turned_kv = jnp.where(is_key, tile_turn(raw, own, right, left, 1.0), raw)
    kv = turned_kv.astype(jnp.bfloat16)
    kv_ref[...] = kv
    all_ref[PDEV] = kv

    @pl.when(place[0] < 2)
    def _():
        all_ref[kv_slot(place, place[0] % 2)] = kv_ref[...]

    second_ref[...] = (unit * par_ref[5:6] + par_ref[6:7]).astype(jnp.bfloat16)
    gather = KvGather(place, kv_ref, all_ref, send, recv)
    gather.begin()
    for tile in range(width // pair):
        cols = slice(tile * pair, (tile + 1) * pair)
        part = jnp.dot(first_ref[...], qkv_ref[:, cols], preferred_element_type=jnp.float32)
        part = tile_turn(part + par_ref[0:1, cols], own, right, left, 1.0)
        low = part.astype(jnp.bfloat16).astype(jnp.float32)
        q_ref[:, cols] = (low * SCORE_SCALE).astype(jnp.bfloat16)
    gather.planes()
    dc_ref[...] = dot_of(cot_ref[0], out_ref[...], NT)
    gather.middle()

    def turn_over(slot):
        flipped = all_ref[slot].astype(jnp.float32).T
        kvt_ref[:, slot * rows : (slot + 1) * rows] = flipped.astype(jnp.bfloat16)

    turn_over(PDEV)
    gather.finish()
    for slot in range(PDEV):
        turn_over(slot)


def vmem_spec():
    return pl.BlockSpec(memory_space=pltpu.VMEM)


def project(tokens, cotangent, qkv_full, out_full, params, tables, collective_id):
    rows, width = tokens.shape[1:]
    pair = 2 * HDIM
    keys = (PDEV + 1) * rows
    low = jnp.bfloat16
    return pl.pallas_call(
        project_kernel,
        in_specs=[vmem_spec()] * 8,
        out_specs=[vmem_spec()] * 7,
        out_shape=[
            jax.ShapeDtypeStruct((rows, width), low),
            jax.ShapeDtypeStruct((rows, pair), low),
            jax.ShapeDtypeStruct((PDEV + 1, rows, pair), low),
            jax.ShapeDtypeStruct((pair, keys), low),
            jax.ShapeDtypeStruct((rows, width), jnp.float32),
            jax.ShapeDtypeStruct((rows, width), low),
            jax.ShapeDtypeStruct((rows, width), low),
        ],
        scratch_shapes=[pltpu.SemaphoreType.DMA((14,)), pltpu.SemaphoreType.DMA((14,))],
        compiler_params=pltpu.CompilerParams(
            collective_id=collective_id, has_side_effects=True, vmem_limit_bytes=48 << 20
        ),
        name="project_with_gather",
    )(tokens, cotangent, qkv_full, out_full, params, *tables)


def mlp_kernel(
    second_ref, cot_ref, up_ref, bias_ref, down_ref, upg_ref, downg_ref, out_ref, dsec_ref, bg_ref
):
    step = pl.program_id(0)
    second = second_ref[...]
    cot = cot_ref[0]
    pre = jnp.dot(second, up_ref[...], preferred_element_type=jnp.float32) + bias_ref[...]
    below = 0.5 + 0.5 * lax.erf(pre * 0.7071067811865476)
    hidden = (pre * below).astype(jnp.bfloat16)
    slope = below + pre * (jnp.exp(pre * pre * -0.5) * 0.3989422804014327)
    d_pre = (dot_of(cot, down_ref[...], NT) * slope).astype(jnp.bfloat16)
    upg_ref[...] = dot_of(second, d_pre, TN).astype(jnp.bfloat16)
    downg_ref[...] = dot_of(hidden, cot, TN).astype(jnp.bfloat16)
    bg_ref[...] = jnp.sum(d_pre.astype(jnp.float32), axis=0, keepdims=True)
    out = jnp.dot(hidden, down_ref[...], preferred_element_type=jnp.float32)
    d_second = dot_of(d_pre, up_ref[...], NT)

    @pl.when(step == 0)
    def _():
        out_ref[...] = out
        dsec_ref[...] = d_second

    @pl.when(step > 0)
    def _():
        out_ref[...] += out
        dsec_ref[...] += d_second


def mlp(second_low, cotangent, up_full, up_bias, down_full):
    rows, width = second_low.shape
    inner = up_full.shape[1]
    tile = 512
    return pl.pallas_call(
        mlp_kernel,
        grid=(inner // tile,),
        in_specs=[
            pl.BlockSpec((rows, width), lambda i: (0, 0)),
            pl.BlockSpec((1, rows, width), lambda i: (0, 0, 0)),
            pl.BlockSpec((width, tile), lambda i: (0, i)),
            pl.BlockSpec((1, tile), lambda i: (0, i)),
            pl.BlockSpec((tile, width), lambda i: (i, 0)),
        ],
        out_specs=[
            pl.BlockSpec((width, tile), lambda i: (0, i)),
            pl.BlockSpec((tile, width), lambda i: (i, 0)),
            pl.BlockSpec((rows, width), lambda i: (0, 0)),
            pl.BlockSpec((rows, width), lambda i: (0, 0)),
            pl.BlockSpec((1, tile), lambda i: (0, i)),
        ],
        out_shape=[
            jax.ShapeDtypeStruct((width, inner), jnp.bfloat16),
            jax.ShapeDtypeStruct((inner, width), jnp.bfloat16),
            jax.ShapeDtypeStruct((rows, width), jnp.float32),
            jax.ShapeDtypeStruct((rows, width), jnp.float32),
            jax.ShapeDtypeStruct((1, inner), jnp.float32),
        ],
        compiler_params=pltpu.CompilerParams(
            dimension_semantics=("arbitrary",), vmem_limit_bytes=48 << 20
        ),
        name="mlp",
    )(second_low, cotangent, up_full, up_bias, down_full)


class KvReduce:
    order = [(plane, half) for plane in (0, 1) for half in (0, 1)]

    def __init__(self, place, in_ref, out_ref, acc, q_box, p_box, z_box, send, recv):
        self.place, self.in_ref, self.out_ref, self.acc = place, in_ref, out_ref, acc
        self.q_box, self.p_box, self.z_box = q_box, p_box, z_box
        self.send, self.recv = send, recv
        self.started = []

    def mail(self, src, dst, index, coords):
        copy = remote(src, dst, self.send.at[index], self.recv.at[index], coords)
        copy.start()
        self.started.append(copy)

    def arrived(self, box, index):
        remote(
            box, box, self.send.at[index], self.recv.at[index], near(self.place, fg=1)
        ).wait_recv()
        return box[...].astype(jnp.float32)

    def slot(self, plane, half, fp=0, fq=0):
        return kv_slot(kv_route(self.place, half, fp, fq), plane)

    def to_z(self, index, box, zz):
        return remote(
            self.acc.at[index],
            self.z_box.at[box],
            self.send.at[12 + index],
            self.recv.at[12 + box],
            (zz,) + self.place[1:],
        )

    def begin(self):
        for fp in (1, 0):
            for plane, half in self.order:
                index = plane * 4 + fp * 2 + half
                src = self.in_ref.at[self.slot(plane, half, fp, 1), half]
                self.mail(src, self.q_box.at[index], index, kv_route(self.place, half, fq=1))

    def middle(self):
        for plane, half in self.order:
            index = plane * 2 + half
            box = plane * 4 + 2 + half
            total = self.in_ref[self.slot(plane, half, 1, 0), half].astype(jnp.float32)
            total = total + self.arrived(self.q_box.at[box], box)
            self.acc[4 + index] = total.astype(self.acc.dtype)
            src = self.acc.at[4 + index]
            self.mail(src, self.p_box.at[index], 8 + index, kv_route(self.place, half, fp=1))

    def planes(self):
        z = self.place[0]
        for plane, half in self.order:
            index = plane * 2 + half
            box = plane * 4 + half
            total = self.in_ref[self.slot(plane, half), half].astype(jnp.float32)
            total = total + self.arrived(self.q_box.at[box], box)
            total = total + self.arrived(self.p_box.at[index], 8 + index)

            @pl.when(z == 2)
            def _():
                passed = total + self.arrived(self.z_box.at[index], 12 + index)
                self.acc[index] = passed.astype(self.acc.dtype)
                self.to_z(index, half, plane).start()

            @pl.when(z == 3)
            def _():
                self.acc[index] = total.astype(self.acc.dtype)
                self.to_z(index, index, 2).start()

            @pl.when(z == 1 - plane)
            def _():
                self.acc[index] = total.astype(self.acc.dtype)
                self.to_z(index, 2 + half, plane).start()

            @pl.when(z == plane)
            def _():
                self.out_ref[half] = total

    def finish(self):
        z = self.place[0]

        @pl.when(z < 2)
        def _():
            for half in range(2):
                first = self.arrived(self.z_box.at[2 + half], 14 + half)
                second = self.arrived(self.z_box.at[half], 12 + half)
                self.out_ref[half] = self.out_ref[half] + first + second

        @pl.when(z >= 2)
        def _():
            self.out_ref[...] = jnp.zeros_like(self.out_ref)

    def close(self):
        z = self.place[0]
        for copy in self.started:
            copy.wait_send()
        for plane, half in self.order:
            index = plane * 2 + half

            @pl.when(z == 2)
            def _():
                self.to_z(index, half, plane).wait_send()

            @pl.when(z == 3)
            def _():
                self.to_z(index, index, 2).wait_send()

            @pl.when(z == 1 - plane)
            def _():
                self.to_z(index, 2 + half, plane).wait_send()


SMALL_ROWS = 16


def finish_kernel(
    x_ref,
    cot_ref,
    ctxa_ref,
    ctxb_ref,
    dqa_ref,
    dqb_ref,
    sent_ref,
    ownkv_ref,
    own_ref,
    right_ref,
    left_ref,
    first_ref,
    par_ref,
    qkv_ref,
    out_ref,
    mlp_ref,
    dsec_ref,
    bg_ref,
    layer_ref,
    xgrad_ref,
    qkvg_ref,
    outg_ref,
    small_ref,
    kv_sum,
    kv_acc,
    q_box,
    p_box,
    z_box,
    kv_send,
    kv_recv,
    proj_ref,
    dfirst_ref,
    qkv_terms,
    out_terms,
    qkv_acc,
    out_acc,
    qkv_box,
    out_box,
    send,
    recv,
    small_acc,
    small_box,
    small_send,
    small_recv,
):
    place = chip_place()
    greet(place)
    kv = KvReduce(place, sent_ref, kv_sum, kv_acc, q_box, p_box, z_box, kv_send, kv_recv)
    kv.begin()
    rows, width = x_ref.shape[1:]
    pair = 2 * HDIM
    cot = cot_ref[0]
    half_width = width // 2
    shard_rows = qkvg_ref.shape[0]
    reduce = Reduce(
        place,
        ("yx", "xy"),
        (qkv_terms, out_terms),
        (qkvg_ref, outg_ref),
        (qkv_acc, out_acc),
        (qkv_box, out_box),
        send,
        recv,
        None,
    )

    def lay(terms, value, first_row, cols):
        for s in range(value.shape[0] // shard_rows):
            part = value[s * shard_rows : (s + 1) * shard_rows]
            terms[first_row // shard_rows + s, :, cols] = part.astype(jnp.bfloat16)

    whole = slice(0, width)
    lay(out_terms, dot_of(ctxa_ref[...], cot, TN), 0, whole)
    lay(out_terms, dot_of(ctxb_ref[...], cot, TN), half_width, whole)
    kv.middle()
    reduce.begin([1], SUM_SLABS)
    own, right, left = own_ref[...], right_ref[...], left_ref[...]
    for side, ref in enumerate((dqa_ref, dqb_ref)):
        for tile in range(half_width // pair):
            at = tile * pair
            part = tile_turn(ref[:, at : at + pair], own, right, left, -1.0)
            at = at + side * half_width
            proj_ref[:, at : at + pair] = part.astype(jnp.bfloat16)
    layer = x_ref[0].astype(jnp.float32)
    layer = layer + jnp.dot(ctxa_ref[...], out_ref[:half_width], preferred_element_type=jnp.float32)
    layer = layer + jnp.dot(ctxb_ref[...], out_ref[half_width:], preferred_element_type=jnp.float32)
    layer = layer + mlp_ref[...] + (par_ref[1:2] + par_ref[2:3])
    layer_ref[0] = layer.astype(jnp.bfloat16)
    kv.planes()
    proj_q = proj_ref[:, :width]
    lay(qkv_terms, dot_of(first_ref[...], proj_q, TN), 0, whole)
    dfirst_ref[...] = dot_of(proj_q, qkv_ref[:, :width], NT)
    reduce.steps([1], SUM_SLABS[:8])
    kv.finish()
    kv_grad = (ownkv_ref[...] + kv_sum[...]).reshape(pair, rows).T
    is_key = lax.broadcasted_iota(jnp.int32, (rows, pair), 1) < HDIM
    turned_kv = jnp.where(is_key, tile_turn(kv_grad, own, right, left, -1.0), kv_grad)
    proj_kv = turned_kv.astype(jnp.bfloat16)
    lay(qkv_terms, dot_of(first_ref[...], proj_kv, TN), 0, slice(width, width + pair))
    d_first = dfirst_ref[...] + dot_of(proj_kv, qkv_ref[:, width:], NT)
    dfirst_ref[...] = d_first
    reduce.begin([0], SUM_SLABS)
    unit, scale = unit_rows(x_ref[0].astype(jnp.float32))
    d_second = dsec_ref[...]

    def column_sum(value):
        return jnp.sum(value, axis=0, keepdims=True)

    small_acc[0:1] = column_sum(proj_ref[:, :width].astype(jnp.float32))
    small_acc[1:2] = column_sum(cot.astype(jnp.float32))
    for j in range(bg_ref.shape[1] // width):
        small_acc[2 + j : 3 + j] = bg_ref[:, j * width : (j + 1) * width]
    small_acc[6:7] = column_sum(d_first * unit)
    small_acc[7:8] = column_sum(d_first)
    small_acc[8:9] = column_sum(d_second * unit)
    small_acc[9:10] = column_sum(d_second)
    small_acc[10:] = jnp.zeros_like(small_acc[10:])
    peers = [near(place, fg=1), near(place, fx=1), near(place, fy=1)]
    peers += [near(place, k=k) for k in (1, 2, 3)]
    sums_out = []

    def small_mail(stage, copy_of):
        copy = remote(
            small_box.at[6 + copy_of],
            small_box.at[stage],
            small_send.at[stage],
            small_recv.at[stage],
            peers[stage],
        )
        copy.start()
        sums_out.append(copy)

    def small_in(stage):
        box = small_box.at[stage]
        remote(box, box, small_send.at[stage], small_recv.at[stage], peers[0]).wait_recv()
        return box[...]

    small_box[6] = small_acc[...]
    small_mail(0, 0)
    d_unit = d_first * par_ref[3:4] + d_second * par_ref[5:6]
    d_unit = d_unit - jnp.mean(d_unit, axis=-1, keepdims=True) - unit * jnp.mean(
        d_unit * unit, axis=-1, keepdims=True
    )
    xgrad_ref[0] = cot.astype(jnp.float32) + scale * d_unit
    for stage in range(1, 3):
        small_box[6 + stage] = small_box[5 + stage] + small_in(stage - 1)
        slabs = SUM_SLABS[:4] if stage == 1 else SUM_SLABS[4:8]
        reduce.steps([0], slabs)
        small_mail(stage, stage)
    small_box[9] = small_box[8] + small_in(2)
    reduce.steps([1, 0], SUM_SLABS[8:12])
    for stage in (3, 4, 5):
        small_mail(stage, 3)
    reduce.steps([1, 0], SUM_SLABS[12:])
    total = small_box[9] + small_in(3) + small_in(4) + small_in(5)
    shard = slot_at(place)
    lead = pltpu.roll(total, (width - shard * shard_rows) % width, 1)[:, :pair]
    inner_share = bg_ref.shape[1] // SLABS
    per_row = width // inner_share
    wide = pltpu.roll(total, (width - (shard % per_row) * inner_share) % width, 1)[:, :pair]
    row_id = lax.broadcasted_iota(jnp.int32, wide.shape, 0)
    wide = column_sum(jnp.where(row_id == 2 + shard // per_row, wide, 0.0))
    small_ref[...] = lead
    small_ref[10:11] = wide
    kv.close()
    reduce.finish()
    for copy in sums_out:
        copy.wait_send()


def finish(args, shapes, collective_id):
    rows, width, columns, shard_rows = shapes
    pair = 2 * HDIM
    low = jnp.bfloat16
    slab = (HDIM, rows)
    qkv_slab, out_slab = (shard_rows, columns), (shard_rows, width)
    return pl.pallas_call(
        finish_kernel,
        in_specs=[vmem_spec()] * len(args),
        out_specs=[vmem_spec()] * 5,
        out_shape=[
            jax.ShapeDtypeStruct((1, rows, width), low),
            jax.ShapeDtypeStruct((1, rows, width), jnp.float32),
            jax.ShapeDtypeStruct(qkv_slab, jnp.float32),
            jax.ShapeDtypeStruct(out_slab, jnp.float32),
            jax.ShapeDtypeStruct((SMALL_ROWS, pair), jnp.float32),
        ],
        scratch_shapes=[
            pltpu.VMEM((2,) + slab, jnp.float32),
            pltpu.VMEM((8,) + slab, low),
            pltpu.VMEM((8,) + slab, low),
            pltpu.VMEM((4,) + slab, low),
            pltpu.VMEM((4,) + slab, low),
            pltpu.SemaphoreType.DMA((16,)),
            pltpu.SemaphoreType.DMA((16,)),
            pltpu.VMEM((rows, width), low),
            pltpu.VMEM((rows, width), jnp.float32),
            pltpu.VMEM((SLABS,) + qkv_slab, low),
            pltpu.VMEM((SLABS,) + out_slab, low),
            pltpu.VMEM((16,) + qkv_slab, low),
            pltpu.VMEM((16,) + out_slab, low),
            pltpu.VMEM((31,) + qkv_slab, low),
            pltpu.VMEM((31,) + out_slab, low),
            pltpu.SemaphoreType.DMA((2, 31)),
            pltpu.SemaphoreType.DMA((2, 31)),
            pltpu.VMEM((SMALL_ROWS, width), jnp.float32),
            pltpu.VMEM((10, SMALL_ROWS, width), jnp.float32),
            pltpu.SemaphoreType.DMA((6,)),
            pltpu.SemaphoreType.DMA((6,)),
        ],
        compiler_params=pltpu.CompilerParams(
            collective_id=collective_id, has_side_effects=True, vmem_limit_bytes=56 << 20
        ),
        name="finish_with_reduce",
    )(*args)


def per_device_direct(
    tokens,
    branch_points,
    qkv_weight,
    out_weight,
    up_weight,
    down_weight,
    query_bias,
    out_bias,
    up_bias,
    down_bias,
    first_gain,
    first_shift,
    second_gain,
    second_shift,
    cotangent,
):
    row_count, width = tokens.shape[1:]
    shard_rows, columns = qkv_weight.shape
    pair = 2 * HDIM
    names = (query_bias, out_bias, down_bias, first_gain, first_shift, second_gain, second_shift)
    small = jnp.stack([jnp.pad(v, (0, pair - v.shape[0])) for v in names + (up_bias,)])
    block_index = lax.axis_index("tok")
    limit = jnp.where(block_index >= PDEV, branch_points[0, 0], block_index * row_count)
    positions = (limit + jnp.arange(row_count, dtype=jnp.int32)).astype(jnp.float32)
    tables = lane_tables(positions, pair)
    key_count = (PDEV + 1) * row_count
    column = jnp.arange(key_count, dtype=jnp.int32)
    shown = jnp.logical_or(column < limit, column >= key_count - row_count)
    bias = jnp.broadcast_to(jnp.where(shown, 0.0, NEGATIVE)[None], (8, key_count))

    def joined(gathered):
        return gathered.reshape(-1, gathered.shape[2])

    qkv_full, out_full, small_all = gather_shards(
        (qkv_weight, out_weight, small), ("yx", "xy", "xy"), 0, "gather"
    )
    qkv_full, out_full = joined(qkv_full), joined(out_full)
    lead = small_all[:, :, :shard_rows].transpose(1, 0, 2).reshape(8, width)
    params = lead.astype(jnp.float32)
    up_bias_full = small_all[:, 7, : up_bias.shape[0]].reshape(1, -1).astype(jnp.float32)
    queries, key_value, all_kv, kv_t, d_context, first_low, second_low = project(
        tokens, cotangent, qkv_full, out_full, params, tables, 1
    )
    kv = (all_kv.reshape(key_count, pair), kv_t, bias)
    context_a, d_query_a, d_keys, d_values, up_full, down_full = attention(
        0, queries, d_context, kv, comm=gather_beside((up_weight, down_weight), ROUTES), collective_id=2
    )
    up_full, down_full = joined(up_full), joined(down_full)
    up_term, down_term, mlp_out, d_second, up_bias_term = mlp(
        second_low, cotangent, up_full, up_bias_full, down_full
    )
    terms = (up_term.reshape(SLABS, -1, up_term.shape[1]), down_term.reshape(SLABS, -1, width))
    context_b, d_query_b, sent, own_term, sum_up_w, sum_down_w = attention(
        1,
        queries,
        d_context,
        kv,
        carried=(d_keys, d_values),
        comm=reduce_beside(terms, ROUTES),
        collective_id=3,
    )
    args = (
        tokens,
        cotangent,
        context_a,
        context_b,
        d_query_a,
        d_query_b,
        sent,
        own_term,
        *tables,
        first_low,
        params,
        qkv_full,
        out_full,
        mlp_out,
        d_second,
        up_bias_term,
    )
    layer_out, input_grad, sum_qkv_w, sum_out_w, sums = finish(
        args, (row_count, width, columns, shard_rows), 4
    )

    def small_sum(row):
        return sums[row, :shard_rows]

    return (
        layer_out,
        key_value[None],
        input_grad,
        sum_qkv_w,
        sum_out_w,
        sum_up_w,
        sum_down_w,
        small_sum(0),
        small_sum(1),
        sums[10, : up_bias.shape[0]],
        small_sum(1),
        small_sum(6),
        small_sum(7),
        small_sum(8),
        small_sum(9),
    )


def pack_small(flat, rows_above, columns):
    shards, count = flat.shape
    rows = -(-count // columns)
    rows += -(rows_above + rows) % 8
    flat = jnp.pad(flat, ((0, 0), (0, rows * columns - count)))
    return flat.reshape(shards, rows, columns)


def unpack_small(packed, sizes):
    shards = packed.shape[0]
    flat = packed.reshape(shards, -1)
    parts = []
    start = 0
    for size in sizes:
        parts.append(flat[:, start : start + size].reshape(shards * size))
        start += size
    return parts


def per_device(
    tokens,
    branch_points,
    qkv_weight,
    out_weight,
    up_weight,
    down_weight,
    query_bias,
    out_bias,
    up_bias,
    down_bias,
    first_gain,
    first_shift,
    second_gain,
    second_shift,
    cotangent,
):
    row_count = tokens.shape[1]
    width = tokens.shape[2]
    shards = lax.axis_size("grp") * lax.axis_size("tok")
    small = [
        query_bias,
        out_bias,
        up_bias,
        down_bias,
        first_gain,
        first_shift,
        second_gain,
        second_shift,
    ]
    sizes = [s.shape[0] for s in small]
    qkv_rows, columns = qkv_weight.shape
    packed = pack_small(jnp.concatenate(small)[None], qkv_rows, columns)[0]
    head = jnp.concatenate([qkv_weight, packed], axis=0)

    def all_of(*shards):
        return [lax.all_gather(w, AXES, axis=0, tiled=False) for w in shards]

    def joined(gathered):
        return gathered.reshape(-1, gathered.shape[2])

    head_all, out_full = all_of(head, out_weight)
    out_full = joined(out_full)
    qkv_full = joined(head_all[:, :qkv_rows])
    (
        query_full,
        out_bias_full,
        up_bias_full,
        down_bias_full,
        gain_one,
        shift_one,
        gain_two,
        shift_two,
    ) = [p.astype(jnp.float32) for p in unpack_small(head_all[:, qkv_rows:], sizes)]
    block_index = lax.axis_index("tok")
    is_cont = block_index >= PDEV
    offsets = jnp.arange(row_count, dtype=jnp.int32)
    limit = jnp.where(is_cont, branch_points[0, 0], block_index * row_count)
    positions = (limit + offsets).astype(jnp.float32)
    tables = turn_tables(positions, 2 * HDIM)
    inputs = tokens[0].astype(jnp.float32)
    first_norm, first_back = jax.vjp(layer_norm, inputs, gain_one, shift_one)
    second_norm, second_back = jax.vjp(layer_norm, inputs, gain_two, shift_two)
    first_low = first_norm.astype(jnp.bfloat16)
    second_low = second_norm.astype(jnp.bfloat16)
    projected = jnp.dot(first_low, qkv_full, preferred_element_type=jnp.float32)
    queries = turn(projected[:, :width] + query_full, tables, 1.0).astype(jnp.bfloat16)
    queries = queries * jnp.asarray(SCORE_SCALE, jnp.bfloat16)
    key_lane = jnp.arange(2 * HDIM, dtype=jnp.int32) < HDIM
    key_tables = (
        jnp.where(key_lane, tables[0], 1.0),
        jnp.where(key_lane, tables[1], 0.0),
        jnp.where(key_lane, tables[2], 0.0),
    )
    key_value = turn(projected[:, width:], key_tables, 1.0).astype(jnp.bfloat16)
    prompt_len = PDEV * row_count
    prompt_kv = lax.all_gather(key_value, "tok", axis=0, tiled=True)[:prompt_len]
    keys_values = jnp.concatenate([prompt_kv, key_value], axis=0)

    grad_rows = cotangent[0]
    grad_float = grad_rows.astype(jnp.float32)
    contract_last = (((1,), (1,)), ((), ()))
    contract_first = (((0,), (0,)), ((), ()))
    matmul = partial(lax.dot_general, preferred_element_type=jnp.float32)
    d_context = matmul(grad_rows, out_full, contract_last)
    tables_kv = attention_tables(keys_values, limit, row_count)
    context_a, d_query_a, d_keys, d_values = attention(0, queries, d_context, tables_kv)
    up_full, down_full = map(joined, all_of(up_weight, down_weight))

    pre_act = matmul(second_low, up_full, (((1,), (0,)), ((), ()))) + up_bias_full
    hidden, gelu_back = jax.vjp(partial(jax.nn.gelu, approximate=False), pre_act)
    hidden_low = hidden.astype(jnp.bfloat16)
    d_hidden = matmul(grad_rows, down_full, contract_last)
    d_pre_low = gelu_back(d_hidden)[0].astype(jnp.bfloat16)
    grad_up_w = matmul(second_low, d_pre_low, contract_first)
    grad_down_w = matmul(hidden_low, grad_rows, contract_first)

    def by_shard(term):
        return term.astype(jnp.bfloat16).reshape(shards, -1, term.shape[1])

    def sum_of(*terms):
        return [
            lax.psum_scatter(t, AXES, scatter_dimension=0, tiled=False).astype(jnp.float32)
            for t in terms
        ]

    wide_terms = (by_shard(grad_up_w), by_shard(grad_down_w))
    context_b, d_query_b, sent, own_term = attention(
        1, queries, d_context, tables_kv, carried=(d_keys, d_values)
    )
    sum_up_w, sum_down_w = sum_of(*wide_terms)
    context_low = jnp.concatenate([context_a, context_b], axis=1)
    d_query = jnp.concatenate([d_query_a, d_query_b], axis=1)
    idle = lax.axis_size("tok") - PDEV
    sent = jnp.pad(sent, ((0, idle), (0, 0), (0, 0), (0, 0)))
    summed = lax.psum_scatter(sent, "tok", scatter_dimension=0, tiled=False)
    summed = summed.astype(jnp.float32)
    kv_grad = (own_term + summed).reshape(2 * HDIM, row_count).T

    result = (
        inputs
        + jnp.dot(context_low, out_full, preferred_element_type=jnp.float32)
        + out_bias_full
    )
    result = (
        result
        + jnp.dot(hidden_low, down_full, preferred_element_type=jnp.float32)
        + down_bias_full
    )
    layer_out = result.astype(jnp.bfloat16)[None]
    d_query_back = turn(d_query, tables, -1.0)
    d_kv_back = turn(kv_grad, key_tables, -1.0)
    d_projected = jnp.concatenate([d_query_back, d_kv_back], axis=1).astype(jnp.bfloat16)
    grad_out_w = matmul(context_low, grad_rows, contract_first)
    grad_qkv_w = matmul(first_low, d_projected, contract_first)
    grad_query_b = jnp.sum(d_projected[:, :width].astype(jnp.float32), axis=0)
    grad_out_b = jnp.sum(grad_float, axis=0)
    grad_up_b = jnp.sum(d_pre_low.astype(jnp.float32), axis=0)
    d_first = matmul(d_projected, qkv_full, contract_last)
    d_second = matmul(d_pre_low, up_full, contract_last)
    input_one, grad_gain_one, grad_shift_one = first_back(d_first)
    input_two, grad_gain_two, grad_shift_two = second_back(d_second)
    input_grad = (grad_float + input_one + input_two)[None]

    small_grads = [
        grad_query_b,
        grad_out_b,
        grad_up_b,
        grad_gain_one,
        grad_shift_one,
        grad_gain_two,
        grad_shift_two,
    ]
    grad_sizes = [g.shape[0] // shards for g in small_grads]
    small_flat = jnp.concatenate([g.reshape(shards, -1) for g in small_grads], axis=1)
    small_flat = pack_small(small_flat, qkv_rows, columns)

    tail = jnp.concatenate([by_shard(grad_qkv_w), small_flat.astype(jnp.bfloat16)], axis=1)
    terms = (tail, by_shard(grad_out_w))
    sum_tail, sum_out_w = sum_of(*terms)
    sum_qkv_w = sum_tail[:qkv_rows]
    (
        sum_query_b,
        sum_out_b,
        sum_up_b,
        sum_gain_one,
        sum_shift_one,
        sum_gain_two,
        sum_shift_two,
    ) = unpack_small(sum_tail[None, qkv_rows:], grad_sizes)
    return (
        layer_out,
        key_value[None],
        input_grad,
        sum_qkv_w,
        sum_out_w,
        sum_up_w,
        sum_down_w,
        sum_query_b,
        sum_out_b,
        sum_up_b,
        sum_out_b,
        sum_gain_one,
        sum_shift_one,
        sum_gain_two,
        sum_shift_two,
    )


def solution(mesh):
    direct = dict(mesh.shape) == {"grp": 2, "tok": 4 * Z_CHIPS}
    placed = (
        P("grp", "tok", None),
        P("grp", "tok"),
        P(("grp", "tok"), None),
        P(("grp", "tok"), None),
        P(("grp", "tok"), None),
        P(("grp", "tok"), None),
        P(("grp", "tok")),
        P(("grp", "tok")),
        P(("grp", "tok")),
        P(("grp", "tok")),
        P(("grp", "tok")),
        P(("grp", "tok")),
        P(("grp", "tok")),
        P(("grp", "tok")),
        P("grp", "tok", None),
    )
    return jax.shard_map(
        per_device_direct if direct else per_device,
        mesh=mesh,
        in_specs=placed,
        out_specs=(
            P("grp", "tok", None),
            P("grp", "tok", None),
            P("grp", "tok", None),
            P(("grp", "tok"), None),
            P(("grp", "tok"), None),
            P(("grp", "tok"), None),
            P(("grp", "tok"), None),
            P(("grp", "tok")),
            P(("grp", "tok")),
            P(("grp", "tok")),
            P(("grp", "tok")),
            P(("grp", "tok")),
            P(("grp", "tok")),
            P(("grp", "tok")),
            P(("grp", "tok")),
        ),
        check_vma=False,
    )
```

```python
from functools import partial

import jax
import jax.numpy as jnp
from jax import lax
from jax.experimental import pallas as pl
from jax.experimental.pallas import tpu as pltpu
from jax.sharding import PartitionSpec as P

HEADS = 12
HDIM = 64
ROT = 16
PDEV = 8
SCORE_SCALE = 0.125
NEGATIVE = -1e30
AXES = ("grp", "tok")
CHUNK = 512


def layer_norm(values, gain, shift):
    centered = values - jnp.mean(values, axis=-1, keepdims=True)
    variance = jnp.mean(centered * centered, axis=-1, keepdims=True)
    return centered * lax.rsqrt(variance + 1e-05) * gain + shift


def turn_tables(positions, width):
    half = ROT // 2
    lane = jnp.arange(width, dtype=jnp.int32) % HDIM
    frequency = 10000.0 ** (-((lane % half).astype(jnp.float32) * 2.0) / ROT)
    short = frequency[:half]
    angles = positions[:, None] * short[None, :]
    reps = width // half
    cosine = jnp.tile(jnp.cos(angles), (1, reps))
    sine = jnp.tile(jnp.sin(angles), (1, reps))
    own = jnp.where(lane < ROT, cosine, 1.0)
    from_right = jnp.where(lane < half, -sine, 0.0)
    from_left = jnp.where(jnp.logical_and(lane >= half, lane < ROT), sine, 0.0)
    return own, from_right, from_left


def lane_tables(positions, width):
    half = ROT // 2
    lane = jnp.arange(width, dtype=jnp.int32) % HDIM
    frequency = 10000.0 ** (-((lane % half).astype(jnp.float32) * 2.0) / ROT)
    angles = positions[:, None] * frequency[None, :]
    cosine, sine = jnp.cos(angles), jnp.sin(angles)
    own = jnp.where(lane < ROT, cosine, 1.0)
    from_right = jnp.where(lane < half, -sine, 0.0)
    from_left = jnp.where(jnp.logical_and(lane >= half, lane < ROT), sine, 0.0)
    return own, from_right, from_left


def turn(values, tables, sign):
    own, from_right, from_left = tables
    reps = values.shape[1] // own.shape[1]
    half = ROT // 2
    own, from_right, from_left = (jnp.tile(t, (1, reps)) for t in tables)
    return (
        values * own
        + sign * (jnp.roll(values, -half, axis=1) * from_right)
        + sign * (jnp.roll(values, half, axis=1) * from_left)
    )


MESH = pl.DeviceIdType.MESH
Z_CHIPS = 4
ROUTES = ("yx", "xy")
SLABS = 32


def chip_place():
    tok = lax.axis_index("tok")
    return tok // 4, (tok // 2) % 2, tok % 2, lax.axis_index("grp")


def near(place, k=0, fy=0, fx=0, fg=0):
    z, y, x, g = place
    zz = (z, z + 1 - 2 * (z % 2), (z + 2) % Z_CHIPS, Z_CHIPS - 1 - z)[k]
    return zz, (1 - y if fy else y), (1 - x if fx else x), (1 - g if fg else g)


def device_at(coords):
    z, y, x, g = coords
    return {"tok": z * 4 + y * 2 + x, "grp": g}


def slot_at(coords):
    z, y, x, g = coords
    return g * 16 + z * 4 + y * 2 + x


def near_pq(place, order, k=0, fp=0, fq=0, fg=0):
    if order == "yx":
        return near(place, k, fp, fq, fg)
    return near(place, k, fq, fp, fg)


def greet(place):
    barrier = pltpu.get_barrier_semaphore()
    peers = [near(place, k=1), near(place, k=2), near(place, k=3)]
    peers += [near(place, fy=1), near(place, fx=1), near(place, fg=1)]
    for peer in peers:
        pl.semaphore_signal(barrier, inc=1, device_id=device_at(peer), device_id_type=MESH)
    pl.semaphore_wait(barrier, len(peers))


def remote(src, dst, send_sem, recv_sem, coords):
    return pltpu.make_async_remote_copy(
        src_ref=src,
        dst_ref=dst,
        send_sem=send_sem,
        recv_sem=recv_sem,
        device_id=device_at(coords),
        device_id_type=MESH,
    )


class Gather:
    def __init__(self, place, orders, ins, outs, send, recv, local):
        self.place, self.orders, self.ins, self.outs = place, orders, ins, outs
        self.send, self.recv, self.local = send, recv, local
        self.started = []

    def push(self, a, slab, index, target):
        def build():
            place, order = self.place, self.orders[a]
            slot = slot_at(near_pq(place, order, *slab))
            dst = self.outs[a].at[slot]
            src = self.ins[a] if slab == (0, 0, 0) else dst
            return remote(src, dst, self.send.at[a, index], self.recv.at[a, index], target())

        build().start()
        self.started.append(build)

    def spread(self, a, k, fp, fq):
        place, order, slab = self.place, self.orders[a], (k, fp, fq)
        if fp == 0 and fq == 0:
            self.push(a, slab, k * 4 + 2, partial(near_pq, place, order, fp=1))
        if fq == 0:
            self.push(a, slab, k * 4 + fp * 2 + 1, partial(near_pq, place, order, fq=1))
        self.push(a, slab, 16 + k * 4 + fp * 2 + fq, partial(near, place, fg=1))

    def arrived(self, a, k, fp, fq, fg=0):
        slot = slot_at(near_pq(self.place, self.orders[a], k, fp, fq, fg))
        index = 16 * fg + k * 4 + fp * 2 + fq
        block = self.outs[a].at[slot]
        remote(
            block, block, self.send.at[a, index], self.recv.at[a, index], near(self.place, fg=1)
        ).wait_recv()

    def own_copy(self, a):
        slot = slot_at(self.place)
        return pltpu.make_async_copy(self.ins[a], self.outs[a].at[slot], self.local.at[a])

    def begin(self, arrays):
        for j in (1, 2, 3):
            for a in arrays:
                self.push(a, (0, 0, 0), j * 4, partial(near, self.place, k=j))
        for a in arrays:
            self.spread(a, 0, 0, 0)
            self.own_copy(a).start()

    def pass_on(self, arrays, slabs):
        for slab in slabs:
            for a in arrays:
                self.arrived(a, *slab)
                self.spread(a, *slab)

    def finish(self, arrays):
        for a in arrays:
            self.own_copy(a).wait()
            for k in range(4):
                for fp in range(2):
                    for fq in range(2):
                        self.arrived(a, k, fp, fq, 1)
        for build in self.started:
            build().wait_send()


Z_SLABS = [(1, 0, 0), (2, 0, 0), (3, 0, 0)]
P_SLABS = [(k, 1, 0) for k in range(4)]
Q_SLABS = [(k, fp, 1) for fp in range(2) for k in range(4)]


def gather_kernel(orders, *refs):
    n = len(orders)
    ins, outs = refs[:n], refs[n : 2 * n]
    send, recv, local = refs[2 * n :]
    place = chip_place()
    greet(place)
    gather = Gather(place, orders, ins, outs, send, recv, local)
    arrays = range(n)
    gather.begin(arrays)
    gather.pass_on(arrays, Z_SLABS + P_SLABS + Q_SLABS)
    gather.finish(arrays)


def gather_shards(shards, orders, collective_id, name):
    n = len(shards)
    return pl.pallas_call(
        partial(gather_kernel, orders),
        in_specs=[pl.BlockSpec(memory_space=pl.ANY)] * n,
        out_specs=[pl.BlockSpec(memory_space=pl.ANY)] * n,
        out_shape=[jax.ShapeDtypeStruct((SLABS,) + s.shape, s.dtype) for s in shards],
        scratch_shapes=[
            pltpu.SemaphoreType.DMA((n, 32)),
            pltpu.SemaphoreType.DMA((n, 32)),
            pltpu.SemaphoreType.DMA((n,)),
        ],
        compiler_params=pltpu.CompilerParams(collective_id=collective_id, has_side_effects=True),
        name=name,
    )(*shards)


class Reduce:
    def __init__(self, place, orders, ins, outs, accs, boxes, send, recv, local):
        self.place, self.orders, self.ins, self.outs = place, orders, ins, outs
        self.accs, self.boxes = accs, boxes
        self.send, self.recv, self.local = send, recv, local
        self.started = []

    def mail(self, a, src, index, target):
        def build():
            box = self.boxes[a].at[index]
            return remote(src(), box, self.send.at[a, index], self.recv.at[a, index], target())

        build().start()
        self.started.append(build)

    def far_term(self, a, slab):
        return self.ins[a].at[slot_at(near_pq(self.place, self.orders[a], *slab, 1))]

    def load(self, a, k, fp, fq):
        slot = slot_at(near_pq(self.place, self.orders[a], k, fp, fq))
        sid = k * 4 + fp * 2 + fq
        return pltpu.make_async_copy(
            self.ins[a].at[slot], self.accs[a].at[sid], self.local.at[a, sid]
        )

    def begin(self, arrays, slabs):
        for k, fp, fq in slabs:
            for a in arrays:
                sid = k * 4 + fp * 2 + fq
                src = partial(self.far_term, a, (k, fp, fq))
                self.mail(a, src, sid, partial(near, self.place, fg=1))
                if self.local is not None:
                    self.load(a, k, fp, fq).start()

    def arrived(self, a, index):
        box = self.boxes[a].at[index]
        remote(
            box, box, self.send.at[a, index], self.recv.at[a, index], near(self.place, fg=1)
        ).wait_recv()
        return box[...].astype(jnp.float32)

    def step(self, a, k, fp, fq):
        sid = k * 4 + fp * 2 + fq
        place, order = self.place, self.orders[a]
        if self.local is not None:
            self.load(a, k, fp, fq).wait()
            total = self.accs[a][sid].astype(jnp.float32)
        else:
            total = self.ins[a][slot_at(near_pq(place, order, k, fp, fq))].astype(jnp.float32)
        total = total + self.arrived(a, sid)
        if fq == 0:
            total = total + self.arrived(a, 16 + k * 2 + fp)
        if fq == 0 and fp == 0:
            total = total + self.arrived(a, 24 + k)
        if (k, fp, fq) == (0, 0, 0):
            for j in (1, 2, 3):
                total = total + self.arrived(a, 27 + j)
            self.outs[a][...] = total
            return
        self.accs[a][sid] = total.astype(jnp.bfloat16)

        def src():
            return self.accs[a].at[sid]

        if fq == 1:
            self.mail(a, src, 16 + k * 2 + fp, partial(near_pq, place, order, fq=1))
        elif fp == 1:
            self.mail(a, src, 24 + k, partial(near_pq, place, order, fp=1))
        else:
            self.mail(a, src, 27 + k, partial(near, place, k=k))

    def steps(self, arrays, slabs):
        for slab in slabs:
            for a in arrays:
                self.step(a, *slab)

    def finish(self):
        for build in self.started:
            build().wait_send()


SUM_SLABS = (
    [(k, 1, 1) for k in (3, 2, 1, 0)]
    + [(k, 0, 1) for k in (3, 2, 1, 0)]
    + [(k, 1, 0) for k in (3, 2, 1, 0)]
    + [(k, 0, 0) for k in (3, 2, 1, 0)]
)


def kv_route(place, half, fp=0, fq=0):
    if half == 0:
        return near(place, fy=fp, fx=fq)
    return near(place, fy=fq, fx=fp)


def kv_slot(coords, plane):
    return plane * 4 + coords[1] * 2 + coords[2]


def attention_kernel(last, plan, counts, *refs):
    inputs, outputs, comm_ins, comm_outs = counts
    q_ref, dc_ref, kv_ref, kvt_ref, bias_ref = refs[:5]
    carried = refs[5:inputs]
    cut = inputs + comm_ins
    ctx_ref, dq_ref = refs[cut : cut + 2]
    results = refs[cut + 2 : cut + outputs]
    scratch = refs[cut + outputs + comm_outs :]
    s_ref, e_ref = scratch[:2]
    if last:
        dkt_ref, dvt_ref = scratch[2:4]
        comm_scratch = scratch[4:]
    else:
        dkt_ref, dvt_ref = results
        comm_scratch = scratch[2:]
    rows = q_ref.shape[0]
    key_count = kv_ref.shape[0]
    pair = 2 * HDIM
    prompt = key_count - rows
    unroll = 4
    step = pl.program_id(0)
    events = {}
    if plan is not None:
        events = plan(refs[inputs:cut], refs[cut + outputs : cut + outputs + comm_outs], comm_scratch)

    def point(index):
        for at_step, at_point in sorted(events):
            if at_point == index:
                pl.when(step == at_step)(events[at_step, at_point])

    @pl.when(step == 0)
    def _():
        if carried:
            dkt_ref[...] = carried[0][...]
            dvt_ref[...] = carried[1][...]
        else:
            dkt_ref[...] = jnp.zeros_like(dkt_ref)
            dvt_ref[...] = jnp.zeros_like(dvt_ref)

    point(0)
    first_head = lax.broadcasted_iota(jnp.int32, (rows, pair), 1) < HDIM

    def stacked(both, on_values):
        swapped = pltpu.roll(both, HDIM, 1)
        if on_values:
            parts = [jnp.where(first_head, 0.0, swapped), jnp.where(first_head, 0.0, both)]
        else:
            parts = [jnp.where(first_head, both, 0.0), jnp.where(first_head, swapped, 0.0)]
        return jnp.concatenate(parts, axis=0).astype(jnp.bfloat16)

    def turned(both):
        flipped = both.T.astype(jnp.bfloat16)
        return jnp.concatenate([flipped[:HDIM], flipped[HDIM:]], axis=1)

    q_both = q_ref[...].astype(jnp.float32)
    q_rows = stacked(q_both, False)
    q_cols = turned(q_both)

    def lane_max(top, scores):
        for j in range(scores.shape[1] // pair):
            top = jnp.maximum(top, scores[:, j * pair : (j + 1) * pair])
        return top

    def score_step(c, top):
        cols = pl.ds(pl.multiple_of(c * CHUNK, CHUNK), CHUNK)
        scores = jnp.dot(q_rows, kvt_ref[:, cols], preferred_element_type=jnp.float32)
        scores = scores + bias_ref[0:1, cols]
        s_ref[:, cols] = scores
        return lane_max(top, scores)

    top = lax.fori_loop(
        0,
        prompt // CHUNK,
        score_step,
        jnp.full((2 * rows, pair), NEGATIVE, jnp.float32),
        unroll=prompt // CHUNK,
    )
    row_id = lax.broadcasted_iota(jnp.int32, (2 * rows, rows), 0) % rows
    col_id = lax.broadcasted_iota(jnp.int32, (2 * rows, rows), 1)
    scores = jnp.dot(q_rows, kvt_ref[:, prompt:], preferred_element_type=jnp.float32)
    scores = jnp.where(col_id <= row_id, scores, NEGATIVE)
    s_ref[:, prompt:] = scores
    top = jnp.max(lane_max(top, scores), axis=1, keepdims=True)
    point(1)

    def weight_step(c, carry):
        total, mixed = carry
        cols = pl.ds(pl.multiple_of(c * CHUNK, CHUNK), CHUNK)
        weights = jnp.exp(s_ref[:, cols] - top)
        for j in range(CHUNK // pair):
            total = total + weights[:, j * pair : (j + 1) * pair]
        low = weights.astype(jnp.bfloat16)
        e_ref[:, cols] = low
        mixed = mixed + jnp.dot(low, kv_ref[cols, :], preferred_element_type=jnp.float32)
        return total, mixed

    zero = jnp.zeros((2 * rows, pair), jnp.float32)
    total, mixed = lax.fori_loop(
        0, key_count // CHUNK, weight_step, (zero, zero), unroll=unroll
    )
    point(3)
    scale = 1.0 / jnp.sum(total, axis=1, keepdims=True)
    mixed = mixed * scale
    context = jnp.where(first_head, pltpu.roll(mixed[:rows], HDIM, 1), mixed[rows:])
    ctx_ref[...] = context.astype(ctx_ref.dtype)
    d_context = dc_ref[...]
    product = d_context * context
    delta_a = jnp.sum(jnp.where(first_head, product, 0.0), axis=1, keepdims=True)
    delta_b = jnp.sum(jnp.where(first_head, 0.0, product), axis=1, keepdims=True)
    delta = jnp.concatenate([delta_a, delta_b], axis=0) * scale
    d_both = d_context * jnp.where(first_head, scale[:rows], scale[rows:])
    d_rows = stacked(d_both, True)
    d_cols = turned(d_both)

    def grad_step(c, d_query):
        cols = pl.ds(pl.multiple_of(c * CHUNK, CHUNK), CHUNK)
        d_probs = jnp.dot(d_rows, kvt_ref[:, cols], preferred_element_type=jnp.float32)
        low = e_ref[:, cols]
        d_scores = (low.astype(jnp.float32) * (d_probs - delta)).astype(jnp.bfloat16)
        dvt_ref[:, cols] += jnp.dot(d_cols, low, preferred_element_type=jnp.float32)
        dkt_ref[:, cols] += jnp.dot(q_cols, d_scores, preferred_element_type=jnp.float32)
        return d_query + jnp.dot(d_scores, kv_ref[cols, :], preferred_element_type=jnp.float32)

    third = key_count // CHUNK // 3
    d_query = lax.fori_loop(0, third, grad_step, zero, unroll=third)
    point(4)
    d_query = lax.fori_loop(third, 2 * third, grad_step, d_query, unroll=third)
    point(5)
    d_query = lax.fori_loop(2 * third, key_count // CHUNK, grad_step, d_query, unroll=3)
    second = pltpu.roll(d_query[rows:], HDIM, 1)
    dq_ref[...] = jnp.where(first_head, d_query[:rows], second) * SCORE_SCALE
    point(6)
    if last:

        @pl.when(step == pl.num_programs(0) - 1)
        def _():
            sent_ref, own_ref = results
            for part, total_ref in enumerate((dkt_ref, dvt_ref)):
                for block in range(prompt // rows):
                    cols = slice(block * rows, (block + 1) * rows)
                    sent_ref[block, part] = total_ref[:, cols].astype(sent_ref.dtype)
                own_ref[part] = total_ref[:, prompt:]


def attention(half, queries, d_context, tables, carried=None, comm=None, collective_id=None):
    keys_values, flipped, bias = tables
    key_count, pair = keys_values.shape
    rows, width = queries.shape
    steps = width // pair // 2
    last = half == 1
    prompt_blocks = key_count // rows - 1

    def whole(*shape):
        return pl.BlockSpec(
            shape, lambda i: (0,) * len(shape), pipeline_mode=pl.Buffered(1)
        )

    def result(*shape):
        return pl.BlockSpec(shape, lambda i: (0,) * len(shape))

    block_in = pl.BlockSpec((rows, pair), lambda i: (0, i + half * steps))
    block = pl.BlockSpec((rows, pair), lambda i: (0, i))
    args = [queries, d_context, keys_values, flipped, bias]
    in_specs = [block_in, block_in] + [whole(*a.shape) for a in args[2:]]
    out_specs = [block, block]
    out_shape = [
        jax.ShapeDtypeStruct((rows, width // 2), jnp.bfloat16),
        jax.ShapeDtypeStruct((rows, width // 2), jnp.float32),
    ]
    scratch = [
        pltpu.VMEM((2 * rows, key_count), jnp.float32),
        pltpu.VMEM((2 * rows, key_count), jnp.bfloat16),
    ]
    sums = [jax.ShapeDtypeStruct((HDIM, key_count), jnp.float32)] * 2
    if last:
        args += list(carried)
        in_specs += [whole(*a.shape) for a in carried]
        out_shape += [
            jax.ShapeDtypeStruct((prompt_blocks, 2, HDIM, rows), jnp.bfloat16),
            jax.ShapeDtypeStruct((2, HDIM, rows), jnp.float32),
        ]
        scratch += [pltpu.VMEM(s.shape, s.dtype) for s in sums]
    else:
        out_shape += sums
    out_specs += [result(*o.shape) for o in out_shape[2:]]
    inputs, outputs = len(args), len(out_shape)
    plan = None
    comm_ins, comm_outs = 0, 0
    if comm is not None:
        plan, more_args, more_out_specs, more_out_shape, more_scratch = comm
        comm_ins, comm_outs = len(more_args), len(more_out_shape)
        args += list(more_args)
        in_specs += [pl.BlockSpec(memory_space=pl.ANY)] * comm_ins
        out_specs += more_out_specs
        out_shape += more_out_shape
        scratch += more_scratch
    return pl.pallas_call(
        partial(attention_kernel, last, plan, (inputs, outputs, comm_ins, comm_outs)),
        grid=(steps,),
        in_specs=in_specs,
        out_specs=out_specs,
        out_shape=out_shape,
        scratch_shapes=scratch,
        compiler_params=pltpu.CompilerParams(
            dimension_semantics=("arbitrary",),
            vmem_limit_bytes=63 << 20,
            collective_id=collective_id,
            has_side_effects=comm is not None,
        ),
        cost_estimate=pl.CostEstimate(
            flops=6 * rows * width * key_count,
            bytes_accessed=8 * rows * width + 16 * key_count * pair,
            transcendentals=rows * HEADS * key_count // 2,
        ),
        name="attention_with_reduce" if last else "attention_with_gather",
    )(*args)


GATHER_PLAN = (
    ((0, 1), [(0, 1, 0)]),
    ((0, 3), [(1, 0, 0)]),
    ((0, 4), [(0, 0, 1)]),
    ((0, 5), [(1, 1, 0), (2, 0, 0)]),
    ((1, 0), [(0, 1, 1)]),
    ((1, 1), [(1, 0, 1)]),
    ((1, 3), [(2, 1, 0), (3, 0, 0)]),
    ((1, 4), [(1, 1, 1)]),
    ((1, 5), [(2, 0, 1)]),
    ((2, 0), [(3, 1, 0)]),
    ((2, 1), [(2, 1, 1), (3, 0, 1)]),
    ((2, 4), [(3, 1, 1)]),
)
BESIDE_SLABS = [(k, fp, fq) for k in (3, 2, 1, 0) for fp, fq in ((1, 1), (0, 1))]
BESIDE_SLABS += [(k, fp, 0) for k in (3, 2, 1, 0) for fp in (1, 0)]
REDUCE_PLAN = (
    ((0, 1), [(3, 1, 1), (3, 0, 1)]),
    ((0, 3), [(2, 1, 1), (2, 0, 1)]),
    ((0, 5), [(3, 1, 0), (1, 1, 1), (1, 0, 1)]),
    ((1, 1), [(2, 1, 0), (0, 1, 1), (0, 0, 1)]),
    ((1, 3), [(3, 0, 0)]),
    ((1, 5), [(1, 1, 0)]),
    ((2, 0), [(2, 0, 0)]),
    ((2, 1), [(0, 1, 0)]),
    ((2, 3), [(1, 0, 0)]),
)


def gather_beside(shards, orders):
    n = len(shards)
    arrays = range(n)

    def plan(ins, outs, scratch):
        place = chip_place()
        gather = Gather(place, orders, ins, outs, *scratch)

        def begin():
            greet(place)
            gather.begin(arrays)

        events = {(0, 0): begin}
        for when, slabs in GATHER_PLAN:
            events[when] = partial(gather.pass_on, arrays, slabs)
        events[2, 6] = partial(gather.finish, arrays)
        return events

    out_shape = [jax.ShapeDtypeStruct((SLABS,) + s.shape, s.dtype) for s in shards]
    out_specs = [pl.BlockSpec(memory_space=pl.ANY)] * n
    scratch = [
        pltpu.SemaphoreType.DMA((n, 32)),
        pltpu.SemaphoreType.DMA((n, 32)),
        pltpu.SemaphoreType.DMA((n,)),
    ]
    return plan, shards, out_specs, out_shape, scratch


def reduce_beside(terms, orders):
    n = len(terms)
    arrays = range(n)

    def plan(ins, outs, scratch):
        place = chip_place()
        reduce = Reduce(place, orders, ins, outs, scratch[:n], scratch[n : 2 * n], *scratch[2 * n :])

        def begin():
            greet(place)
            reduce.begin(arrays, BESIDE_SLABS)

        def end():
            reduce.steps(arrays, SUM_SLABS[15:])
            reduce.finish()

        events = {(0, 0): begin, (2, 6): end}
        for when, slabs in REDUCE_PLAN:
            events[when] = partial(reduce.steps, arrays, slabs)
        return events

    slabs = [t.shape[1:] for t in terms]
    out_shape = [jax.ShapeDtypeStruct(s, jnp.float32) for s in slabs]
    out_specs = [pl.BlockSpec(s, lambda i: (0, 0)) for s in slabs]
    scratch = (
        [pltpu.VMEM((16,) + s, jnp.bfloat16) for s in slabs]
        + [pltpu.VMEM((31,) + s, jnp.bfloat16) for s in slabs]
        + [
            pltpu.SemaphoreType.DMA((n, 31)),
            pltpu.SemaphoreType.DMA((n, 31)),
            pltpu.SemaphoreType.DMA((n, 16)),
        ]
    )
    return plan, terms, out_specs, out_shape, scratch


def attention_tables(keys_values, limit, rows):
    key_count = keys_values.shape[0]
    column = jnp.arange(key_count, dtype=jnp.int32)
    shown = jnp.logical_or(column < limit, column >= key_count - rows)
    bias = jnp.broadcast_to(jnp.where(shown, 0.0, NEGATIVE)[None], (8, key_count))
    return keys_values, keys_values.T, bias


def tile_turn(values, own, from_right, from_left, sign):
    half = ROT // 2
    lanes = values.shape[1]
    ahead = pltpu.roll(values, lanes - half, 1)
    behind = pltpu.roll(values, half, 1)
    return values * own + sign * (ahead * from_right + behind * from_left)


def unit_rows(values):
    centered = values - jnp.mean(values, axis=-1, keepdims=True)
    variance = jnp.mean(centered * centered, axis=-1, keepdims=True)
    scale = lax.rsqrt(variance + 1e-05)
    return centered * scale, scale


NT = (((1,), (1,)), ((), ()))
TN = (((0,), (0,)), ((), ()))
dot_of = partial(lax.dot_general, preferred_element_type=jnp.float32)


class KvGather:
    def __init__(self, place, kv_ref, all_ref, send, recv):
        self.place, self.kv_ref, self.all_ref = place, kv_ref, all_ref
        self.send, self.recv = send, recv
        self.rows = kv_ref.shape[0] // 2
        self.started = []

    def at_z(self, zz):
        return (zz,) + self.place[1:]

    def block(self, slot, half=None):
        if half is None:
            return self.all_ref.at[slot]
        return self.all_ref.at[slot, pl.ds(half * self.rows, self.rows)]

    def wait(self, ref, index):
        remote(
            ref, ref, self.send.at[index], self.recv.at[index], near(self.place, fg=1)
        ).wait_recv()

    def own_push(self, index, zz):
        plane = self.place[0] % 2
        dst = self.block(kv_slot(self.place, plane))
        return remote(
            self.kv_ref, dst, self.send.at[index], self.recv.at[plane], self.at_z(zz)
        )

    def relay(self, plane):
        ref = self.block(kv_slot(self.place, plane))
        return remote(ref, ref, self.send.at[plane], self.recv.at[plane], self.at_z(3))

    def push(self, ref, index, coords):
        copy = remote(ref, ref, self.send.at[index], self.recv.at[index], coords)
        copy.start()
        self.started.append(copy)

    def begin(self):
        @pl.when(self.place[0] < 2)
        def _():
            self.own_push(0, 1 - self.place[0] % 2).start()
            self.own_push(1, 2).start()

    def planes(self):
        z = self.place[0]
        for plane in (1, 0):

            @pl.when(z != plane)
            def _():
                self.wait(self.block(kv_slot(self.place, plane)), plane)

            @pl.when(z == 2)
            def _():
                self.relay(plane).start()

            for half in range(2):
                ref = self.block(kv_slot(self.place, plane), half)
                self.push(ref, 2 + plane * 2 + half, kv_route(self.place, half, fp=1))
                self.push(ref, 6 + plane * 4 + half, kv_route(self.place, half, fq=1))

    def middle(self):
        for plane in (1, 0):
            for half in range(2):
                ref = self.block(kv_slot(kv_route(self.place, half, fp=1), plane), half)
                self.wait(ref, 2 + plane * 2 + half)
                self.push(ref, 6 + plane * 4 + 2 + half, kv_route(self.place, half, fq=1))

    def finish(self):
        for plane in (1, 0):
            for fp in range(2):
                for half in range(2):
                    slot = kv_slot(kv_route(self.place, half, fp, 1), plane)
                    self.wait(self.block(slot, half), 6 + plane * 4 + fp * 2 + half)
        for copy in self.started:
            copy.wait_send()
        z = self.place[0]

        @pl.when(z < 2)
        def _():
            self.own_push(0, 1 - z % 2).wait_send()
            self.own_push(1, 2).wait_send()

        @pl.when(z == 2)
        def _():
            self.relay(0).wait_send()
            self.relay(1).wait_send()


def project_kernel(
    x_ref,
    cot_ref,
    qkv_ref,
    out_ref,
    par_ref,
    own_ref,
    right_ref,
    left_ref,
    q_ref,
    kv_ref,
    all_ref,
    kvt_ref,
    dc_ref,
    first_ref,
    second_ref,
    send,
    recv,
):
    place = chip_place()
    greet(place)
    rows = kv_ref.shape[0]
    pair = 2 * HDIM
    width = q_ref.shape[1]
    unit, _ = unit_rows(x_ref[0].astype(jnp.float32))
    first = (unit * par_ref[3:4] + par_ref[4:5]).astype(jnp.bfloat16)
    first_ref[...] = first
    own, right, left = own_ref[...], right_ref[...], left_ref[...]
    is_key = lax.broadcasted_iota(jnp.int32, (rows, pair), 1) < HDIM
    raw = jnp.dot(first, qkv_ref[:, width:], preferred_element_type=jnp.float32)
    turned_kv = jnp.where(is_key, tile_turn(raw, own, right, left, 1.0), raw)
    kv = turned_kv.astype(jnp.bfloat16)
    kv_ref[...] = kv
    all_ref[PDEV] = kv

    @pl.when(place[0] < 2)
    def _():
        all_ref[kv_slot(place, place[0] % 2)] = kv_ref[...]

    second_ref[...] = (unit * par_ref[5:6] + par_ref[6:7]).astype(jnp.bfloat16)
    gather = KvGather(place, kv_ref, all_ref, send, recv)
    gather.begin()
    for tile in range(width // pair):
        cols = slice(tile * pair, (tile + 1) * pair)
        part = jnp.dot(first_ref[...], qkv_ref[:, cols], preferred_element_type=jnp.float32)
        part = tile_turn(part + par_ref[0:1, cols], own, right, left, 1.0)
        low = part.astype(jnp.bfloat16).astype(jnp.float32)
        q_ref[:, cols] = (low * SCORE_SCALE).astype(jnp.bfloat16)
    gather.planes()
    dc_ref[...] = dot_of(cot_ref[0], out_ref[...], NT)
    gather.middle()

    def turn_over(slot):
        flipped = all_ref[slot].astype(jnp.float32).T
        kvt_ref[:, slot * rows : (slot + 1) * rows] = flipped.astype(jnp.bfloat16)

    turn_over(PDEV)
    gather.finish()
    for slot in range(PDEV):
        turn_over(slot)


def vmem_spec():
    return pl.BlockSpec(memory_space=pltpu.VMEM)


def project(tokens, cotangent, qkv_full, out_full, params, tables, collective_id):
    rows, width = tokens.shape[1:]
    pair = 2 * HDIM
    keys = (PDEV + 1) * rows
    low = jnp.bfloat16
    return pl.pallas_call(
        project_kernel,
        in_specs=[vmem_spec()] * 8,
        out_specs=[vmem_spec()] * 7,
        out_shape=[
            jax.ShapeDtypeStruct((rows, width), low),
            jax.ShapeDtypeStruct((rows, pair), low),
            jax.ShapeDtypeStruct((PDEV + 1, rows, pair), low),
            jax.ShapeDtypeStruct((pair, keys), low),
            jax.ShapeDtypeStruct((rows, width), jnp.float32),
            jax.ShapeDtypeStruct((rows, width), low),
            jax.ShapeDtypeStruct((rows, width), low),
        ],
        scratch_shapes=[pltpu.SemaphoreType.DMA((14,)), pltpu.SemaphoreType.DMA((14,))],
        compiler_params=pltpu.CompilerParams(
            collective_id=collective_id, has_side_effects=True, vmem_limit_bytes=48 << 20
        ),
        name="project_with_gather",
    )(tokens, cotangent, qkv_full, out_full, params, *tables)


def mlp_kernel(
    second_ref, cot_ref, up_ref, bias_ref, down_ref, upg_ref, downg_ref, out_ref, dsec_ref, bg_ref
):
    step = pl.program_id(0)
    second = second_ref[...]
    cot = cot_ref[0]
    pre = jnp.dot(second, up_ref[...], preferred_element_type=jnp.float32) + bias_ref[...]
    below = 0.5 + 0.5 * lax.erf(pre * 0.7071067811865476)
    hidden = (pre * below).astype(jnp.bfloat16)
    slope = below + pre * (jnp.exp(pre * pre * -0.5) * 0.3989422804014327)
    d_pre = (dot_of(cot, down_ref[...], NT) * slope).astype(jnp.bfloat16)
    upg_ref[...] = dot_of(second, d_pre, TN).astype(jnp.bfloat16)
    downg_ref[...] = dot_of(hidden, cot, TN).astype(jnp.bfloat16)
    bg_ref[...] = jnp.sum(d_pre.astype(jnp.float32), axis=0, keepdims=True)
    out = jnp.dot(hidden, down_ref[...], preferred_element_type=jnp.float32)
    d_second = dot_of(d_pre, up_ref[...], NT)

    @pl.when(step == 0)
    def _():
        out_ref[...] = out
        dsec_ref[...] = d_second

    @pl.when(step > 0)
    def _():
        out_ref[...] += out
        dsec_ref[...] += d_second


def mlp(second_low, cotangent, up_full, up_bias, down_full):
    rows, width = second_low.shape
    inner = up_full.shape[1]
    tile = 512
    return pl.pallas_call(
        mlp_kernel,
        grid=(inner // tile,),
        in_specs=[
            pl.BlockSpec((rows, width), lambda i: (0, 0)),
            pl.BlockSpec((1, rows, width), lambda i: (0, 0, 0)),
            pl.BlockSpec((width, tile), lambda i: (0, i)),
            pl.BlockSpec((1, tile), lambda i: (0, i)),
            pl.BlockSpec((tile, width), lambda i: (i, 0)),
        ],
        out_specs=[
            pl.BlockSpec((width, tile), lambda i: (0, i)),
            pl.BlockSpec((tile, width), lambda i: (i, 0)),
            pl.BlockSpec((rows, width), lambda i: (0, 0)),
            pl.BlockSpec((rows, width), lambda i: (0, 0)),
            pl.BlockSpec((1, tile), lambda i: (0, i)),
        ],
        out_shape=[
            jax.ShapeDtypeStruct((width, inner), jnp.bfloat16),
            jax.ShapeDtypeStruct((inner, width), jnp.bfloat16),
            jax.ShapeDtypeStruct((rows, width), jnp.float32),
            jax.ShapeDtypeStruct((rows, width), jnp.float32),
            jax.ShapeDtypeStruct((1, inner), jnp.float32),
        ],
        compiler_params=pltpu.CompilerParams(
            dimension_semantics=("arbitrary",), vmem_limit_bytes=48 << 20
        ),
        name="mlp",
    )(second_low, cotangent, up_full, up_bias, down_full)


class KvReduce:
    order = [(plane, half) for plane in (0, 1) for half in (0, 1)]

    def __init__(self, place, in_ref, out_ref, acc, q_box, p_box, z_box, send, recv):
        self.place, self.in_ref, self.out_ref, self.acc = place, in_ref, out_ref, acc
        self.q_box, self.p_box, self.z_box = q_box, p_box, z_box
        self.send, self.recv = send, recv
        self.started = []

    def mail(self, src, dst, index, coords):
        copy = remote(src, dst, self.send.at[index], self.recv.at[index], coords)
        copy.start()
        self.started.append(copy)

    def arrived(self, box, index):
        remote(
            box, box, self.send.at[index], self.recv.at[index], near(self.place, fg=1)
        ).wait_recv()
        return box[...].astype(jnp.float32)

    def slot(self, plane, half, fp=0, fq=0):
        return kv_slot(kv_route(self.place, half, fp, fq), plane)

    def to_z(self, index, box, zz):
        return remote(
            self.acc.at[index],
            self.z_box.at[box],
            self.send.at[12 + index],
            self.recv.at[12 + box],
            (zz,) + self.place[1:],
        )

    def begin(self):
        for fp in (1, 0):
            for plane, half in self.order:
                index = plane * 4 + fp * 2 + half
                src = self.in_ref.at[self.slot(plane, half, fp, 1), half]
                self.mail(src, self.q_box.at[index], index, kv_route(self.place, half, fq=1))

    def middle(self):
        for plane, half in self.order:
            index = plane * 2 + half
            box = plane * 4 + 2 + half
            total = self.in_ref[self.slot(plane, half, 1, 0), half].astype(jnp.float32)
            total = total + self.arrived(self.q_box.at[box], box)
            self.acc[4 + index] = total.astype(self.acc.dtype)
            src = self.acc.at[4 + index]
            self.mail(src, self.p_box.at[index], 8 + index, kv_route(self.place, half, fp=1))

    def planes(self):
        z = self.place[0]
        for plane, half in self.order:
            index = plane * 2 + half
            box = plane * 4 + half
            total = self.in_ref[self.slot(plane, half), half].astype(jnp.float32)
            total = total + self.arrived(self.q_box.at[box], box)
            total = total + self.arrived(self.p_box.at[index], 8 + index)

            @pl.when(z == 2)
            def _():
                passed = total + self.arrived(self.z_box.at[index], 12 + index)
                self.acc[index] = passed.astype(self.acc.dtype)
                self.to_z(index, half, plane).start()

            @pl.when(z == 3)
            def _():
                self.acc[index] = total.astype(self.acc.dtype)
                self.to_z(index, index, 2).start()

            @pl.when(z == 1 - plane)
            def _():
                self.acc[index] = total.astype(self.acc.dtype)
                self.to_z(index, 2 + half, plane).start()

            @pl.when(z == plane)
            def _():
                self.out_ref[half] = total

    def finish(self):
        z = self.place[0]

        @pl.when(z < 2)
        def _():
            for half in range(2):
                first = self.arrived(self.z_box.at[2 + half], 14 + half)
                second = self.arrived(self.z_box.at[half], 12 + half)
                self.out_ref[half] = self.out_ref[half] + first + second

        @pl.when(z >= 2)
        def _():
            self.out_ref[...] = jnp.zeros_like(self.out_ref)

    def close(self):
        z = self.place[0]
        for copy in self.started:
            copy.wait_send()
        for plane, half in self.order:
            index = plane * 2 + half

            @pl.when(z == 2)
            def _():
                self.to_z(index, half, plane).wait_send()

            @pl.when(z == 3)
            def _():
                self.to_z(index, index, 2).wait_send()

            @pl.when(z == 1 - plane)
            def _():
                self.to_z(index, 2 + half, plane).wait_send()


SMALL_ROWS = 16


def finish_kernel(
    x_ref,
    cot_ref,
    ctxa_ref,
    ctxb_ref,
    dqa_ref,
    dqb_ref,
    sent_ref,
    ownkv_ref,
    own_ref,
    right_ref,
    left_ref,
    first_ref,
    par_ref,
    qkv_ref,
    out_ref,
    mlp_ref,
    dsec_ref,
    bg_ref,
    layer_ref,
    xgrad_ref,
    qkvg_ref,
    outg_ref,
    small_ref,
    kv_sum,
    kv_acc,
    q_box,
    p_box,
    z_box,
    kv_send,
    kv_recv,
    proj_ref,
    dfirst_ref,
    qkv_terms,
    out_terms,
    qkv_acc,
    out_acc,
    qkv_box,
    out_box,
    send,
    recv,
    small_acc,
    small_box,
    small_send,
    small_recv,
):
    place = chip_place()
    greet(place)
    kv = KvReduce(place, sent_ref, kv_sum, kv_acc, q_box, p_box, z_box, kv_send, kv_recv)
    kv.begin()
    rows, width = x_ref.shape[1:]
    pair = 2 * HDIM
    cot = cot_ref[0]
    half_width = width // 2
    shard_rows = qkvg_ref.shape[0]
    reduce = Reduce(
        place,
        ("yx", "xy"),
        (qkv_terms, out_terms),
        (qkvg_ref, outg_ref),
        (qkv_acc, out_acc),
        (qkv_box, out_box),
        send,
        recv,
        None,
    )

    def lay(terms, value, first_row, cols):
        for s in range(value.shape[0] // shard_rows):
            part = value[s * shard_rows : (s + 1) * shard_rows]
            terms[first_row // shard_rows + s, :, cols] = part.astype(jnp.bfloat16)

    whole = slice(0, width)
    lay(out_terms, dot_of(ctxa_ref[...], cot, TN), 0, whole)
    lay(out_terms, dot_of(ctxb_ref[...], cot, TN), half_width, whole)
    kv.middle()
    reduce.begin([1], SUM_SLABS)
    own, right, left = own_ref[...], right_ref[...], left_ref[...]
    for side, ref in enumerate((dqa_ref, dqb_ref)):
        for tile in range(half_width // pair):
            at = tile * pair
            part = tile_turn(ref[:, at : at + pair], own, right, left, -1.0)
            at = at + side * half_width
            proj_ref[:, at : at + pair] = part.astype(jnp.bfloat16)
    layer = x_ref[0].astype(jnp.float32)
    layer = layer + jnp.dot(ctxa_ref[...], out_ref[:half_width], preferred_element_type=jnp.float32)
    layer = layer + jnp.dot(ctxb_ref[...], out_ref[half_width:], preferred_element_type=jnp.float32)
    layer = layer + mlp_ref[...] + (par_ref[1:2] + par_ref[2:3])
    layer_ref[0] = layer.astype(jnp.bfloat16)
    kv.planes()
    proj_q = proj_ref[:, :width]
    lay(qkv_terms, dot_of(first_ref[...], proj_q, TN), 0, whole)
    dfirst_ref[...] = dot_of(proj_q, qkv_ref[:, :width], NT)
    reduce.steps([1], SUM_SLABS[:8])
    kv.finish()
    kv_grad = (ownkv_ref[...] + kv_sum[...]).reshape(pair, rows).T
    is_key = lax.broadcasted_iota(jnp.int32, (rows, pair), 1) < HDIM
    turned_kv = jnp.where(is_key, tile_turn(kv_grad, own, right, left, -1.0), kv_grad)
    proj_kv = turned_kv.astype(jnp.bfloat16)
    lay(qkv_terms, dot_of(first_ref[...], proj_kv, TN), 0, slice(width, width + pair))
    d_first = dfirst_ref[...] + dot_of(proj_kv, qkv_ref[:, width:], NT)
    dfirst_ref[...] = d_first
    reduce.begin([0], SUM_SLABS)
    unit, scale = unit_rows(x_ref[0].astype(jnp.float32))
    d_second = dsec_ref[...]

    def column_sum(value):
        return jnp.sum(value, axis=0, keepdims=True)

    small_acc[0:1] = column_sum(proj_ref[:, :width].astype(jnp.float32))
    small_acc[1:2] = column_sum(cot.astype(jnp.float32))
    for j in range(bg_ref.shape[1] // width):
        small_acc[2 + j : 3 + j] = bg_ref[:, j * width : (j + 1) * width]
    small_acc[6:7] = column_sum(d_first * unit)
    small_acc[7:8] = column_sum(d_first)
    small_acc[8:9] = column_sum(d_second * unit)
    small_acc[9:10] = column_sum(d_second)
    small_acc[10:] = jnp.zeros_like(small_acc[10:])
    peers = [near(place, fg=1), near(place, fx=1), near(place, fy=1)]
    peers += [near(place, k=k) for k in (1, 2, 3)]
    sums_out = []

    def small_mail(stage, copy_of):
        copy = remote(
            small_box.at[6 + copy_of],
            small_box.at[stage],
            small_send.at[stage],
            small_recv.at[stage],
            peers[stage],
        )
        copy.start()
        sums_out.append(copy)

    def small_in(stage):
        box = small_box.at[stage]
        remote(box, box, small_send.at[stage], small_recv.at[stage], peers[0]).wait_recv()
        return box[...]

    small_box[6] = small_acc[...]
    small_mail(0, 0)
    d_unit = d_first * par_ref[3:4] + d_second * par_ref[5:6]
    d_unit = d_unit - jnp.mean(d_unit, axis=-1, keepdims=True) - unit * jnp.mean(
        d_unit * unit, axis=-1, keepdims=True
    )
    xgrad_ref[0] = cot.astype(jnp.float32) + scale * d_unit
    for stage in range(1, 3):
        small_box[6 + stage] = small_box[5 + stage] + small_in(stage - 1)
        slabs = SUM_SLABS[:4] if stage == 1 else SUM_SLABS[4:8]
        reduce.steps([0], slabs)
        small_mail(stage, stage)
    small_box[9] = small_box[8] + small_in(2)
    reduce.steps([1, 0], SUM_SLABS[8:12])
    for stage in (3, 4, 5):
        small_mail(stage, 3)
    reduce.steps([1, 0], SUM_SLABS[12:])
    total = small_box[9] + small_in(3) + small_in(4) + small_in(5)
    shard = slot_at(place)
    lead = pltpu.roll(total, (width - shard * shard_rows) % width, 1)[:, :pair]
    inner_share = bg_ref.shape[1] // SLABS
    per_row = width // inner_share
    wide = pltpu.roll(total, (width - (shard % per_row) * inner_share) % width, 1)[:, :pair]
    row_id = lax.broadcasted_iota(jnp.int32, wide.shape, 0)
    wide = column_sum(jnp.where(row_id == 2 + shard // per_row, wide, 0.0))
    small_ref[...] = lead
    small_ref[10:11] = wide
    kv.close()
    reduce.finish()
    for copy in sums_out:
        copy.wait_send()


def finish(args, shapes, collective_id):
    rows, width, columns, shard_rows = shapes
    pair = 2 * HDIM
    low = jnp.bfloat16
    slab = (HDIM, rows)
    qkv_slab, out_slab = (shard_rows, columns), (shard_rows, width)
    return pl.pallas_call(
        finish_kernel,
        in_specs=[vmem_spec()] * len(args),
        out_specs=[vmem_spec()] * 5,
        out_shape=[
            jax.ShapeDtypeStruct((1, rows, width), low),
            jax.ShapeDtypeStruct((1, rows, width), jnp.float32),
            jax.ShapeDtypeStruct(qkv_slab, jnp.float32),
            jax.ShapeDtypeStruct(out_slab, jnp.float32),
            jax.ShapeDtypeStruct((SMALL_ROWS, pair), jnp.float32),
        ],
        scratch_shapes=[
            pltpu.VMEM((2,) + slab, jnp.float32),
            pltpu.VMEM((8,) + slab, low),
            pltpu.VMEM((8,) + slab, low),
            pltpu.VMEM((4,) + slab, low),
            pltpu.VMEM((4,) + slab, low),
            pltpu.SemaphoreType.DMA((16,)),
            pltpu.SemaphoreType.DMA((16,)),
            pltpu.VMEM((rows, width), low),
            pltpu.VMEM((rows, width), jnp.float32),
            pltpu.VMEM((SLABS,) + qkv_slab, low),
            pltpu.VMEM((SLABS,) + out_slab, low),
            pltpu.VMEM((16,) + qkv_slab, low),
            pltpu.VMEM((16,) + out_slab, low),
            pltpu.VMEM((31,) + qkv_slab, low),
            pltpu.VMEM((31,) + out_slab, low),
            pltpu.SemaphoreType.DMA((2, 31)),
            pltpu.SemaphoreType.DMA((2, 31)),
            pltpu.VMEM((SMALL_ROWS, width), jnp.float32),
            pltpu.VMEM((10, SMALL_ROWS, width), jnp.float32),
            pltpu.SemaphoreType.DMA((6,)),
            pltpu.SemaphoreType.DMA((6,)),
        ],
        compiler_params=pltpu.CompilerParams(
            collective_id=collective_id, has_side_effects=True, vmem_limit_bytes=56 << 20
        ),
        name="finish_with_reduce",
    )(*args)


def per_device_direct(
    tokens,
    branch_points,
    qkv_weight,
    out_weight,
    up_weight,
    down_weight,
    query_bias,
    out_bias,
    up_bias,
    down_bias,
    first_gain,
    first_shift,
    second_gain,
    second_shift,
    cotangent,
):
    row_count, width = tokens.shape[1:]
    shard_rows, columns = qkv_weight.shape
    pair = 2 * HDIM
    names = (query_bias, out_bias, down_bias, first_gain, first_shift, second_gain, second_shift)
    small = jnp.stack([jnp.pad(v, (0, pair - v.shape[0])) for v in names + (up_bias,)])
    block_index = lax.axis_index("tok")
    limit = jnp.where(block_index >= PDEV, branch_points[0, 0], block_index * row_count)
    positions = (limit + jnp.arange(row_count, dtype=jnp.int32)).astype(jnp.float32)
    tables = lane_tables(positions, pair)
    key_count = (PDEV + 1) * row_count
    column = jnp.arange(key_count, dtype=jnp.int32)
    shown = jnp.logical_or(column < limit, column >= key_count - row_count)
    bias = jnp.broadcast_to(jnp.where(shown, 0.0, NEGATIVE)[None], (8, key_count))

    def joined(gathered):
        return gathered.reshape(-1, gathered.shape[2])

    qkv_full, out_full, small_all = gather_shards(
        (qkv_weight, out_weight, small), ("yx", "xy", "xy"), 0, "gather"
    )
    qkv_full, out_full = joined(qkv_full), joined(out_full)
    lead = small_all[:, :, :shard_rows].transpose(1, 0, 2).reshape(8, width)
    params = lead.astype(jnp.float32)
    up_bias_full = small_all[:, 7, : up_bias.shape[0]].reshape(1, -1).astype(jnp.float32)
    queries, key_value, all_kv, kv_t, d_context, first_low, second_low = project(
        tokens, cotangent, qkv_full, out_full, params, tables, 1
    )
    kv = (all_kv.reshape(key_count, pair), kv_t, bias)
    context_a, d_query_a, d_keys, d_values, up_full, down_full = attention(
        0, queries, d_context, kv, comm=gather_beside((up_weight, down_weight), ROUTES), collective_id=2
    )
    up_full, down_full = joined(up_full), joined(down_full)
    up_term, down_term, mlp_out, d_second, up_bias_term = mlp(
        second_low, cotangent, up_full, up_bias_full, down_full
    )
    terms = (up_term.reshape(SLABS, -1, up_term.shape[1]), down_term.reshape(SLABS, -1, width))
    context_b, d_query_b, sent, own_term, sum_up_w, sum_down_w = attention(
        1,
        queries,
        d_context,
        kv,
        carried=(d_keys, d_values),
        comm=reduce_beside(terms, ROUTES),
        collective_id=3,
    )
    args = (
        tokens,
        cotangent,
        context_a,
        context_b,
        d_query_a,
        d_query_b,
        sent,
        own_term,
        *tables,
        first_low,
        params,
        qkv_full,
        out_full,
        mlp_out,
        d_second,
        up_bias_term,
    )
    layer_out, input_grad, sum_qkv_w, sum_out_w, sums = finish(
        args, (row_count, width, columns, shard_rows), 4
    )

    def small_sum(row):
        return sums[row, :shard_rows]

    return (
        layer_out,
        key_value[None],
        input_grad,
        sum_qkv_w,
        sum_out_w,
        sum_up_w,
        sum_down_w,
        small_sum(0),
        small_sum(1),
        sums[10, : up_bias.shape[0]],
        small_sum(1),
        small_sum(6),
        small_sum(7),
        small_sum(8),
        small_sum(9),
    )


def pack_small(flat, rows_above, columns):
    shards, count = flat.shape
    rows = -(-count // columns)
    rows += -(rows_above + rows) % 8
    flat = jnp.pad(flat, ((0, 0), (0, rows * columns - count)))
    return flat.reshape(shards, rows, columns)


def unpack_small(packed, sizes):
    shards = packed.shape[0]
    flat = packed.reshape(shards, -1)
    parts = []
    start = 0
    for size in sizes:
        parts.append(flat[:, start : start + size].reshape(shards * size))
        start += size
    return parts


def per_device(
    tokens,
    branch_points,
    qkv_weight,
    out_weight,
    up_weight,
    down_weight,
    query_bias,
    out_bias,
    up_bias,
    down_bias,
    first_gain,
    first_shift,
    second_gain,
    second_shift,
    cotangent,
):
    row_count = tokens.shape[1]
    width = tokens.shape[2]
    shards = lax.axis_size("grp") * lax.axis_size("tok")
    small = [
        query_bias,
        out_bias,
        up_bias,
        down_bias,
        first_gain,
        first_shift,
        second_gain,
        second_shift,
    ]
    sizes = [s.shape[0] for s in small]
    qkv_rows, columns = qkv_weight.shape
    packed = pack_small(jnp.concatenate(small)[None], qkv_rows, columns)[0]
    head = jnp.concatenate([qkv_weight, packed], axis=0)

    def all_of(*shards):
        return [lax.all_gather(w, AXES, axis=0, tiled=False) for w in shards]

    def joined(gathered):
        return gathered.reshape(-1, gathered.shape[2])

    head_all, out_full = all_of(head, out_weight)
    out_full = joined(out_full)
    qkv_full = joined(head_all[:, :qkv_rows])
    (
        query_full,
        out_bias_full,
        up_bias_full,
        down_bias_full,
        gain_one,
        shift_one,
        gain_two,
        shift_two,
    ) = [p.astype(jnp.float32) for p in unpack_small(head_all[:, qkv_rows:], sizes)]
    block_index = lax.axis_index("tok")
    is_cont = block_index >= PDEV
    offsets = jnp.arange(row_count, dtype=jnp.int32)
    limit = jnp.where(is_cont, branch_points[0, 0], block_index * row_count)
    positions = (limit + offsets).astype(jnp.float32)
    tables = turn_tables(positions, 2 * HDIM)
    inputs = tokens[0].astype(jnp.float32)
    first_norm, first_back = jax.vjp(layer_norm, inputs, gain_one, shift_one)
    second_norm, second_back = jax.vjp(layer_norm, inputs, gain_two, shift_two)
    first_low = first_norm.astype(jnp.bfloat16)
    second_low = second_norm.astype(jnp.bfloat16)
    projected = jnp.dot(first_low, qkv_full, preferred_element_type=jnp.float32)
    queries = turn(projected[:, :width] + query_full, tables, 1.0).astype(jnp.bfloat16)
    queries = queries * jnp.asarray(SCORE_SCALE, jnp.bfloat16)
    key_lane = jnp.arange(2 * HDIM, dtype=jnp.int32) < HDIM
    key_tables = (
        jnp.where(key_lane, tables[0], 1.0),
        jnp.where(key_lane, tables[1], 0.0),
        jnp.where(key_lane, tables[2], 0.0),
    )
    key_value = turn(projected[:, width:], key_tables, 1.0).astype(jnp.bfloat16)
    prompt_len = PDEV * row_count
    prompt_kv = lax.all_gather(key_value, "tok", axis=0, tiled=True)[:prompt_len]
    keys_values = jnp.concatenate([prompt_kv, key_value], axis=0)

    grad_rows = cotangent[0]
    grad_float = grad_rows.astype(jnp.float32)
    contract_last = (((1,), (1,)), ((), ()))
    contract_first = (((0,), (0,)), ((), ()))
    matmul = partial(lax.dot_general, preferred_element_type=jnp.float32)
    d_context = matmul(grad_rows, out_full, contract_last)
    tables_kv = attention_tables(keys_values, limit, row_count)
    context_a, d_query_a, d_keys, d_values = attention(0, queries, d_context, tables_kv)
    up_full, down_full = map(joined, all_of(up_weight, down_weight))

    pre_act = matmul(second_low, up_full, (((1,), (0,)), ((), ()))) + up_bias_full
    hidden, gelu_back = jax.vjp(partial(jax.nn.gelu, approximate=False), pre_act)
    hidden_low = hidden.astype(jnp.bfloat16)
    d_hidden = matmul(grad_rows, down_full, contract_last)
    d_pre_low = gelu_back(d_hidden)[0].astype(jnp.bfloat16)
    grad_up_w = matmul(second_low, d_pre_low, contract_first)
    grad_down_w = matmul(hidden_low, grad_rows, contract_first)

    def by_shard(term):
        return term.astype(jnp.bfloat16).reshape(shards, -1, term.shape[1])

    def sum_of(*terms):
        return [
            lax.psum_scatter(t, AXES, scatter_dimension=0, tiled=False).astype(jnp.float32)
            for t in terms
        ]

    wide_terms = (by_shard(grad_up_w), by_shard(grad_down_w))
    context_b, d_query_b, sent, own_term = attention(
        1, queries, d_context, tables_kv, carried=(d_keys, d_values)
    )
    sum_up_w, sum_down_w = sum_of(*wide_terms)
    context_low = jnp.concatenate([context_a, context_b], axis=1)
    d_query = jnp.concatenate([d_query_a, d_query_b], axis=1)
    idle = lax.axis_size("tok") - PDEV
    sent = jnp.pad(sent, ((0, idle), (0, 0), (0, 0), (0, 0)))
    summed = lax.psum_scatter(sent, "tok", scatter_dimension=0, tiled=False)
    summed = summed.astype(jnp.float32)
    kv_grad = (own_term + summed).reshape(2 * HDIM, row_count).T

    result = (
        inputs
        + jnp.dot(context_low, out_full, preferred_element_type=jnp.float32)
        + out_bias_full
    )
    result = (
        result
        + jnp.dot(hidden_low, down_full, preferred_element_type=jnp.float32)
        + down_bias_full
    )
    layer_out = result.astype(jnp.bfloat16)[None]
    d_query_back = turn(d_query, tables, -1.0)
    d_kv_back = turn(kv_grad, key_tables, -1.0)
    d_projected = jnp.concatenate([d_query_back, d_kv_back], axis=1).astype(jnp.bfloat16)
    grad_out_w = matmul(context_low, grad_rows, contract_first)
    grad_qkv_w = matmul(first_low, d_projected, contract_first)
    grad_query_b = jnp.sum(d_projected[:, :width].astype(jnp.float32), axis=0)
    grad_out_b = jnp.sum(grad_float, axis=0)
    grad_up_b = jnp.sum(d_pre_low.astype(jnp.float32), axis=0)
    d_first = matmul(d_projected, qkv_full, contract_last)
    d_second = matmul(d_pre_low, up_full, contract_last)
    input_one, grad_gain_one, grad_shift_one = first_back(d_first)
    input_two, grad_gain_two, grad_shift_two = second_back(d_second)
    input_grad = (grad_float + input_one + input_two)[None]

    small_grads = [
        grad_query_b,
        grad_out_b,
        grad_up_b,
        grad_gain_one,
        grad_shift_one,
        grad_gain_two,
        grad_shift_two,
    ]
    grad_sizes = [g.shape[0] // shards for g in small_grads]
    small_flat = jnp.concatenate([g.reshape(shards, -1) for g in small_grads], axis=1)
    small_flat = pack_small(small_flat, qkv_rows, columns)

    tail = jnp.concatenate([by_shard(grad_qkv_w), small_flat.astype(jnp.bfloat16)], axis=1)
    terms = (tail, by_shard(grad_out_w))
    sum_tail, sum_out_w = sum_of(*terms)
    sum_qkv_w = sum_tail[:qkv_rows]
    (
        sum_query_b,
        sum_out_b,
        sum_up_b,
        sum_gain_one,
        sum_shift_one,
        sum_gain_two,
        sum_shift_two,
    ) = unpack_small(sum_tail[None, qkv_rows:], grad_sizes)
    return (
        layer_out,
        key_value[None],
        input_grad,
        sum_qkv_w,
        sum_out_w,
        sum_up_w,
        sum_down_w,
        sum_query_b,
        sum_out_b,
        sum_up_b,
        sum_out_b,
        sum_gain_one,
        sum_shift_one,
        sum_gain_two,
        sum_shift_two,
    )


def solution(mesh):
    direct = dict(mesh.shape) == {"grp": 2, "tok": 4 * Z_CHIPS}
    placed = (
        P("grp", "tok", None),
        P("grp", "tok"),
        P(("grp", "tok"), None),
        P(("grp", "tok"), None),
        P(("grp", "tok"), None),
        P(("grp", "tok"), None),
        P(("grp", "tok")),
        P(("grp", "tok")),
        P(("grp", "tok")),
        P(("grp", "tok")),
        P(("grp", "tok")),
        P(("grp", "tok")),
        P(("grp", "tok")),
        P(("grp", "tok")),
        P("grp", "tok", None),
    )
    return jax.shard_map(
        per_device_direct if direct else per_device,
        mesh=mesh,
        in_specs=placed,
        out_specs=(
            P("grp", "tok", None),
            P("grp", "tok", None),
            P("grp", "tok", None),
            P(("grp", "tok"), None),
            P(("grp", "tok"), None),
            P(("grp", "tok"), None),
            P(("grp", "tok"), None),
            P(("grp", "tok")),
            P(("grp", "tok")),
            P(("grp", "tok")),
            P(("grp", "tok")),
            P(("grp", "tok")),
            P(("grp", "tok")),
            P(("grp", "tok")),
            P(("grp", "tok")),
        ),
        check_vma=False,
    )
```
